128 devices in a mesh: dp: 1, ep: 128 (over z, y, x, core).
Axes of the slice: x: 4, y: 4, z: 4, core: 2. Of those that a mesh axis runs over, the one named last changes fastest.
Arguments:
- x_tokens: bfloat16 [8192, 1536], P(('dp', 'ep'))
- slot_expert: int32 [128], replicated
- w1_slots: bfloat16 [128, 1536, 512], P('ep')
- w3_slots: bfloat16 [128, 1536, 512], P('ep')
- w2_slots: bfloat16 [128, 512, 1536], P('ep')
- assign: int32 [8192, 6], P(('dp', 'ep'))
- w_router: bfloat16 [1536, 64], replicated
- w1_shared: bfloat16 [1536, 1024], replicated
- w3_shared: bfloat16 [1536, 1024], replicated
- w2_shared: bfloat16 [1024, 1536], replicated
Outputs:
- output: bfloat16 [8192, 1536], P(('dp', 'ep'))
All inputs are finite; a program needn't handle non-finite values.
Results may differ from the reference program's by a relative error of at most 0.00656328.
Values are sent between devices in bfloat16 or wider.
A program may use at most 1 GiB of HBM per device.

```python
import jax
import jax.numpy as jnp
from jax import lax

DIM_MODEL = 1536
FF_EXPERT = 512
FF_SHARED = 1024
NUM_EXPERTS = 64
TOP_K = 6
NUM_SLOTS = 128
GROUP_SIZE = 128
TOK_DEV = 64

TOKENS = TOK_DEV * GROUP_SIZE
CAP_ROWS = max(4, (3 * TOK_DEV * TOP_K) // NUM_SLOTS)
SEG_ROWS = min(TOKENS, GROUP_SIZE * CAP_ROWS)
ROUTE_SCALE = 2.5


def draw_routing(key_shared, key_part):
    key_rank, key_place = jax.random.split(key_shared, 2)
    rank_expert = jax.random.permutation(key_rank, NUM_EXPERTS).astype(jnp.int32)
    base_of_slot = jax.random.permutation(key_place, NUM_SLOTS).astype(jnp.int32)
    slot_expert = rank_expert[base_of_slot % NUM_EXPERTS]
    slot_of_base = jnp.argsort(base_of_slot).astype(jnp.int32)
    key_noise, key_coin, key_pick = jax.random.split(key_part, 3)
    rank_ids = jnp.arange(NUM_EXPERTS, dtype=jnp.int32)
    rank_bias = (2 * TOP_K * 4096) // (NUM_EXPERTS * (rank_ids + 1))
    noise_int = jax.random.randint(key_noise, (TOKENS, NUM_EXPERTS), 0, 4096, dtype=jnp.int32)
    token_ids = jnp.arange(TOKENS, dtype=jnp.int32)
    forced = token_ids < CAP_ROWS
    force_bonus = jnp.where(forced[:, None] & (rank_ids[None, :] == 0), 16384, 0)
    rank_score = (noise_int + rank_bias[None, :] + force_bonus) * NUM_EXPERTS + rank_ids[None, :]
    chosen_rank = lax.top_k(rank_score, TOP_K)[1].astype(jnp.int32)
    copies = (NUM_SLOTS - 1 - chosen_rank) // NUM_EXPERTS + 1
    coin_flip = jax.random.randint(key_coin, (TOKENS, TOP_K), 0, 2, dtype=jnp.int32)
    pick_copy = jax.random.randint(key_pick, (TOKENS, TOP_K), 0, 65536, dtype=jnp.int32) % copies
    keep_first = (coin_flip == 0) | (forced[:, None] & (chosen_rank == 0))
    copy_index = jnp.where(keep_first, 0, pick_copy)
    slot_pick = slot_of_base[chosen_rank + copy_index * NUM_EXPERTS]
    device_of = (token_ids // TOK_DEV)[:, None]
    group_key = (device_of * NUM_SLOTS + slot_pick).reshape(-1)
    sort_order = jnp.argsort(group_key, stable=True)
    sorted_key = group_key[sort_order]
    first_pos = jnp.searchsorted(sorted_key, sorted_key, side='left').astype(jnp.int32)
    rank_sorted = jnp.arange(TOKENS * TOP_K, dtype=jnp.int32) - first_pos
    rank_flat = jnp.zeros((TOKENS * TOP_K,), jnp.int32).at[sort_order].set(rank_sorted)
    assign = jnp.where(rank_flat < CAP_ROWS, slot_pick.reshape(-1), -1).reshape(TOKENS, TOP_K)
    return slot_expert, assign.astype(jnp.int32)


def setup_inputs(seed: int = 0, part: int = 0) -> dict:
    weight_keys = jax.random.split(jax.random.key(seed), 8)
    part_key = jax.random.fold_in(jax.random.key(seed + 1), part)
    key_tokens, key_route = jax.random.split(part_key, 2)
    slot_expert, assign = draw_routing(weight_keys[0], key_route)
    x_tokens = jax.random.normal(key_tokens, (TOKENS, DIM_MODEL), jnp.float32)
    w1_experts = jax.random.normal(weight_keys[1], (NUM_EXPERTS, DIM_MODEL, FF_EXPERT), jnp.float32) * DIM_MODEL ** -0.5
    w3_experts = jax.random.normal(weight_keys[2], (NUM_EXPERTS, DIM_MODEL, FF_EXPERT), jnp.float32) * DIM_MODEL ** -0.5
    w2_experts = jax.random.normal(weight_keys[3], (NUM_EXPERTS, FF_EXPERT, DIM_MODEL), jnp.float32) * FF_EXPERT ** -0.5
    w_router = jax.random.normal(weight_keys[4], (DIM_MODEL, NUM_EXPERTS), jnp.float32) * DIM_MODEL ** -0.5
    w1_shared = jax.random.normal(weight_keys[5], (DIM_MODEL, FF_SHARED), jnp.float32) * DIM_MODEL ** -0.5
    w3_shared = jax.random.normal(weight_keys[6], (DIM_MODEL, FF_SHARED), jnp.float32) * DIM_MODEL ** -0.5
    w2_shared = jax.random.normal(weight_keys[7], (FF_SHARED, DIM_MODEL), jnp.float32) * FF_SHARED ** -0.5
    return {
        'x_tokens': x_tokens.astype(jnp.bfloat16),
        'slot_expert': slot_expert,
        'w1_slots': w1_experts.astype(jnp.bfloat16)[slot_expert],
        'w3_slots': w3_experts.astype(jnp.bfloat16)[slot_expert],
        'w2_slots': w2_experts.astype(jnp.bfloat16)[slot_expert],
        'assign': assign,
        'w_router': w_router.astype(jnp.bfloat16),
        'w1_shared': w1_shared.astype(jnp.bfloat16),
        'w3_shared': w3_shared.astype(jnp.bfloat16),
        'w2_shared': w2_shared.astype(jnp.bfloat16),
    }


def gate_weights(x_tokens, assign, slot_expert, w_router):
    logits = jnp.dot(x_tokens, w_router, preferred_element_type=jnp.float32)
    gate_prob = jax.nn.sigmoid(logits)
    is_kept = assign >= 0
    chosen = slot_expert[jnp.maximum(assign, 0)]
    picked = jnp.where(is_kept, jnp.take_along_axis(gate_prob, chosen, axis=1), 0.0)
    gate_total = jnp.sum(picked, axis=1, keepdims=True)
    return ROUTE_SCALE * picked / jnp.maximum(gate_total, 1e-30), is_kept


def shared_expert(x_tokens, w1_shared, w3_shared, w2_shared):
    h_gate = jnp.dot(x_tokens, w1_shared, preferred_element_type=jnp.float32)
    h_up = jnp.dot(x_tokens, w3_shared, preferred_element_type=jnp.float32)
    mid_act = (jax.nn.silu(h_gate) * h_up).astype(jnp.bfloat16)
    return jnp.dot(mid_act, w2_shared, preferred_element_type=jnp.float32)


def reference(x_tokens, slot_expert, w1_slots, w3_slots, w2_slots, assign, w_router, w1_shared, w3_shared, w2_shared):
    route_weight, is_kept = gate_weights(x_tokens, assign, slot_expert, w_router)
    shared_out = shared_expert(x_tokens, w1_shared, w3_shared, w2_shared)
    flat_slot = jnp.where(is_kept, assign, NUM_SLOTS).reshape(-1)
    sort_order = jnp.argsort(flat_slot, stable=True)
    sorted_slot = flat_slot[sort_order]
    slot_ids = jnp.arange(NUM_SLOTS, dtype=jnp.int32)
    seg_start = jnp.searchsorted(sorted_slot, slot_ids, side='left').astype(jnp.int32)
    seg_end = jnp.searchsorted(sorted_slot, slot_ids, side='right').astype(jnp.int32)
    token_list = jnp.concatenate([(sort_order // TOP_K).astype(jnp.int32), jnp.zeros((SEG_ROWS,), jnp.int32)])
    weight_list = jnp.concatenate([route_weight.reshape(-1)[sort_order], jnp.zeros((SEG_ROWS,), route_weight.dtype)])
    row_offsets = jnp.arange(SEG_ROWS, dtype=jnp.int32)

    def slot_step(acc_rows, slot_id):
        seg_begin = seg_start[slot_id]
        row_ids = lax.dynamic_slice(token_list, (seg_begin,), (SEG_ROWS,))
        row_weight = lax.dynamic_slice(weight_list, (seg_begin,), (SEG_ROWS,))
        row_weight = jnp.where(row_offsets < seg_end[slot_id] - seg_begin, row_weight, 0.0)
        x_rows = x_tokens[row_ids]
        h_gate = jnp.dot(x_rows, w1_slots[slot_id], preferred_element_type=jnp.float32)
        h_up = jnp.dot(x_rows, w3_slots[slot_id], preferred_element_type=jnp.float32)
        mid_act = (jax.nn.silu(h_gate) * h_up).astype(jnp.bfloat16)
        out_rows = jnp.dot(mid_act, w2_slots[slot_id], preferred_element_type=jnp.float32).astype(jnp.bfloat16)
        acc_rows = acc_rows.at[row_ids].add(row_weight[:, None] * out_rows.astype(jnp.float32))
        return acc_rows, None

    routed = lax.scan(slot_step, jnp.zeros((TOKENS, DIM_MODEL), jnp.float32), slot_ids)[0]
    return (shared_out + routed).astype(jnp.bfloat16)
```

```python
import jax
import jax.numpy as jnp
from jax import lax
from jax.experimental import pallas as pl
from jax.experimental.pallas import tpu as pltpu
from jax.sharding import PartitionSpec as P

ROUTE_SCALE = 2.5
RING = 4
CAP = 9
BF16 = jnp.bfloat16
F32 = jnp.float32
STRIDE = {'x': 2, 'y': 8, 'z': 32}
CLASSES = (('y', 'z', 'x'), ('z', 'x', 'y'), ('x', 'y', 'z'))


def iota(shape, dim):
    return lax.broadcasted_iota(jnp.int32, shape, dim)


def dot(a, b):
    return jnp.dot(a, b, preferred_element_type=F32)


def as_onehot(cond):
    return jnp.where(cond, 1.0, 0.0).astype(BF16)


def three_parts(v):
    hi = v.astype(BF16)
    rest = v - hi.astype(F32)
    mid = rest.astype(BF16)
    lo = (rest - mid.astype(F32)).astype(BF16)
    return hi, mid, lo


def moe_kernel(x_ref, assign_ref, slot_expert_ref, wr_ref, w1_hbm, w3_hbm, w2_hbm, s1_hbm, s3_hbm, s2_hbm, y_ref,
               G, T, tab, Pm, Sb, R, Ob, Hb, Z, F, zs, w1, w3, w2, s1, s3, s2,
               wsem, lsem, g1s, g1r, g2s, g2r, t1s, t1r, t2s, t2r, d3s, d3r, d5s, d5r, d6s, d6r):
    me = lax.axis_index('ep')
    core = me % 2
    pos = {'x': (me // 2) % RING, 'y': (me // 8) % RING, 'z': me // 32}
    third = x_ref.shape[1] // 3

    def moved(axis, value):
        return (value - pos[axis]) * STRIDE[axis]

    def remote(src, dst, ssem, rsem, dev):
        return pltpu.make_async_remote_copy(src_ref=src, dst_ref=dst, send_sem=ssem, recv_sem=rsem,
                                            device_id={'ep': dev}, device_id_type=pl.DeviceIdType.MESH)

    barrier = pltpu.get_barrier_semaphore()
    partners = 0

    def greet(dev):
        pl.semaphore_signal(barrier, inc=1, device_id={'ep': dev}, device_id_type=pl.DeviceIdType.MESH)

    other = 1 - 2 * core
    greet(me + other)
    partners += 1
    for axis in 'xyz':
        for d in range(1, RING):
            dev = me + moved(axis, (pos[axis] + d) % RING)
            greet(dev)
            greet(dev + other)
            partners += 2
    for a, b, _ in CLASSES:
        for d in range(1, RING):
            for e in range(1, RING):
                greet(me + moved(a, (pos[a] + d) % RING) + moved(b, (pos[b] + e) % RING))
                partners += 1

    weight_copies = [pltpu.make_async_copy(s, d, wsem.at[i]) for i, (s, d) in enumerate(
        ((s1_hbm, s1), (s3_hbm, s3), (s2_hbm, s2), (w1_hbm.at[0], w1), (w3_hbm.at[0], w3), (w2_hbm.at[0], w2)))]
    for c in weight_copies:
        c.start()

    tokens = x_ref.shape[0]
    slots = slot_expert_ref.shape[1]
    slot_lane = iota((tokens, slots), 1)
    chosen = jnp.zeros((tokens, slots), F32)
    for k in range(assign_ref.shape[1]):
        chosen = chosen + jnp.where(assign_ref[:, k:k + 1] == slot_lane, 1.0, 0.0)
    lower = as_onehot(iota((tokens, tokens), 1) < iota((tokens, tokens), 0))
    rank = jnp.where(chosen > 0.5, dot(lower, chosen.astype(BF16)), 99.0)
    token_id = (iota((tokens, slots), 0) + 1).astype(F32)
    tab_rows = [jnp.sum(jnp.where(rank == float(r), token_id, 0.0), axis=0, keepdims=True) for r in range(CAP)]
    tab[...] = jnp.concatenate(tab_rows + [jnp.zeros((16 - CAP, slots), F32)], axis=0).astype(BF16)

    pl.semaphore_wait(barrier, partners)

    for cls, (a1, a2, a3) in enumerate(CLASSES):
        cols = pl.ds(cls * third, third)
        here = (cls, pos[a2], pos[a1])
        for d in (2, 1, 3):
            dev = me + moved(a1, (pos[a1] + d) % RING)
            remote(tab, T.at[here], t1s.at[cls, d], t1r.at[cls, d], dev).start()
            remote(x_ref.at[:, cols], G.at[here], g1s.at[cls, d], g1r.at[cls, d], dev).start()
        pltpu.make_async_copy(tab, T.at[here], t1r.at[cls, 0]).start()
        pltpu.make_async_copy(x_ref.at[:, cols], G.at[here], g1r.at[cls, 0]).start()

    gate = jax.nn.sigmoid(dot(x_ref[...], wr_ref[...]))
    num_experts = wr_ref.shape[1]
    slot_of = as_onehot(iota((num_experts, slots), 0) == slot_expert_ref[...])
    gate_slot = sum(dot(p, slot_of) for p in three_parts(gate))
    picked = jnp.where(chosen > 0.5, gate_slot, 0.0)
    route = ROUTE_SCALE * picked / jnp.maximum(jnp.sum(picked, axis=1, keepdims=True), 1e-30)
    route_parts = jnp.concatenate(three_parts(route), axis=0)
    rank_bf = rank.astype(BF16)

    for cls, (a1, a2, a3) in enumerate(CLASSES):
        cols = pl.ds(cls * third, third)
        here = (cls, pos[a2], pos[a1])
        for d in range(RING):
            pltpu.make_async_copy(tab, T.at[here], t1r.at[cls, d]).wait()
            pltpu.make_async_copy(x_ref.at[:, cols], G.at[here], g1r.at[cls, d]).wait()
        row = (cls, pos[a2])
        for d in (2, 1, 3):
            dev = me + moved(a2, (pos[a2] + d) % RING)
            remote(T.at[row], T.at[row], t2s.at[cls, d], t2r.at[cls, d], dev).start()
            remote(G.at[row], G.at[row], g2s.at[cls, d], g2r.at[cls, d], dev).start()

    for c in weight_copies[:3]:
        c.wait()
    ff_shared = s1.shape[1]
    step = 512
    acc = jnp.zeros((tokens, x_ref.shape[1]), F32)
    for f in range(0, ff_shared, step):
        xs = x_ref[...]
        mid = (jax.nn.silu(dot(xs, s1[:, f:f + step])) * dot(xs, s3[:, f:f + step])).astype(BF16)
        acc = acc + dot(mid, s2[f:f + step, :])
    zs[...] = acc

    rows = CAP * 16
    qi, qj = iota((rows, 256), 0), iota((rows, 256), 1)
    by_rank = as_onehot(qj == (qi % 16) * 16 + qi // 16)
    src_base = ((iota((rows, 128), 0) % 16) * tokens).astype(F32)
    lane = iota((rows, 128), 1).astype(F32)
    for cls, (a1, a2, a3) in enumerate(CLASSES):
        row = (cls, pos[a2])
        for d in (2, 1, 3):
            pltpu.make_async_copy(T.at[row], T.at[row], t2r.at[cls, d]).wait()
            pltpu.make_async_copy(G.at[row], G.at[row], g2r.at[cls, d]).wait()
        tabs = dot(by_rank, T[cls].reshape(256, slots)).astype(BF16)
        line = me - core - pos[a3] * STRIDE[a3]

        def select(i, _, cls=cls, a3=a3, tabs=tabs, line=line):
            d = (i + 2) % RING
            v = (pos[a3] + d) % RING
            for e in range(2):
                slot = line + v * STRIDE[a3] + (core + e) % 2
                pick = as_onehot(iota((slots, 128), 0) == slot)
                val = dot(tabs, pick)
                code = jnp.where(val > 0.5, val - 1.0 + src_base, -1.0)
                for b in range(16 * tokens // 128):
                    Pm[e * rows:(e + 1) * rows, b * 128:(b + 1) * 128] = as_onehot(code == lane + float(b * 128))
            out = dot(Pm[...], G[cls].reshape(16 * tokens, third)).astype(BF16)
            Sb[cls, pl.ds(2 * d, 2)] = out.reshape(2, CAP, 16, third)
            for e in range(2):
                k = 2 * d + e
                dev = me + moved(a3, v) + (core + e) % 2 - core
                src, dst = Sb.at[cls, k], R.at[cls, pl.ds(core * CAP, CAP), pos[a3]]
                if e == 0:
                    @pl.when(d == 0)
                    def _():
                        pltpu.make_async_copy(src, dst, d3r.at[cls, k]).start()

                    @pl.when(d != 0)
                    def _():
                        remote(src, dst, d3s.at[cls, k], d3r.at[cls, k], dev).start()
                else:
                    remote(src, dst, d3s.at[cls, k], d3r.at[cls, k], dev).start()
            return 0

        lax.fori_loop(0, RING, select, 0)

    for c in weight_copies[3:]:
        c.wait()
    blk = 3 * 64
    pi, pj = iota((blk, blk), 0), iota((blk, blk), 1)

    def bits(v):
        return v // 16 % 4, v // 4 % 4, v % 4

    ix, iz, iy = bits(pi)
    jx, jz, jy = bits(pj)
    to_first = {1: as_onehot(pj == pi // 64 * 64 + iy * 16 + ix * 4 + iz),
                2: as_onehot(pj == pi // 64 * 64 + iz * 16 + iy * 4 + ix)}
    from_first = {1: as_onehot(pi == pj // 64 * 64 + jy * 16 + jx * 4 + jz),
                  2: as_onehot(pi == pj // 64 * 64 + jz * 16 + jy * 4 + jx)}

    def permuted(mats, cls, value):
        if cls == 0:
            return value
        return jnp.concatenate([dot(mats[cls], value[i:i + blk]).astype(BF16)
                                for i in range(0, value.shape[0], blk)], axis=0)

    def expert(e, _):
        half = (core + e) % 2
        for cls in range(3):
            for d in range(RING):
                pltpu.make_async_copy(Sb.at[cls, 0], Sb.at[cls, 0], d3r.at[cls, 2 * d + e]).wait()
        n = CAP * 64
        xs = jnp.concatenate([permuted(to_first, cls, R[cls, pl.ds(half * CAP, CAP)].reshape(n, third))
                              for cls in range(3)], axis=1)
        mid = (jax.nn.silu(dot(xs, w1[...])) * dot(xs, w3[...])).astype(BF16)
        for cls, (a1, a2, a3) in enumerate(CLASSES):
            out = dot(mid, w2[:, cls * third:(cls + 1) * third]).astype(BF16)
            Ob[cls, pl.ds(half * CAP, CAP)] = permuted(from_first, cls, out).reshape(CAP, RING, 16, third)
            for d in (2, 1, 3, 0):
                v = (pos[a3] + d) % RING
                k = 2 * d + e
                dev = me + moved(a3, v) + half - core
                src, dst = Ob.at[cls, pl.ds(half * CAP, CAP), v], Hb.at[cls, :, pos[a3] * 2 + core]
                if d == 0:
                    @pl.when(e == 0)
                    def _():
                        pltpu.make_async_copy(src, dst, d5r.at[cls, k]).start()

                    @pl.when(e != 0)
                    def _():
                        remote(src, dst, d5s.at[cls, k], d5r.at[cls, k], dev).start()
                else:
                    remote(src, dst, d5s.at[cls, k], d5r.at[cls, k], dev).start()
        return 0

    lax.fori_loop(0, 2, expert, 0)

    ri, rj = iota((256, 256), 0), iota((256, 256), 1)
    by_source = as_onehot(rj == ri // 8 % 2 * 128 + ri % 8 * 16 + ri // 16)
    for cls, (a1, a2, a3) in enumerate(CLASSES):
        for k in range(8):
            pltpu.make_async_copy(Hb.at[cls, :, 0], Hb.at[cls, :, 0], d5r.at[cls, k]).wait()
        for rp in range(5):
            if rp < 4:
                out = dot(by_source, Hb[cls, 2 * rp:2 * rp + 2].reshape(256, third))
            else:
                out = dot(by_source[:, :128], Hb[cls, 8].reshape(128, third))
            Z[cls, rp] = out.astype(BF16).reshape(16, 16, third)

        home = pos[a2] * RING + pos[a1]

        def send_home(k, _, cls=cls, a1=a1, a2=a2, home=home):
            v2, v1 = (pos[a2] + k // RING) % RING, (pos[a1] + k % RING) % RING
            dev = me + moved(a2, v2) + moved(a1, v1)
            remote(Z.at[cls, :, v2 * RING + v1], F.at[cls, :, home], d6s.at[cls, k], d6r.at[cls, k], dev).start()
            return 0

        lax.fori_loop(1, 16, send_home, 0)
        pltpu.make_async_copy(Z.at[cls, :, home], F.at[cls, :, home], d6r.at[cls, 0]).start()

    ei, ej = iota((slots, 256), 0), iota((slots, 256), 1)
    rank_bit = (iota((tokens, 256), 1) // 8 % 2).astype(F32)
    for cls, (a1, a2, a3) in enumerate(CLASSES):
        slot = ej // 64 * STRIDE[a2] + ej // 16 % 4 * STRIDE[a1] + ej // 2 % 4 * STRIDE[a3] + ej % 2
        spread = as_onehot(ei == slot)
        rank_exp = dot(rank_bf, spread) - rank_bit
        w_exp = dot(route_parts, spread)
        for k in range(16):
            pltpu.make_async_copy(Z.at[cls, :, 0], Z.at[cls, :, 0], d6r.at[cls, k]).wait()
        acc = jnp.zeros((3 * tokens, third), F32)
        for rp in range(5):
            hit = rank_exp == float(2 * rp)
            w = jnp.where(jnp.concatenate([hit, hit, hit], axis=0), w_exp, 0.0).astype(BF16)
            acc = acc + dot(w, F[cls, rp].reshape(256, third))
        routed = acc[2 * tokens:] + acc[tokens:2 * tokens] + acc[:tokens]
        y_ref[:, cls * third:(cls + 1) * third] = (zs[:, cls * third:(cls + 1) * third] + routed).astype(BF16)

    for cls, (a1, a2, a3) in enumerate(CLASSES):
        here = (cls, pos[a2], pos[a1])
        row = (cls, pos[a2])
        for d in range(1, RING):
            pltpu.make_async_copy(tab, T.at[here], t1s.at[cls, d]).wait()
            pltpu.make_async_copy(x_ref.at[:, pl.ds(cls * third, third)], G.at[here], g1s.at[cls, d]).wait()
            pltpu.make_async_copy(T.at[row], T.at[row], t2s.at[cls, d]).wait()
            pltpu.make_async_copy(G.at[row], G.at[row], g2s.at[cls, d]).wait()
        for k in range(1, 8):
            pltpu.make_async_copy(Sb.at[cls, 0], Sb.at[cls, 0], d3s.at[cls, k]).wait()
            pltpu.make_async_copy(Sb.at[cls, 0], Sb.at[cls, 0], d5s.at[cls, k]).wait()
        for k in range(1, 16):
            pltpu.make_async_copy(Z.at[cls, :, 0], Z.at[cls, :, 0], d6s.at[cls, k]).wait()


def solution(mesh):
    def device_step(x_tokens, slot_expert, w1_slots, w3_slots, w2_slots, assign, w_router, w1_shared, w3_shared, w2_shared):
        tokens, dim = x_tokens.shape
        third = dim // 3
        vmem = pl.BlockSpec(memory_space=pltpu.VMEM)
        hbm = pl.BlockSpec(memory_space=pl.ANY)
        dma = pltpu.SemaphoreType.DMA
        V = pltpu.VMEM
        return pl.pallas_call(
            moe_kernel,
            out_shape=jax.ShapeDtypeStruct((tokens, dim), BF16),
            in_specs=[vmem] * 4 + [hbm] * 6,
            out_specs=vmem,
            scratch_shapes=[
                V((3, RING, RING, tokens, third), BF16),
                V((3, RING, RING, 16, slot_expert.shape[0]), BF16),
                V((16, slot_expert.shape[0]), BF16),
                V((2 * CAP * 16, 16 * tokens), BF16),
                V((3, 8, CAP, 16, third), BF16),
                V((3, 2 * CAP, RING, 16, third), BF16),
                V((3, 2 * CAP, RING, 16, third), BF16),
                V((3, CAP, 8, 16, third), BF16),
                V((3, 5, 16, 16, third), BF16),
                V((3, 5, 16, 16, third), BF16),
                V((tokens, dim), F32),
                V(w1_slots.shape[1:], BF16), V(w3_slots.shape[1:], BF16), V(w2_slots.shape[1:], BF16),
                V(w1_shared.shape, BF16), V(w3_shared.shape, BF16), V(w2_shared.shape, BF16),
                dma((6,)), dma((3,)),
                dma((3, 4)), dma((3, 4)), dma((3, 4)), dma((3, 4)),
                dma((3, 4)), dma((3, 4)), dma((3, 4)), dma((3, 4)),
                dma((3, 8)), dma((3, 8)), dma((3, 8)), dma((3, 8)),
                dma((3, 16)), dma((3, 16)),
            ],
            compiler_params=pltpu.CompilerParams(collective_id=0, has_side_effects=True,
                                                 vmem_limit_bytes=60 * 2 ** 20),
        )(x_tokens, assign, slot_expert.reshape(1, -1), w_router, w1_slots, w3_slots, w2_slots,
          w1_shared, w3_shared, w2_shared)

    token_spec = P(('dp', 'ep'), None)
    slot_spec = P('ep', None, None)
    return jax.shard_map(device_step, mesh=mesh,
                         in_specs=(token_spec, P(), slot_spec, slot_spec, slot_spec, token_spec, P(), P(), P(), P()),
                         out_specs=token_spec, check_vma=False)
```

```python
import jax
import jax.numpy as jnp
from jax import lax
from jax.experimental import pallas as pl
from jax.experimental.pallas import tpu as pltpu
from jax.sharding import PartitionSpec as P

ROUTE_SCALE = 2.5
RING = 4
CAP = 9
BF16 = jnp.bfloat16
F32 = jnp.float32
STRIDE = {'x': 2, 'y': 8, 'z': 32}
CLASSES = (('y', 'z', 'x'), ('z', 'x', 'y'), ('x', 'y', 'z'))


def iota(shape, dim):
    return lax.broadcasted_iota(jnp.int32, shape, dim)


def dot(a, b):
    return jnp.dot(a, b, preferred_element_type=F32)


def dot_t(a, b):
    return lax.dot_general(a, b, (((1,), (1,)), ((), ())), preferred_element_type=F32)


def as_onehot(cond):
    return jnp.where(cond, 1.0, 0.0).astype(BF16)


def three_parts(v):
    hi = v.astype(BF16)
    rest = v - hi.astype(F32)
    mid = rest.astype(BF16)
    lo = (rest - mid.astype(F32)).astype(BF16)
    return hi, mid, lo


def moe_kernel(x_ref, assign_ref, slot_expert_ref, wr_ref, w1_hbm, w3_hbm, w2_hbm, s1_hbm, s3_hbm, s2_hbm, y_ref,
               G, T, tab, Pm, Sb, R, Ob, Hb, Z, F, Cs, Cr, U, A, zs, w1, w3, w2, s1, s3, s2,
               wsem, g1s, g1r, g2s, g2r, t1s, t1r, t2s, t2r, cs, cr, d3s, d3r, d5s, d5r, d6s, d6r, d7s, d7r):
    me = lax.axis_index('ep')
    core = me % 2
    pos = {'x': (me // 2) % RING, 'y': (me // 8) % RING, 'z': me // 32}
    third = x_ref.shape[1] // 3

    def moved(axis, value):
        return (value - pos[axis]) * STRIDE[axis]

    def step_to(axis, d):
        return (pos[axis] + d) % RING

    def remote(src, dst, ssem, rsem, dev):
        return pltpu.make_async_remote_copy(src_ref=src, dst_ref=dst, send_sem=ssem, recv_sem=rsem,
                                            device_id={'ep': dev}, device_id_type=pl.DeviceIdType.MESH)

    def local(src, dst, sem):
        return pltpu.make_async_copy(src, dst, sem)

    barrier = pltpu.get_barrier_semaphore()

    def greet(dev):
        pl.semaphore_signal(barrier, inc=1, device_id={'ep': dev}, device_id_type=pl.DeviceIdType.MESH)

    other = 1 - 2 * core
    greet(me + other)
    for axis in 'xyz':
        for d in range(1, RING):
            dev = me + moved(axis, step_to(axis, d))
            greet(dev)
            greet(dev + other)

    weight_copies = [pltpu.make_async_copy(s, d, wsem.at[i]) for i, (s, d) in enumerate(
        ((s1_hbm, s1), (s3_hbm, s3), (s2_hbm, s2), (w1_hbm.at[0], w1), (w3_hbm.at[0], w3), (w2_hbm.at[0], w2)))]
    for c in weight_copies:
        c.start()

    tokens = x_ref.shape[0]
    slots = slot_expert_ref.shape[1]
    slot_row = iota((slots, tokens), 0)
    chosen_t = jnp.zeros((slots, tokens), F32)
    for k in range(assign_ref.shape[0]):
        chosen_t = chosen_t + jnp.where(assign_ref[k:k + 1, :] == slot_row, 1.0, 0.0)
    ti, tj = iota((tokens, tokens), 0), iota((tokens, tokens), 1)
    chosen = dot_t(as_onehot(ti == tj), chosen_t.astype(BF16))
    rank = jnp.where(chosen > 0.5, dot(as_onehot(tj < ti), chosen.astype(BF16)), 99.0)
    token_id = (iota((tokens, slots), 0) + 1).astype(F32)
    tab_rows = [jnp.sum(jnp.where(rank == float(r), token_id, 0.0), axis=0, keepdims=True) for r in range(CAP)]
    tab[...] = jnp.concatenate(tab_rows + [jnp.zeros((16 - CAP, slots), F32)], axis=0).astype(BF16)

    pl.semaphore_wait(barrier, 19)

    def spread(cls, k, src_t, src_g, to):
        a1, a2, _ = CLASSES[cls]
        here = (cls, pos[a2], to)
        for d in (1, 3, 2):
            dev = me + moved(a2, step_to(a2, d))
            remote(src_t, T.at[here], t2s.at[cls, k, d], t2r.at[cls, k, d], dev).start()
            remote(src_g, G.at[here], g2s.at[cls, k, d], g2r.at[cls, k, d], dev).start()

    def cols(cls):
        return x_ref.at[:, pl.ds(cls * third, third)]

    for cls, (a1, a2, a3) in enumerate(CLASSES):
        here = (cls, pos[a2], pos[a1])
        for d in (1, 3, 2):
            dev = me + moved(a1, step_to(a1, d))
            remote(tab, T.at[here], t1s.at[cls, d], t1r.at[cls, d], dev).start()
            remote(cols(cls), G.at[here], g1s.at[cls, d], g1r.at[cls, d], dev).start()
    for cls, (a1, a2, a3) in enumerate(CLASSES):
        here = (cls, pos[a2], pos[a1])
        spread(cls, 0, tab, cols(cls), pos[a1])
        local(tab, T.at[here], t1r.at[cls, 0]).start()
        local(cols(cls), G.at[here], g1r.at[cls, 0]).start()

    gate = jax.nn.sigmoid(dot_t(x_ref[...], wr_ref[...]))
    num_experts = wr_ref.shape[0]
    slot_of = as_onehot(iota((num_experts, slots), 0) == slot_expert_ref[...])
    gate_slot = sum(dot(p, slot_of) for p in three_parts(gate))
    picked = jnp.where(chosen > 0.5, gate_slot, 0.0)
    route = ROUTE_SCALE * picked / jnp.maximum(jnp.sum(picked, axis=1, keepdims=True), 1e-30)
    route_rank = jnp.concatenate(three_parts(route) + (rank.astype(BF16),), axis=1)

    for d in (3, 1, 2):
        for cls, (a1, a2, a3) in enumerate(CLASSES):
            owner = (pos[a1] + RING - d) % RING
            here = (cls, pos[a2], owner)
            local(tab, T.at[here], t1r.at[cls, d]).wait()
            local(cols(cls), G.at[here], g1r.at[cls, d]).wait()
            spread(cls, d, T.at[here], G.at[here], owner)

    si, sj = iota((4 * slots, 128), 0), iota((4 * slots, 128), 1)
    for cls, (a1, a2, a3) in enumerate(CLASSES):
        q_slot = (sj // 32 * slots + sj // 8 % 4 * STRIDE[a2] + sj // 4 % 2 + sj % 4 * STRIDE[a3])
        for v in range(RING):
            Cs[cls, v] = dot(route_rank, as_onehot(si == q_slot + v * STRIDE[a1])).astype(BF16)
        for d in (1, 3, 2, 0):
            v = step_to(a1, d)
            if d == 0:
                local(Cs.at[cls, v], Cr.at[cls, pos[a1]], cr.at[cls, d]).start()
            else:
                remote(Cs.at[cls, v], Cr.at[cls, pos[a1]], cs.at[cls, d], cr.at[cls, d], me + moved(a1, v)).start()

    for c in weight_copies[:3]:
        c.wait()
    ff_shared = s1.shape[1]
    step = 512
    acc = jnp.zeros((tokens, x_ref.shape[1]), F32)
    for f in range(0, ff_shared, step):
        xs = x_ref[...]
        mid = (jax.nn.silu(dot(xs, s1[:, f:f + step])) * dot(xs, s3[:, f:f + step])).astype(BF16)
        acc = acc + dot(mid, s2[f:f + step, :])
    zs[...] = acc

    rows = CAP * 8
    qi, qj = iota((rows, 256), 0), iota((rows, 256), 1)
    by_rank = [as_onehot(qj == (qi % 8 + 8 * h) * 16 + qi // 8) for h in range(2)]
    src_base = ((iota((rows, 128), 0) % 8) * tokens).astype(F32)
    lane = iota((rows, 128), 1).astype(F32)
    tabs, lines = [], []
    for cls, (a1, a2, a3) in enumerate(CLASSES):
        for k in range(RING):
            here = (cls, pos[a2], pos[a1])
            for d in (1, 3, 2):
                local(tab, T.at[here], t2r.at[cls, k, d]).wait()
                local(cols(cls), G.at[here], g2r.at[cls, k, d]).wait()
        local(tab, T.at[here], t1r.at[cls, 0]).wait()
        local(cols(cls), G.at[here], g1r.at[cls, 0]).wait()
        tabs.append([dot(m, T[cls].reshape(256, slots)).astype(BF16) for m in by_rank])
        lines.append(me - core - pos[a3] * STRIDE[a3])

    def select(i, _):
        e, p = i // 2, i % 2
        for cls, (a1, a2, a3) in enumerate(CLASSES):
            picks = []
            for q in range(2):
                d = 2 + q - p * (1 + 2 * q)
                slot = lines[cls] + step_to(a3, d) * STRIDE[a3] + (core + e) % 2
                picks.append(as_onehot(iota((slots, 128), 0) == slot))
            outs = []
            for h in range(2):
                for q in range(2):
                    val = dot(tabs[cls][h], picks[q])
                    code = jnp.where(val > 0.5, val - 1.0 + src_base, -1.0)
                    for b in range(8 * tokens // 128):
                        Pm[cls, h, q * rows:(q + 1) * rows, b * 128:(b + 1) * 128] = (
                            jnp.where(code == lane + float(b * 128), 1.0, 0.0))
                out = dot(Pm[cls, h].astype(BF16), G[cls, 2 * h:2 * h + 2].reshape(8 * tokens, third))
                outs.append(out.reshape(2, CAP, 8, third))
            both = jnp.concatenate(outs, axis=2).astype(BF16)
            for q in range(2):
                d = 2 + q - p * (1 + 2 * q)
                k = 2 * d + e
                Sb[cls, k] = both[q]
                dev = me + moved(a3, step_to(a3, d)) + (core + e) % 2 - core
                src, dst = Sb.at[cls, k], R.at[cls, pl.ds(core * CAP, CAP), pos[a3]]
                if q == 1:
                    @pl.when(i == 1)
                    def _():
                        local(src, dst, d3r.at[cls, k]).start()

                    @pl.when(i != 1)
                    def _():
                        remote(src, dst, d3s.at[cls, k], d3r.at[cls, k], dev).start()
                else:
                    remote(src, dst, d3s.at[cls, k], d3r.at[cls, k], dev).start()
        return 0

    lax.fori_loop(0, RING, select, 0)

    for c in weight_copies[3:]:
        c.wait()
    blk = 3 * 64
    pi, pj = iota((blk, blk), 0), iota((blk, blk), 1)

    def bits(v):
        return v // 16 % 4, v // 4 % 4, v % 4

    ix, iz, iy = bits(pi)
    jx, jz, jy = bits(pj)
    to_first = {1: as_onehot(pj == pi // 64 * 64 + iy * 16 + ix * 4 + iz),
                2: as_onehot(pj == pi // 64 * 64 + iz * 16 + iy * 4 + ix)}
    from_first = {1: as_onehot(pi == pj // 64 * 64 + jy * 16 + jx * 4 + jz),
                  2: as_onehot(pi == pj // 64 * 64 + jz * 16 + jy * 4 + jx)}

    def permuted(mats, cls, value):
        if cls == 0:
            return value
        return jnp.concatenate([dot(mats[cls], value[i:i + blk]).astype(BF16)
                                for i in range(0, value.shape[0], blk)], axis=0)

    def expert(e, _):
        half = (core + e) % 2
        for cls in range(3):
            for d in range(RING):
                local(Sb.at[cls, 0], Sb.at[cls, 0], d3r.at[cls, 2 * d + e]).wait()
        n = CAP * 64
        xs = jnp.concatenate([permuted(to_first, cls, R[cls, pl.ds(half * CAP, CAP)].reshape(n, third))
                              for cls in range(3)], axis=1)
        mid = (jax.nn.silu(dot(xs, w1[...])) * dot(xs, w3[...])).astype(BF16)
        for cls, (a1, a2, a3) in enumerate(CLASSES):
            out = dot(mid, w2[:, cls * third:(cls + 1) * third]).astype(BF16)
            Ob[cls, pl.ds(half * CAP, CAP)] = permuted(from_first, cls, out).reshape(CAP, RING, 16, third)
            for d in (2, 1, 3, 0):
                v = step_to(a3, d)
                k = 2 * d + e
                dev = me + moved(a3, v) + half - core
                src, dst = Ob.at[cls, pl.ds(half * CAP, CAP), v], Hb.at[cls, core, :, pos[a3]]
                if d == 0:
                    @pl.when(e == 0)
                    def _():
                        local(src, dst, d5r.at[cls, k]).start()

                    @pl.when(e != 0)
                    def _():
                        remote(src, dst, d5s.at[cls, k], d5r.at[cls, k], dev).start()
                else:
                    remote(src, dst, d5s.at[cls, k], d5r.at[cls, k], dev).start()
        return 0

    lax.fori_loop(0, 2, expert, 0)

    u2, v3 = pi // 16 % 4, pi // 4 % 4
    by_second = as_onehot(pj == pi // 64 * 64 + v3 * 16 + u2 * 4 + pi % 4)

    def regroup(e, _):
        half = (core + e) % 2
        for cls, (a1, a2, a3) in enumerate(CLASSES):
            for d in range(RING):
                local(Sb.at[cls, 0], Sb.at[cls, 0], d5r.at[cls, 2 * d + e]).wait()
            rows_in = Hb[cls, half].reshape(CAP * 64, third)
            Z[cls, half] = jnp.concatenate([dot(by_second, rows_in[i:i + blk]).astype(BF16) for i in
                                            range(0, CAP * 64, blk)], axis=0).reshape(CAP, RING, 16, third)
            for d in (2, 1, 3, 0):
                v = step_to(a2, d)
                src, dst = Z.at[cls, half, :, v], F.at[cls, :, pos[a2], half]
                if d == 0:
                    local(src, dst, d6r.at[cls, e, d]).start()
                else:
                    remote(src, dst, d6s.at[cls, e, d], d6r.at[cls, e, d], me + moved(a2, v)).start()
        return 0

    lax.fori_loop(0, 2, regroup, 0)

    all_tok = RING * tokens
    ei, ej = iota((128, 128), 0), iota((128, 128), 1)
    spreads = [as_onehot(ei == ej // 4 + 32 * part) for part in range(4)]
    same = iota((all_tok, 128), 0) // tokens == iota((all_tok, 128), 1) % 4
    for cls, (a1, a2, a3) in enumerate(CLASSES):
        for d in range(RING):
            local(Cs.at[cls, 0], Cr.at[cls, 0], cr.at[cls, d]).wait()
        c_all = Cr[cls].reshape(all_tok, 128)
        w_exp = [dot(c_all, spreads[part]) for part in range(3)]
        rank_exp = jnp.where(same, dot(c_all, spreads[3]), 99.0)
        for e in range(2):
            for d in range(RING):
                local(Sb.at[cls, 0], Sb.at[cls, 0], d6r.at[cls, e, d]).wait()
        acc = jnp.zeros((3 * all_tok, third), F32)
        for r0 in range(0, CAP, 2):
            ranks = range(r0, min(r0 + 2, CAP))
            w = jnp.concatenate([jnp.concatenate([jnp.where(rank_exp == float(r), w_exp[part], 0.0) for r in ranks], axis=1)
                                 for part in range(3)], axis=0).astype(BF16)
            acc = acc + dot(w, F[cls, r0:r0 + len(ranks)].reshape(128 * len(ranks), third))
        U[cls] = (acc[2 * all_tok:] + acc[all_tok:2 * all_tok] + acc[:all_tok]).reshape(RING, tokens, third)
        for d in (2, 1, 3, 0):
            v = step_to(a1, d)
            if d == 0:
                local(U.at[cls, v], A.at[cls, pos[a1]], d7r.at[cls, d]).start()
            else:
                remote(U.at[cls, v], A.at[cls, pos[a1]], d7s.at[cls, d], d7r.at[cls, d], me + moved(a1, v)).start()
    for cls in range(3):
        for d in range(RING):
            local(U.at[cls, 0], A.at[cls, 0], d7r.at[cls, d]).wait()
        routed = (A[cls, 0] + A[cls, 1]) + (A[cls, 2] + A[cls, 3])
        y_ref[:, cls * third:(cls + 1) * third] = (zs[:, cls * third:(cls + 1) * third] + routed).astype(BF16)

    for cls, (a1, a2, a3) in enumerate(CLASSES):
        here = (cls, pos[a2], pos[a1])
        for d in range(1, RING):
            local(tab, T.at[here], t1s.at[cls, d]).wait()
            local(cols(cls), G.at[here], g1s.at[cls, d]).wait()
            local(Cs.at[cls, 0], Cr.at[cls, 0], cs.at[cls, d]).wait()
            for k in range(RING):
                local(tab, T.at[here], t2s.at[cls, k, d]).wait()
                local(cols(cls), G.at[here], g2s.at[cls, k, d]).wait()
        for k in range(1, 8):
            local(Sb.at[cls, 0], Sb.at[cls, 0], d3s.at[cls, k]).wait()
            local(Sb.at[cls, 0], Sb.at[cls, 0], d5s.at[cls, k]).wait()
        for d in range(1, RING):
            local(U.at[cls, 0], A.at[cls, 0], d7s.at[cls, d]).wait()
            for e in range(2):
                local(Sb.at[cls, 0], Sb.at[cls, 0], d6s.at[cls, e, d]).wait()


def solution(mesh):
    def device_step(x_tokens, slot_expert, w1_slots, w3_slots, w2_slots, assign, w_router, w1_shared, w3_shared, w2_shared):
        tokens, dim = x_tokens.shape
        third = dim // 3
        slots = slot_expert.shape[0]
        vmem = pl.BlockSpec(memory_space=pltpu.VMEM)
        hbm = pl.BlockSpec(memory_space=pl.ANY)
        dma = pltpu.SemaphoreType.DMA
        V = pltpu.VMEM
        return pl.pallas_call(
            moe_kernel,
            out_shape=jax.ShapeDtypeStruct((tokens, dim), BF16),
            in_specs=[vmem] * 4 + [hbm] * 6,
            out_specs=vmem,
            scratch_shapes=[
                V((3, RING, RING, tokens, third), BF16),
                V((3, RING, RING, 16, slots), BF16),
                V((16, slots), BF16),
                V((3, 2, 2 * CAP * 8, 8 * tokens), F32),
                V((3, 8, CAP, 16, third), BF16),
                V((3, 2 * CAP, RING, 16, third), BF16),
                V((3, 2 * CAP, RING, 16, third), BF16),
                V((3, 2, CAP, RING, 16, third), BF16),
                V((3, 2, CAP, RING, 16, third), BF16),
                V((3, CAP, RING, 2, 16, third), BF16),
                V((3, RING, tokens, 128), BF16), V((3, RING, tokens, 128), BF16),
                V((3, RING, tokens, third), F32), V((3, RING, tokens, third), F32),
                V((tokens, dim), F32),
                V(w1_slots.shape[1:], BF16), V(w3_slots.shape[1:], BF16), V(w2_slots.shape[1:], BF16),
                V(w1_shared.shape, BF16), V(w3_shared.shape, BF16), V(w2_shared.shape, BF16),
                dma((6,)),
                dma((3, 4)), dma((3, 4)), dma((3, 4, 4)), dma((3, 4, 4)),
                dma((3, 4)), dma((3, 4)), dma((3, 4, 4)), dma((3, 4, 4)),
                dma((3, 4)), dma((3, 4)),
                dma((3, 8)), dma((3, 8)), dma((3, 8)), dma((3, 8)),
                dma((3, 2, 4)), dma((3, 2, 4)), dma((3, 4)), dma((3, 4)),
            ],
            compiler_params=pltpu.CompilerParams(collective_id=0, has_side_effects=True,
                                                 vmem_limit_bytes=60 * 2 ** 20),
        )(x_tokens, assign.T, slot_expert.reshape(1, -1), w_router.T, w1_slots, w3_slots, w2_slots,
          w1_shared, w3_shared, w2_shared)

    token_spec = P(('dp', 'ep'), None)
    slot_spec = P('ep', None, None)
    return jax.shard_map(device_step, mesh=mesh,
                         in_specs=(token_spec, P(), slot_spec, slot_spec, slot_spec, token_spec, P(), P(), P(), P()),
                         out_specs=token_spec, check_vma=False)
```

```python
import jax
import jax.numpy as jnp
from jax import lax
from jax.experimental import pallas as pl
from jax.experimental.pallas import tpu as pltpu
from jax.sharding import PartitionSpec as P

ROUTE_SCALE = 2.5
RING = 4
CAP = 9
BF16 = jnp.bfloat16
F32 = jnp.float32
STRIDE = {'x': 2, 'y': 8, 'z': 32}
CLASSES = (('y', 'z', 'x'), ('z', 'x', 'y'), ('x', 'y', 'z'))


def iota(shape, dim):
    return lax.broadcasted_iota(jnp.int32, shape, dim)


def dot(a, b):
    return jnp.dot(a, b, preferred_element_type=F32)


def dot_t(a, b):
    return lax.dot_general(a, b, (((1,), (1,)), ((), ())), preferred_element_type=F32)


def as_onehot(cond):
    return jnp.where(cond, 1.0, 0.0).astype(BF16)


def three_parts(v):
    hi = v.astype(BF16)
    rest = v - hi.astype(F32)
    mid = rest.astype(BF16)
    lo = (rest - mid.astype(F32)).astype(BF16)
    return hi, mid, lo


def moe_kernel(x_hbm, assign_hbm, slot_expert_hbm, wr_hbm, w1_hbm, w3_hbm, w2_hbm, s1_hbm, s3_hbm, s2_hbm, y_ref,
               x_ref, assign_ref, slot_expert_ref, wr_ref,
               G, T, tab, Pm, Sb, R, Ob, Hb, Z, F, Cs, Cr, U, A, zs, w1, w3, w2, s1, s3, s2,
               wsem, isem, g1s, g1r, g2s, g2r, t1s, t1r, t2s, t2r, cs, cr, d3s, d3r, d5s, d5r, d6s, d6r, d7s, d7r):
    me = lax.axis_index('ep')
    core = me % 2
    pos = {'x': (me // 2) % RING, 'y': (me // 8) % RING, 'z': me // 32}
    third = x_ref.shape[1] // 3
    sixth = third // 2

    def moved(axis, value):
        return (value - pos[axis]) * STRIDE[axis]

    def step_to(axis, d):
        return (pos[axis] + d) % RING

    def remote(src, dst, ssem, rsem, dev):
        return pltpu.make_async_remote_copy(src_ref=src, dst_ref=dst, send_sem=ssem, recv_sem=rsem,
                                            device_id={'ep': dev}, device_id_type=pl.DeviceIdType.MESH)

    def local(src, dst, sem):
        return pltpu.make_async_copy(src, dst, sem)

    barrier = pltpu.get_barrier_semaphore()

    def greet(dev):
        pl.semaphore_signal(barrier, inc=1, device_id={'ep': dev}, device_id_type=pl.DeviceIdType.MESH)

    other = 1 - 2 * core
    greet(me + other)
    for axis in 'xyz':
        for d in range(1, RING):
            dev = me + moved(axis, step_to(axis, d))
            greet(dev)
            greet(dev + other)

    input_copies = [local(s, d, isem.at[i]) for i, (s, d) in enumerate(
        ((assign_hbm, assign_ref), (x_hbm, x_ref), (slot_expert_hbm, slot_expert_ref), (wr_hbm, wr_ref)))]
    for c in input_copies:
        c.start()
    weight_copies = [pltpu.make_async_copy(s, d, wsem.at[i]) for i, (s, d) in enumerate(
        ((s1_hbm, s1), (s3_hbm, s3), (s2_hbm, s2), (w1_hbm.at[0], w1), (w3_hbm.at[0], w3), (w2_hbm.at[0], w2)))]
    for c in weight_copies:
        c.start()

    input_copies[0].wait()
    tokens = x_ref.shape[0]
    slots = slot_expert_ref.shape[1]
    slot_row = iota((slots, tokens), 0)
    chosen_t = jnp.zeros((slots, tokens), F32)
    for k in range(assign_ref.shape[0]):
        chosen_t = chosen_t + jnp.where(assign_ref[k:k + 1, :] == slot_row, 1.0, 0.0)
    ti, tj = iota((tokens, tokens), 0), iota((tokens, tokens), 1)
    chosen = dot_t(as_onehot(ti == tj), chosen_t.astype(BF16))
    rank = jnp.where(chosen > 0.5, dot(as_onehot(tj < ti), chosen.astype(BF16)), 99.0)
    token_id = (iota((tokens, slots), 0) + 1).astype(F32)
    tab_rows = [jnp.sum(jnp.where(rank == float(r), token_id, 0.0), axis=0, keepdims=True) for r in range(CAP)]
    tab[...] = jnp.concatenate(tab_rows + [jnp.zeros((16 - CAP, slots), F32)], axis=0).astype(BF16)

    for c in input_copies[1:]:
        c.wait()
    pl.semaphore_wait(barrier, 19)

    def cols(cls, g):
        return x_ref.at[:, pl.ds((2 * cls + g) * sixth, sixth)]

    def spread(cls, g, k, src, to):
        a2 = CLASSES[cls][1]
        for d in (1, 3, 2):
            remote(src, G.at[cls, g, pos[a2], to], g2s.at[cls, g, k, d], g2r.at[cls, g, k, d],
                   me + moved(a2, step_to(a2, d))).start()

    for g in range(2):
        for cls, (a1, a2, a3) in enumerate(CLASSES):
            for d in (1, 3, 2):
                dev = me + moved(a1, step_to(a1, d))
                if g == 0:
                    remote(tab, T.at[cls, pos[a2], pos[a1]], t1s.at[cls, d], t1r.at[cls, d], dev).start()
                remote(cols(cls, g), G.at[cls, g, pos[a2], pos[a1]], g1s.at[cls, g, d], g1r.at[cls, g, d], dev).start()
        for cls, (a1, a2, a3) in enumerate(CLASSES):
            spread(cls, g, 0, cols(cls, g), pos[a1])
            local(cols(cls, g), G.at[cls, g, pos[a2], pos[a1]], g1r.at[cls, g, 0]).start()
            if g == 0:
                local(tab, T.at[cls, pos[a2], pos[a1]], t1r.at[cls, 0]).start()

    gate = jax.nn.sigmoid(dot_t(x_ref[...], wr_ref[...]))
    num_experts = wr_ref.shape[0]
    slot_of = as_onehot(iota((num_experts, slots), 0) == slot_expert_ref[...])
    gate_slot = sum(dot(p, slot_of) for p in three_parts(gate))
    picked = jnp.where(chosen > 0.5, gate_slot, 0.0)
    route = ROUTE_SCALE * picked / jnp.maximum(jnp.sum(picked, axis=1, keepdims=True), 1e-30)
    route_rank = jnp.concatenate(three_parts(route) + (rank.astype(BF16),), axis=1)

    for g in range(2):
        for d in (3, 1, 2):
            for cls, (a1, a2, a3) in enumerate(CLASSES):
                owner = (pos[a1] + RING - d) % RING
                src = G.at[cls, g, pos[a2], owner]
                local(cols(cls, g), src, g1r.at[cls, g, d]).wait()
                spread(cls, g, d, src, owner)
        if g == 0:
            for cls, (a1, a2, a3) in enumerate(CLASSES):
                for d in range(RING):
                    local(tab, T.at[cls, 0, 0], t1r.at[cls, d]).wait()
                row = T.at[cls, pos[a2]]
                for d in (1, 3, 2):
                    remote(row, row, t2s.at[cls, d], t2r.at[cls, d], me + moved(a2, step_to(a2, d))).start()

    si, sj = iota((4 * slots, 128), 0), iota((4 * slots, 128), 1)
    for cls, (a1, a2, a3) in enumerate(CLASSES):
        q_slot = (sj // 32 * slots + sj // 8 % 4 * STRIDE[a2] + sj // 4 % 2 + sj % 4 * STRIDE[a3])
        for v in range(RING):
            Cs[cls, v] = dot(route_rank, as_onehot(si == q_slot + v * STRIDE[a1])).astype(BF16)
        for d in (1, 3, 2, 0):
            v = step_to(a1, d)
            if d == 0:
                local(Cs.at[cls, v], Cr.at[cls, pos[a1]], cr.at[cls, d]).start()
            else:
                remote(Cs.at[cls, v], Cr.at[cls, pos[a1]], cs.at[cls, d], cr.at[cls, d], me + moved(a1, v)).start()

    for c in weight_copies[:3]:
        c.wait()
    ff_shared = s1.shape[1]
    step = 512
    acc = jnp.zeros((tokens, x_ref.shape[1]), F32)
    for f in range(0, ff_shared, step):
        xs = x_ref[...]
        mid = (jax.nn.silu(dot(xs, s1[:, f:f + step])) * dot(xs, s3[:, f:f + step])).astype(BF16)
        acc = acc + dot(mid, s2[f:f + step, :])
    zs[...] = acc

    rows = CAP * 8
    qi, qj = iota((rows, 256), 0), iota((rows, 256), 1)
    by_rank = [as_onehot(qj == (qi % 8 + 8 * h) * 16 + qi // 8) for h in range(2)]
    src_base = ((iota((rows, 128), 0) % 8) * tokens).astype(F32)
    lane = iota((rows, 128), 1).astype(F32)
    tabs, lines = [], []

    def gathered(g):
        for cls in range(3):
            for k in range(RING):
                for d in (1, 3, 2):
                    local(cols(cls, g), G.at[cls, g, 0, 0], g2r.at[cls, g, k, d]).wait()
            local(cols(cls, g), G.at[cls, g, 0, 0], g1r.at[cls, g, 0]).wait()

    gathered(0)
    for cls, (a1, a2, a3) in enumerate(CLASSES):
        for d in (1, 3, 2):
            local(T.at[cls, 0], T.at[cls, 0], t2r.at[cls, d]).wait()
        tabs.append([dot(m, T[cls].reshape(256, slots)).astype(BF16) for m in by_rank])
        lines.append(me - core - pos[a3] * STRIDE[a3])

    def select(n, _):
        g, e, p = n // 2 % 2, n // 4, n % 2

        @pl.when(n == 2)
        def _():
            gathered(1)

        for cls, (a1, a2, a3) in enumerate(CLASSES):
            picks = []
            for q in range(2):
                d = 2 + q - p * (1 + 2 * q)
                slot = lines[cls] + step_to(a3, d) * STRIDE[a3] + (core + e) % 2
                picks.append(as_onehot(iota((slots, 128), 0) == slot))
            outs = []
            for h in range(2):
                for q in range(2):
                    val = dot(tabs[cls][h], picks[q])
                    code = jnp.where(val > 0.5, val - 1.0 + src_base, -1.0)
                    for b in range(8 * tokens // 128):
                        Pm[cls, h, q * rows:(q + 1) * rows, b * 128:(b + 1) * 128] = (
                            jnp.where(code == lane + float(b * 128), 1.0, 0.0))
                out = dot(Pm[cls, h].astype(BF16), G[cls, g, 2 * h:2 * h + 2].reshape(8 * tokens, sixth))
                outs.append(out.reshape(2, CAP, 8, sixth))
            both = jnp.concatenate(outs, axis=2).astype(BF16)
            for q in range(2):
                d = 2 + q - p * (1 + 2 * q)
                k = 2 * d + e
                Sb[cls, g, k] = both[q]
                dev = me + moved(a3, step_to(a3, d)) + (core + e) % 2 - core
                src, dst = Sb.at[cls, g, k], R.at[cls, g, pl.ds(core * CAP, CAP), pos[a3]]
                if q == 1:
                    mine = jnp.logical_and(n < 4, n % 2 == 1)

                    @pl.when(mine)
                    def _():
                        local(src, dst, d3r.at[cls, g, k]).start()

                    @pl.when(jnp.logical_not(mine))
                    def _():
                        remote(src, dst, d3s.at[cls, g, k], d3r.at[cls, g, k], dev).start()
                else:
                    remote(src, dst, d3s.at[cls, g, k], d3r.at[cls, g, k], dev).start()
        return 0

    lax.fori_loop(0, 2 * RING, select, 0)

    for c in weight_copies[3:]:
        c.wait()
    blk = 3 * 64
    pi, pj = iota((blk, blk), 0), iota((blk, blk), 1)

    def bits(v):
        return v // 16 % 4, v // 4 % 4, v % 4

    ix, iz, iy = bits(pi)
    jx, jz, jy = bits(pj)
    to_first = {1: as_onehot(pj == pi // 64 * 64 + iy * 16 + ix * 4 + iz),
                2: as_onehot(pj == pi // 64 * 64 + iz * 16 + iy * 4 + ix)}
    from_first = {1: as_onehot(pi == pj // 64 * 64 + jy * 16 + jx * 4 + jz),
                  2: as_onehot(pi == pj // 64 * 64 + jz * 16 + jy * 4 + jx)}

    def permuted(mats, cls, value):
        if cls == 0:
            return value
        return jnp.concatenate([dot(mats[cls], value[i:i + blk]).astype(BF16)
                                for i in range(0, value.shape[0], blk)], axis=0)

    def expert(e, _):
        half = (core + e) % 2
        for cls in range(3):
            for d in range(RING):
                for g in range(2):
                    local(Sb.at[cls, g, 0], Sb.at[cls, g, 0], d3r.at[cls, g, 2 * d + e]).wait()
        n = CAP * 64
        xs = jnp.concatenate([permuted(to_first, cls, R[cls, g, pl.ds(half * CAP, CAP)].reshape(n, sixth))
                              for cls in range(3) for g in range(2)], axis=1)
        mid = (jax.nn.silu(dot(xs, w1[...])) * dot(xs, w3[...])).astype(BF16)
        for cls, (a1, a2, a3) in enumerate(CLASSES):
            out = dot(mid, w2[:, cls * third:(cls + 1) * third]).astype(BF16)
            Ob[cls, pl.ds(half * CAP, CAP)] = permuted(from_first, cls, out).reshape(CAP, RING, 16, third)
            for d in (2, 1, 3, 0):
                v = step_to(a3, d)
                k = 2 * d + e
                dev = me + moved(a3, v) + half - core
                src, dst = Ob.at[cls, pl.ds(half * CAP, CAP), v], Hb.at[cls, core, :, pos[a3]]
                if d == 0:
                    @pl.when(e == 0)
                    def _():
                        local(src, dst, d5r.at[cls, k]).start()

                    @pl.when(e != 0)
                    def _():
                        remote(src, dst, d5s.at[cls, k], d5r.at[cls, k], dev).start()
                else:
                    remote(src, dst, d5s.at[cls, k], d5r.at[cls, k], dev).start()
        return 0

    lax.fori_loop(0, 2, expert, 0)
    piece = Z.at[0, 0, :, 0]

    u2, v3 = pi // 16 % 4, pi // 4 % 4
    by_second = as_onehot(pj == pi // 64 * 64 + v3 * 16 + u2 * 4 + pi % 4)

    def regroup(e, _):
        half = (core + e) % 2
        for cls, (a1, a2, a3) in enumerate(CLASSES):
            for d in range(RING):
                local(piece, piece, d5r.at[cls, 2 * d + e]).wait()
            rows_in = Hb[cls, half].reshape(CAP * 64, third)
            Z[cls, half] = jnp.concatenate([dot(by_second, rows_in[i:i + blk]).astype(BF16) for i in
                                            range(0, CAP * 64, blk)], axis=0).reshape(CAP, RING, 16, third)
            for d in (2, 1, 3, 0):
                v = step_to(a2, d)
                src, dst = Z.at[cls, half, :, v], F.at[cls, half, :, pos[a2]]
                if d == 0:
                    local(src, dst, d6r.at[cls, e, d]).start()
                else:
                    remote(src, dst, d6s.at[cls, e, d], d6r.at[cls, e, d], me + moved(a2, v)).start()
        return 0

    lax.fori_loop(0, 2, regroup, 0)

    for cls in range(3):
        for d in range(RING):
            local(Cs.at[cls, 0], Cr.at[cls, 0], cr.at[cls, d]).wait()

    def spreads(half):
        ei, ej = iota((128, 256), 0), iota((128, 256), 1)
        q = ej // 16 % 4 * 8 + half * 4 + ej // 4 % 4
        return [as_onehot(ei == q + 32 * part) for part in range(4)]

    def weigh(cls, half, spread_mats, targets):
        m = tokens * len(targets)
        lane_pos = iota((m, 256), 1)
        c = jnp.concatenate([Cr[cls, v] for v in targets], axis=0)
        w_exp = [dot(c, spread_mats[part]) for part in range(3)]
        source = jnp.concatenate([jnp.full((tokens, 256), v, jnp.int32) for v in targets], axis=0)
        rank_exp = jnp.where(lane_pos % 4 == source, dot(c, spread_mats[3]) - (lane_pos // 64).astype(F32), 99.0)
        acc = jnp.zeros((3 * m, third), F32)
        for r0 in range(0, CAP, 4):
            k = 64 * min(4, CAP - r0)
            hit = rank_exp == float(r0)
            w = jnp.concatenate([jnp.where(hit, w_exp[part], 0.0) for part in range(3)], axis=0).astype(BF16)
            acc = acc + dot(w[:, :k], F[cls, half, r0:r0 + k // 64].reshape(k, third))
        return (acc[2 * m:] + acc[m:2 * m] + acc[:m]).reshape(len(targets), tokens, third)

    def arrived(cls, e):
        for d in range(RING):
            local(piece, piece, d6r.at[cls, e, d]).wait()

    mats = spreads(core)
    for cls in range(3):
        arrived(cls, 0)
        U[cls] = weigh(cls, core, mats, list(range(RING)))
    mats = spreads(1 - core)
    for group in ((2,), (1, 3), (0,)):
        for cls, (a1, a2, a3) in enumerate(CLASSES):
            if group == (2,):
                arrived(cls, 1)
            targets = [step_to(a1, d) for d in group]
            part = weigh(cls, 1 - core, mats, targets)
            for i, (d, v) in enumerate(zip(group, targets)):
                if d == 0:
                    A[cls, pos[a1]] = U[cls, v] + part[i]
                else:
                    U[cls, v] = U[cls, v] + part[i]
                    remote(U.at[cls, v], A.at[cls, pos[a1]], d7s.at[cls, d], d7r.at[cls, d], me + moved(a1, v)).start()
    for cls in range(3):
        for d in range(1, RING):
            local(U.at[cls, 0], A.at[cls, 0], d7r.at[cls, d]).wait()
        routed = (A[cls, 0] + A[cls, 1]) + (A[cls, 2] + A[cls, 3])
        y_ref[:, cls * third:(cls + 1) * third] = (zs[:, cls * third:(cls + 1) * third] + routed).astype(BF16)

    for cls in range(3):
        for d in range(1, RING):
            local(tab, T.at[cls, 0, 0], t1s.at[cls, d]).wait()
            local(T.at[cls, 0], T.at[cls, 0], t2s.at[cls, d]).wait()
            local(Cs.at[cls, 0], Cr.at[cls, 0], cs.at[cls, d]).wait()
            for g in range(2):
                local(cols(cls, g), G.at[cls, g, 0, 0], g1s.at[cls, g, d]).wait()
                for k in range(RING):
                    local(cols(cls, g), G.at[cls, g, 0, 0], g2s.at[cls, g, k, d]).wait()
        for k in range(1, 8):
            for g in range(2):
                local(Sb.at[cls, g, 0], Sb.at[cls, g, 0], d3s.at[cls, g, k]).wait()
            local(piece, piece, d5s.at[cls, k]).wait()
        for d in range(1, RING):
            local(U.at[cls, 0], A.at[cls, 0], d7s.at[cls, d]).wait()
            for e in range(2):
                local(piece, piece, d6s.at[cls, e, d]).wait()


def solution(mesh):
    def device_step(x_tokens, slot_expert, w1_slots, w3_slots, w2_slots, assign, w_router, w1_shared, w3_shared, w2_shared):
        tokens, dim = x_tokens.shape
        third = dim // 3
        slots = slot_expert.shape[0]
        vmem = pl.BlockSpec(memory_space=pltpu.VMEM)
        hbm = pl.BlockSpec(memory_space=pl.ANY)
        dma = pltpu.SemaphoreType.DMA
        V = pltpu.VMEM
        return pl.pallas_call(
            moe_kernel,
            out_shape=jax.ShapeDtypeStruct((tokens, dim), BF16),
            in_specs=[hbm] * 10,
            out_specs=vmem,
            scratch_shapes=[
                V((tokens, dim), BF16), V(assign.T.shape, jnp.int32), V((1, slots), jnp.int32), V(w_router.T.shape, BF16),
                V((3, 2, RING, RING, tokens, third // 2), BF16),
                V((3, RING, RING, 16, slots), BF16),
                V((16, slots), BF16),
                V((3, 2, 2 * CAP * 8, 8 * tokens), F32),
                V((3, 2, 8, CAP, 16, third // 2), BF16),
                V((3, 2, 2 * CAP, RING, 16, third // 2), BF16),
                V((3, 2 * CAP, RING, 16, third), BF16),
                V((3, 2, CAP, RING, 16, third), BF16),
                V((3, 2, CAP, RING, 16, third), BF16),
                V((3, 2, CAP, RING, 16, third), BF16),
                V((3, RING, tokens, 128), BF16), V((3, RING, tokens, 128), BF16),
                V((3, RING, tokens, third), F32), V((3, RING, tokens, third), F32),
                V((tokens, dim), F32),
                V(w1_slots.shape[1:], BF16), V(w3_slots.shape[1:], BF16), V(w2_slots.shape[1:], BF16),
                V(w1_shared.shape, BF16), V(w3_shared.shape, BF16), V(w2_shared.shape, BF16),
                dma((6,)), dma((4,)),
                dma((3, 2, 4)), dma((3, 2, 4)), dma((3, 2, 4, 4)), dma((3, 2, 4, 4)),
                dma((3, 4)), dma((3, 4)), dma((3, 4)), dma((3, 4)),
                dma((3, 4)), dma((3, 4)),
                dma((3, 2, 8)), dma((3, 2, 8)), dma((3, 8)), dma((3, 8)),
                dma((3, 2, 4)), dma((3, 2, 4)), dma((3, 4)), dma((3, 4)),
            ],
            compiler_params=pltpu.CompilerParams(collective_id=0, has_side_effects=True,
                                                 vmem_limit_bytes=60 * 2 ** 20),
        )(x_tokens, assign.T, slot_expert.reshape(1, -1), w_router.T, w1_slots, w3_slots, w2_slots,
          w1_shared, w3_shared, w2_shared)

    token_spec = P(('dp', 'ep'), None)
    slot_spec = P('ep', None, None)
    return jax.shard_map(device_step, mesh=mesh,
                         in_specs=(token_spec, P(), slot_spec, slot_spec, slot_spec, token_spec, P(), P(), P(), P()),
                         out_specs=token_spec, check_vma=False)
```

```python
import jax
import jax.numpy as jnp
from jax import lax
from jax.experimental import pallas as pl
from jax.experimental.pallas import tpu as pltpu
from jax.sharding import PartitionSpec as P

ROUTE_SCALE = 2.5
RING = 4
CAP = 9
BF16 = jnp.bfloat16
F32 = jnp.float32
STRIDE = {'x': 2, 'y': 8, 'z': 32}
CLASSES = (('y', 'z', 'x'), ('z', 'x', 'y'), ('x', 'y', 'z'))


def iota(shape, dim):
    return lax.broadcasted_iota(jnp.int32, shape, dim)


def dot(a, b):
    return jnp.dot(a, b, preferred_element_type=F32)


def dot_t(a, b):
    return lax.dot_general(a, b, (((1,), (1,)), ((), ())), preferred_element_type=F32)


def as_onehot(cond):
    return jnp.where(cond, 1.0, 0.0).astype(BF16)


def three_parts(v):
    hi = v.astype(BF16)
    rest = v - hi.astype(F32)
    mid = rest.astype(BF16)
    lo = (rest - mid.astype(F32)).astype(BF16)
    return hi, mid, lo


def moe_kernel(x_hbm, assign_hbm, slot_expert_hbm, wr_hbm, w1_hbm, w3_hbm, w2_hbm, s1_hbm, s3_hbm, s2_hbm, y_ref,
               x_ref, assign_ref, slot_expert_ref, wr_ref,
               G, T, tab, Pm, Sb, R, Ob, Hb, Z, F, Cs, Cr, U, A, zs, w1, w3, w2, s1, s3, s2,
               wsem, isem, sent, t1r, t2r, g0r, g1r, g2r, cr, d3r, d5r, d6r, d7r):
    t1s, t2s, g1s, g2s, cs, d3s, d5s, d6s, d7s = (sent.at[i] for i in range(9))
    me = lax.axis_index('ep')
    core = me % 2
    pos = {'x': (me // 2) % RING, 'y': (me // 8) % RING, 'z': me // 32}
    third = x_ref.shape[1] // 3
    sixth = third // 2

    def moved(axis, value):
        return (value - pos[axis]) * STRIDE[axis]

    def step_to(axis, d):
        return (pos[axis] + d) % RING

    def remote(src, dst, ssem, rsem, dev):
        return pltpu.make_async_remote_copy(src_ref=src, dst_ref=dst, send_sem=ssem, recv_sem=rsem,
                                            device_id={'ep': dev}, device_id_type=pl.DeviceIdType.MESH)

    def local(src, dst, sem):
        return pltpu.make_async_copy(src, dst, sem)

    def wait_bytes(ref, sem):
        pltpu.make_async_copy(ref, ref, sem).wait()

    barrier = pltpu.get_barrier_semaphore()

    def greet(dev):
        pl.semaphore_signal(barrier, inc=1, device_id={'ep': dev}, device_id_type=pl.DeviceIdType.MESH)

    other = 1 - 2 * core
    greet(me + other)
    for axis in 'xyz':
        for d in range(1, RING):
            dev = me + moved(axis, step_to(axis, d))
            greet(dev)
            greet(dev + other)

    input_copies = [local(s, d, isem.at[i]) for i, (s, d) in enumerate(
        ((assign_hbm, assign_ref), (x_hbm, x_ref), (slot_expert_hbm, slot_expert_ref), (wr_hbm, wr_ref)))]
    for c in input_copies:
        c.start()
    weight_copies = [pltpu.make_async_copy(s, d, wsem.at[i]) for i, (s, d) in enumerate(
        ((s1_hbm, s1), (s3_hbm, s3), (s2_hbm, s2), (w1_hbm.at[0], w1), (w3_hbm.at[0], w3), (w2_hbm.at[0], w2)))]
    for c in weight_copies:
        c.start()

    input_copies[0].wait()
    tokens = x_ref.shape[0]
    slots = slot_expert_ref.shape[1]
    slot_row = iota((slots, tokens), 0)
    chosen_t = jnp.zeros((slots, tokens), F32)
    for k in range(assign_ref.shape[0]):
        chosen_t = chosen_t + jnp.where(assign_ref[k:k + 1, :] == slot_row, 1.0, 0.0)
    ti, tj = iota((tokens, tokens), 0), iota((tokens, tokens), 1)
    chosen = dot_t(as_onehot(ti == tj), chosen_t.astype(BF16))
    rank = jnp.where(chosen > 0.5, dot(as_onehot(tj < ti), chosen.astype(BF16)), 99.0)
    token_id = (iota((tokens, slots), 0) + 1).astype(F32)
    tab_rows = [jnp.sum(jnp.where(rank == float(r), token_id, 0.0), axis=0, keepdims=True) for r in range(CAP)]
    tab[...] = jnp.concatenate(tab_rows + [jnp.zeros((16 - CAP, slots), F32)], axis=0).astype(BF16)

    for c in input_copies[1:]:
        c.wait()
    pl.semaphore_wait(barrier, 19)

    def cols(cls, g):
        return x_ref.at[:, pl.ds((2 * cls + g) * sixth, sixth)]

    def spread(cls, g, k, src, to):
        a2 = CLASSES[cls][1]
        for d in (1, 3, 2):
            remote(src, G.at[cls, g, pos[a2], to], g2s, g2r.at[g],
                   me + moved(a2, step_to(a2, d))).start()

    for g in range(2):
        for cls, (a1, a2, a3) in enumerate(CLASSES):
            for d in (1, 3, 2):
                dev = me + moved(a1, step_to(a1, d))
                if g == 0:
                    remote(tab, T.at[cls, pos[a2], pos[a1]], t1s, t1r.at[0], dev).start()
                remote(cols(cls, g), G.at[cls, g, pos[a2], pos[a1]], g1s, g1r.at[g, d - 1], dev).start()
        for cls, (a1, a2, a3) in enumerate(CLASSES):
            spread(cls, g, 0, cols(cls, g), pos[a1])
            local(cols(cls, g), G.at[cls, g, pos[a2], pos[a1]], g0r.at[0]).start()
            if g == 0:
                T[cls, pos[a2], pos[a1]] = tab[...]

    gate = jax.nn.sigmoid(dot_t(x_ref[...], wr_ref[...]))
    num_experts = wr_ref.shape[0]
    slot_of = as_onehot(iota((num_experts, slots), 0) == slot_expert_ref[...])
    gate_slot = sum(dot(p, slot_of) for p in three_parts(gate))
    picked = jnp.where(chosen > 0.5, gate_slot, 0.0)
    route = ROUTE_SCALE * picked / jnp.maximum(jnp.sum(picked, axis=1, keepdims=True), 1e-30)
    route_rank = jnp.concatenate(three_parts(route) + (rank.astype(BF16),), axis=1)

    for g in range(2):
        for d in (3, 1, 2):
            wait_bytes(G.at[:, g, 0, 0], g1r.at[g, d - 1])
            for cls, (a1, a2, a3) in enumerate(CLASSES):
                owner = (pos[a1] + RING - d) % RING
                spread(cls, g, d, G.at[cls, g, pos[a2], owner], owner)
        if g == 0:
            wait_bytes(T.at[:, 0, 0:3], t1r.at[0])
            for cls, (a1, a2, a3) in enumerate(CLASSES):
                row = T.at[cls, pos[a2]]
                for d in (1, 3, 2):
                    remote(row, row, t2s, t2r.at[0], me + moved(a2, step_to(a2, d))).start()

    si, sj = iota((4 * slots, 128), 0), iota((4 * slots, 128), 1)
    for cls, (a1, a2, a3) in enumerate(CLASSES):
        q_slot = (sj // 32 * slots + sj // 8 % 4 * STRIDE[a2] + sj // 4 % 2 + sj % 4 * STRIDE[a3])
        for v in range(RING):
            Cs[cls, v] = dot(route_rank, as_onehot(si == q_slot + v * STRIDE[a1])).astype(BF16)
        for d in (1, 3, 2, 0):
            v = step_to(a1, d)
            if d == 0:
                Cr[cls, pos[a1]] = Cs[cls, v]
            else:
                remote(Cs.at[cls, v], Cr.at[cls, pos[a1]], cs, cr.at[0], me + moved(a1, v)).start()

    for c in weight_copies[:3]:
        c.wait()
    ff_shared = s1.shape[1]
    step = 512
    acc = jnp.zeros((tokens, x_ref.shape[1]), F32)
    for f in range(0, ff_shared, step):
        xs = x_ref[...]
        mid = (jax.nn.silu(dot(xs, s1[:, f:f + step])) * dot(xs, s3[:, f:f + step])).astype(BF16)
        acc = acc + dot(mid, s2[f:f + step, :])
    zs[...] = acc

    rows = CAP * 8
    qi, qj = iota((rows, 256), 0), iota((rows, 256), 1)
    by_rank = [as_onehot(qj == (qi % 8 + 8 * h) * 16 + qi // 8) for h in range(2)]
    src_base = ((iota((rows, 128), 0) % 8) * tokens).astype(F32)
    lane = iota((rows, 128), 1).astype(F32)
    tabs, lines = [], []

    wait_bytes(G.at[:, :, 0, 0], g0r.at[0])
    wait_bytes(G.at[:, 0, 0:3], g2r.at[0])
    wait_bytes(T.at[:, 0:3], t2r.at[0])
    for cls, (a1, a2, a3) in enumerate(CLASSES):
        tabs.append([dot(m, T[cls].reshape(256, slots)).astype(BF16) for m in by_rank])
        lines.append(me - core - pos[a3] * STRIDE[a3])

    def select(n, _):
        g, e, p = n // 2 % 2, n // 4, n % 2

        @pl.when(n == 2)
        def _():
            wait_bytes(G.at[:, 1, 0:3], g2r.at[1])

        for cls, (a1, a2, a3) in enumerate(CLASSES):
            picks = []
            for q in range(2):
                d = 2 + q - p * (1 + 2 * q)
                slot = lines[cls] + step_to(a3, d) * STRIDE[a3] + (core + e) % 2
                picks.append(as_onehot(iota((slots, 128), 0) == slot))
            outs = []
            for h in range(2):
                for q in range(2):
                    val = dot(tabs[cls][h], picks[q])
                    code = jnp.where(val > 0.5, val - 1.0 + src_base, -1.0)
                    for b in range(8 * tokens // 128):
                        Pm[cls, h, q * rows:(q + 1) * rows, b * 128:(b + 1) * 128] = (
                            jnp.where(code == lane + float(b * 128), 1.0, 0.0))
                out = dot(Pm[cls, h].astype(BF16), G[cls, g, 2 * h:2 * h + 2].reshape(8 * tokens, sixth))
                outs.append(out.reshape(2, CAP, 8, sixth))
            both = jnp.concatenate(outs, axis=2).astype(BF16)
            for q in range(2):
                d = 2 + q - p * (1 + 2 * q)
                k = 2 * d + e
                Sb[cls, g, k] = both[q]
                dev = me + moved(a3, step_to(a3, d)) + (core + e) % 2 - core
                src, dst = Sb.at[cls, g, k], R.at[cls, g, pl.ds(core * CAP, CAP), pos[a3]]
                if q == 1:
                    mine = jnp.logical_and(n < 4, n % 2 == 1)

                    @pl.when(mine)
                    def _():
                        local(src, dst, d3r.at[e]).start()

                    @pl.when(jnp.logical_not(mine))
                    def _():
                        remote(src, dst, d3s, d3r.at[e], dev).start()
                else:
                    remote(src, dst, d3s, d3r.at[e], dev).start()
        return 0

    lax.fori_loop(0, 2 * RING, select, 0)

    for c in weight_copies[3:]:
        c.wait()
    blk = 3 * 64
    pi, pj = iota((blk, blk), 0), iota((blk, blk), 1)

    def bits(v):
        return v // 16 % 4, v // 4 % 4, v % 4

    ix, iz, iy = bits(pi)
    jx, jz, jy = bits(pj)
    to_first = {1: as_onehot(pj == pi // 64 * 64 + iy * 16 + ix * 4 + iz),
                2: as_onehot(pj == pi // 64 * 64 + iz * 16 + iy * 4 + ix)}
    from_first = {1: as_onehot(pi == pj // 64 * 64 + jy * 16 + jx * 4 + jz),
                  2: as_onehot(pi == pj // 64 * 64 + jz * 16 + jy * 4 + jx)}

    def permuted(mats, cls, value):
        if cls == 0:
            return value
        return jnp.concatenate([dot(mats[cls], value[i:i + blk]).astype(BF16)
                                for i in range(0, value.shape[0], blk)], axis=0)

    def expert(e, _):
        half = (core + e) % 2
        wait_bytes(R.at[:, :, 0:CAP], d3r.at[e])
        n = CAP * 64
        xs = jnp.concatenate([permuted(to_first, cls, R[cls, g, pl.ds(half * CAP, CAP)].reshape(n, sixth))
                              for cls in range(3) for g in range(2)], axis=1)
        mid = (jax.nn.silu(dot(xs, w1[...])) * dot(xs, w3[...])).astype(BF16)
        for cls, (a1, a2, a3) in enumerate(CLASSES):
            out = dot(mid, w2[:, cls * third:(cls + 1) * third]).astype(BF16)
            Ob[cls, pl.ds(half * CAP, CAP)] = permuted(from_first, cls, out).reshape(CAP, RING, 16, third)
            for d in (2, 1, 3, 0):
                v = step_to(a3, d)
                dev = me + moved(a3, v) + half - core
                src, dst = Ob.at[cls, pl.ds(half * CAP, CAP), v], Hb.at[cls, core, :, pos[a3]]
                if d == 0:
                    @pl.when(e == 0)
                    def _():
                        local(src, dst, d5r.at[e, cls]).start()

                    @pl.when(e != 0)
                    def _():
                        remote(src, dst, d5s, d5r.at[e, cls], dev).start()
                else:
                    remote(src, dst, d5s, d5r.at[e, cls], dev).start()
        return 0

    lax.fori_loop(0, 2, expert, 0)

    u2, v3 = pi // 16 % 4, pi // 4 % 4
    by_second = as_onehot(pj == pi // 64 * 64 + v3 * 16 + u2 * 4 + pi % 4)

    def regroup(e, _):
        half = (core + e) % 2
        for cls, (a1, a2, a3) in enumerate(CLASSES):
            wait_bytes(Hb.at[cls, half], d5r.at[e, cls])
            rows_in = Hb[cls, half].reshape(CAP * 64, third)
            Z[cls, half] = jnp.concatenate([dot(by_second, rows_in[i:i + blk]).astype(BF16) for i in
                                            range(0, CAP * 64, blk)], axis=0).reshape(CAP, RING, 16, third)
            for d in (2, 1, 3, 0):
                v = step_to(a2, d)
                src, dst = Z.at[cls, half, :, v], F.at[cls, half, :, pos[a2]]
                if d == 0:
                    local(src, dst, d6r.at[e, cls]).start()
                else:
                    remote(src, dst, d6s, d6r.at[e, cls], me + moved(a2, v)).start()
        return 0

    lax.fori_loop(0, 2, regroup, 0)

    wait_bytes(Cr.at[:, 0:3], cr.at[0])

    def spreads(half):
        ei, ej = iota((128, 256), 0), iota((128, 256), 1)
        q = ej // 16 % 4 * 8 + half * 4 + ej // 4 % 4
        return [as_onehot(ei == q + 32 * part) for part in range(4)]

    def weigh(cls, half, spread_mats, targets):
        m = tokens * len(targets)
        lane_pos = iota((m, 256), 1)
        c = jnp.concatenate([Cr[cls, v] for v in targets], axis=0)
        w_exp = [dot(c, spread_mats[part]) for part in range(3)]
        source = jnp.concatenate([jnp.full((tokens, 256), v, jnp.int32) for v in targets], axis=0)
        rank_exp = jnp.where(lane_pos % 4 == source, dot(c, spread_mats[3]) - (lane_pos // 64).astype(F32), 99.0)
        acc = jnp.zeros((3 * m, third), F32)
        for r0 in range(0, CAP, 4):
            k = 64 * min(4, CAP - r0)
            hit = rank_exp == float(r0)
            w = jnp.concatenate([jnp.where(hit, w_exp[part], 0.0) for part in range(3)], axis=0).astype(BF16)
            acc = acc + dot(w[:, :k], F[cls, half, r0:r0 + k // 64].reshape(k, third))
        return (acc[2 * m:] + acc[m:2 * m] + acc[:m]).reshape(len(targets), tokens, third)

    mats = spreads(core)
    for cls in range(3):
        wait_bytes(F.at[cls, core], d6r.at[0, cls])
        U[cls] = weigh(cls, core, mats, list(range(RING)))
    mats = spreads(1 - core)
    for group in ((2,), (1, 3), (0,)):
        for cls, (a1, a2, a3) in enumerate(CLASSES):
            if group == (2,):
                wait_bytes(F.at[cls, 1 - core], d6r.at[1, cls])
            targets = [step_to(a1, d) for d in group]
            part = weigh(cls, 1 - core, mats, targets)
            for i, (d, v) in enumerate(zip(group, targets)):
                if d == 0:
                    A[cls, pos[a1]] = U[cls, v] + part[i]
                else:
                    U[cls, v] = U[cls, v] + part[i]
                    remote(U.at[cls, v], A.at[cls, pos[a1]], d7s, d7r.at[cls], me + moved(a1, v)).start()
    for cls in range(3):
        wait_bytes(A.at[cls, 0:3], d7r.at[cls])
        routed = (A[cls, 0] + A[cls, 1]) + (A[cls, 2] + A[cls, 3])
        y_ref[:, cls * third:(cls + 1) * third] = (zs[:, cls * third:(cls + 1) * third] + routed).astype(BF16)

    for ref, sem in ((T.at[:, 0, 0:3], t1s), (T.at[:, 0:3], t2s), (G.at[:, :, 0, 0:3], g1s), (G.at[:, :, 0:3], g2s),
                     (Cs.at[:, 0:3], cs), (Sb.at[:, :, 0:7], d3s), (Sb.at[:, :, 0:7], d5s), (Z.at[:, :, :, 0:3], d6s),
                     (U.at[:, 0:3], d7s)):
        wait_bytes(ref, sem)


def solution(mesh):
    def device_step(x_tokens, slot_expert, w1_slots, w3_slots, w2_slots, assign, w_router, w1_shared, w3_shared, w2_shared):
        tokens, dim = x_tokens.shape
        third = dim // 3
        slots = slot_expert.shape[0]
        vmem = pl.BlockSpec(memory_space=pltpu.VMEM)
        hbm = pl.BlockSpec(memory_space=pl.ANY)
        dma = pltpu.SemaphoreType.DMA
        V = pltpu.VMEM
        return pl.pallas_call(
            moe_kernel,
            out_shape=jax.ShapeDtypeStruct((tokens, dim), BF16),
            in_specs=[hbm] * 10,
            out_specs=vmem,
            scratch_shapes=[
                V((tokens, dim), BF16), V(assign.T.shape, jnp.int32), V((1, slots), jnp.int32), V(w_router.T.shape, BF16),
                V((3, 2, RING, RING, tokens, third // 2), BF16),
                V((3, RING, RING, 16, slots), BF16),
                V((16, slots), BF16),
                V((3, 2, 2 * CAP * 8, 8 * tokens), F32),
                V((3, 2, 8, CAP, 16, third // 2), BF16),
                V((3, 2, 2 * CAP, RING, 16, third // 2), BF16),
                V((3, 2 * CAP, RING, 16, third), BF16),
                V((3, 2, CAP, RING, 16, third), BF16),
                V((3, 2, CAP, RING, 16, third), BF16),
                V((3, 2, CAP, RING, 16, third), BF16),
                V((3, RING, tokens, 128), BF16), V((3, RING, tokens, 128), BF16),
                V((3, RING, tokens, third), F32), V((3, RING, tokens, third), F32),
                V((tokens, dim), F32),
                V(w1_slots.shape[1:], BF16), V(w3_slots.shape[1:], BF16), V(w2_slots.shape[1:], BF16),
                V(w1_shared.shape, BF16), V(w3_shared.shape, BF16), V(w2_shared.shape, BF16),
                dma((6,)), dma((4,)), dma((9,)), dma((1,)), dma((1,)), dma((1,)), dma((2, 3)), dma((2,)), dma((1,)),
                dma((2,)), dma((2, 3)), dma((2, 3)), dma((3,)),
            ],
            compiler_params=pltpu.CompilerParams(collective_id=0, has_side_effects=True,
                                                 vmem_limit_bytes=60 * 2 ** 20),
        )(x_tokens, assign.T, slot_expert.reshape(1, -1), w_router.T, w1_slots, w3_slots, w2_slots,
          w1_shared, w3_shared, w2_shared)

    token_spec = P(('dp', 'ep'), None)
    slot_spec = P('ep', None, None)
    return jax.shard_map(device_step, mesh=mesh,
                         in_specs=(token_spec, P(), slot_spec, slot_spec, slot_spec, token_spec, P(), P(), P(), P()),
                         out_specs=token_spec, check_vma=False)
```

```python
import jax
import jax.numpy as jnp
from jax import lax
from jax.experimental import pallas as pl
from jax.experimental.pallas import tpu as pltpu
from jax.sharding import PartitionSpec as P

ROUTE_SCALE = 2.5
RING = 4
CAP = 9
BF16 = jnp.bfloat16
F32 = jnp.float32
STRIDE = {'x': 2, 'y': 8, 'z': 32}
CLASSES = (('y', 'z', 'x'), ('z', 'x', 'y'), ('x', 'y', 'z'))


def iota(shape, dim):
    return lax.broadcasted_iota(jnp.int32, shape, dim)


def dot(a, b):
    return jnp.dot(a, b, preferred_element_type=F32)


def dot_t(a, b):
    return lax.dot_general(a, b, (((1,), (1,)), ((), ())), preferred_element_type=F32)


def as_onehot(cond):
    return jnp.where(cond, 1.0, 0.0).astype(BF16)


def three_parts(v):
    hi = v.astype(BF16)
    rest = v - hi.astype(F32)
    mid = rest.astype(BF16)
    lo = (rest - mid.astype(F32)).astype(BF16)
    return hi, mid, lo


def moe_kernel(x_hbm, assign_hbm, slot_expert_hbm, wr_hbm, w1_hbm, w3_hbm, w2_hbm, s1_hbm, s3_hbm, s2_hbm, y_ref,
               x_ref, assign_ref, slot_expert_ref, wr_ref,
               G, T, tab, Pm, Sb, R, Ob, Hb, Z, F, Cs, Cr, U, A, zs, w1, w3, w2, s1, s3, s2,
               wsem, isem, sent, t1r, t2r, g0r, g1r, g2r, gfr, cr, d3r, d5r, d6r, d7r):
    t1s, t2s, g1s, g2s, cs, d3s, d5s, d6s, d7s = (sent.at[i] for i in range(9))
    me = lax.axis_index('ep')
    core = me % 2
    pos = {'x': (me // 2) % RING, 'y': (me // 8) % RING, 'z': me // 32}
    third = x_ref.shape[1] // 3
    sixth = third // 2

    def moved(axis, value):
        return (value - pos[axis]) * STRIDE[axis]

    def step_to(axis, d):
        return (pos[axis] + d) % RING

    def remote(src, dst, ssem, rsem, dev):
        return pltpu.make_async_remote_copy(src_ref=src, dst_ref=dst, send_sem=ssem, recv_sem=rsem,
                                            device_id={'ep': dev}, device_id_type=pl.DeviceIdType.MESH)

    def local(src, dst, sem):
        return pltpu.make_async_copy(src, dst, sem)

    def wait_bytes(ref, sem):
        pltpu.make_async_copy(ref, ref, sem).wait()

    barrier = pltpu.get_barrier_semaphore()

    def greet(dev):
        pl.semaphore_signal(barrier, inc=1, device_id={'ep': dev}, device_id_type=pl.DeviceIdType.MESH)

    other = 1 - 2 * core
    greet(me + other)
    for axis in 'xyz':
        for d in range(1, RING):
            dev = me + moved(axis, step_to(axis, d))
            greet(dev)
            greet(dev + other)

    input_copies = [local(s, d, isem.at[i]) for i, (s, d) in enumerate(
        ((assign_hbm, assign_ref), (x_hbm, x_ref), (slot_expert_hbm, slot_expert_ref), (wr_hbm, wr_ref)))]
    for c in input_copies:
        c.start()
    weight_copies = [pltpu.make_async_copy(s, d, wsem.at[i]) for i, (s, d) in enumerate(
        ((s1_hbm, s1), (s3_hbm, s3), (s2_hbm, s2), (w1_hbm.at[0], w1), (w3_hbm.at[0], w3), (w2_hbm.at[0], w2)))]
    for c in weight_copies:
        c.start()

    input_copies[0].wait()
    tokens = x_ref.shape[0]
    slots = slot_expert_ref.shape[1]
    slot_row = iota((slots, tokens), 0)
    chosen_t = jnp.zeros((slots, tokens), F32)
    for k in range(assign_ref.shape[0]):
        chosen_t = chosen_t + jnp.where(assign_ref[k:k + 1, :] == slot_row, 1.0, 0.0)
    ti, tj = iota((tokens, tokens), 0), iota((tokens, tokens), 1)
    chosen = dot_t(as_onehot(ti == tj), chosen_t.astype(BF16))
    rank = jnp.where(chosen > 0.5, dot(as_onehot(tj < ti), chosen.astype(BF16)), 99.0)
    token_id = (iota((tokens, slots), 0) + 1).astype(F32)
    tab_rows = [jnp.sum(jnp.where(rank == float(r), token_id, 0.0), axis=0, keepdims=True) for r in range(CAP)]
    tab[...] = jnp.concatenate(tab_rows + [jnp.zeros((16 - CAP, slots), F32)], axis=0).astype(BF16)

    for c in input_copies[1:]:
        c.wait()
    pl.semaphore_wait(barrier, 19)

    def cols(cls, g):
        return x_ref.at[:, pl.ds((2 * cls + g) * sixth, sixth)]

    def spread(cls, g, k, src, to):
        a2 = CLASSES[cls][1]
        for d in (1, 3):
            passed_on = (k % 2 == 0) == (d == 1)
            remote(src, G.at[cls, g, pos[a2], to], g2s, gfr.at[g, k] if passed_on else g2r.at[g],
                   me + moved(a2, step_to(a2, d))).start()

    def pass_on(g, k):
        wait_bytes(G.at[:, g, 0, 0], gfr.at[g, k])
        d = 1 if k % 2 == 0 else 3
        for cls, (a1, a2, a3) in enumerate(CLASSES):
            block = G.at[cls, g, step_to(a2, RING - d), step_to(a1, RING - k)]
            remote(block, block, g2s, g2r.at[g], me + moved(a2, step_to(a2, d))).start()

    for g in range(2):
        for cls, (a1, a2, a3) in enumerate(CLASSES):
            for d in (1, 3, 2):
                dev = me + moved(a1, step_to(a1, d))
                if g == 0:
                    remote(tab, T.at[cls, pos[a2], pos[a1]], t1s, t1r.at[0], dev).start()
                remote(cols(cls, g), G.at[cls, g, pos[a2], pos[a1]], g1s, g1r.at[g, d - 1], dev).start()
        for cls, (a1, a2, a3) in enumerate(CLASSES):
            spread(cls, g, 0, cols(cls, g), pos[a1])
            local(cols(cls, g), G.at[cls, g, pos[a2], pos[a1]], g0r.at[0]).start()
            if g == 0:
                T[cls, pos[a2], pos[a1]] = tab[...]

    gate = jax.nn.sigmoid(dot_t(x_ref[...], wr_ref[...]))
    num_experts = wr_ref.shape[0]
    slot_of = as_onehot(iota((num_experts, slots), 0) == slot_expert_ref[...])
    gate_slot = sum(dot(p, slot_of) for p in three_parts(gate))
    picked = jnp.where(chosen > 0.5, gate_slot, 0.0)
    route = ROUTE_SCALE * picked / jnp.maximum(jnp.sum(picked, axis=1, keepdims=True), 1e-30)
    route_rank = jnp.concatenate(three_parts(route) + (rank.astype(BF16),), axis=1)

    for g in range(2):
        for d in (3, 1, 2):
            wait_bytes(G.at[:, g, 0, 0], g1r.at[g, d - 1])
            for cls, (a1, a2, a3) in enumerate(CLASSES):
                owner = step_to(a1, RING - d)
                spread(cls, g, d, G.at[cls, g, pos[a2], owner], owner)
            if d == 1:
                pass_on(g, 0)
        for k in (3, 1, 2):
            pass_on(g, k)
        if g == 0:
            wait_bytes(T.at[:, 0, 0:3], t1r.at[0])
            for cls, (a1, a2, a3) in enumerate(CLASSES):
                row = T.at[cls, pos[a2]]
                for d in (1, 3, 2):
                    remote(row, row, t2s, t2r.at[0], me + moved(a2, step_to(a2, d))).start()

    si, sj = iota((4 * slots, 128), 0), iota((4 * slots, 128), 1)
    for cls, (a1, a2, a3) in enumerate(CLASSES):
        q_slot = (sj // 32 * slots + sj // 8 % 4 * STRIDE[a2] + sj // 4 % 2 + sj % 4 * STRIDE[a3])
        for v in range(RING):
            Cs[cls, v] = dot(route_rank, as_onehot(si == q_slot + v * STRIDE[a1])).astype(BF16)
        for d in (1, 3, 2, 0):
            v = step_to(a1, d)
            if d == 0:
                Cr[cls, pos[a1]] = Cs[cls, v]
            else:
                remote(Cs.at[cls, v], Cr.at[cls, pos[a1]], cs, cr.at[0], me + moved(a1, v)).start()

    for c in weight_copies[:3]:
        c.wait()
    ff_shared = s1.shape[1]
    step = 512
    acc = jnp.zeros((tokens, x_ref.shape[1]), F32)
    for f in range(0, ff_shared, step):
        xs = x_ref[...]
        mid = (jax.nn.silu(dot(xs, s1[:, f:f + step])) * dot(xs, s3[:, f:f + step])).astype(BF16)
        acc = acc + dot(mid, s2[f:f + step, :])
    zs[...] = acc

    rows = CAP * 8
    qi, qj = iota((rows, 256), 0), iota((rows, 256), 1)
    by_rank = [as_onehot(qj == (qi % 8 + 8 * h) * 16 + qi // 8) for h in range(2)]
    src_base = ((iota((rows, 128), 0) % 8) * tokens).astype(F32)
    lane = iota((rows, 128), 1).astype(F32)
    tabs, lines = [], []

    wait_bytes(G.at[:, :, 0, 0], g0r.at[0])
    wait_bytes(G.at[:, 0, 0:2], g2r.at[0])
    wait_bytes(T.at[:, 0:3], t2r.at[0])
    for cls, (a1, a2, a3) in enumerate(CLASSES):
        tabs.append([dot(m, T[cls].reshape(256, slots)).astype(BF16) for m in by_rank])
        lines.append(me - core - pos[a3] * STRIDE[a3])

    def select(n, _):
        g, e, p = n // 2 % 2, n // 4, n % 2

        @pl.when(n == 2)
        def _():
            wait_bytes(G.at[:, 1, 0:2], g2r.at[1])

        for cls, (a1, a2, a3) in enumerate(CLASSES):
            picks = []
            for q in range(2):
                d = 2 + q - p * (1 + 2 * q)
                slot = lines[cls] + step_to(a3, d) * STRIDE[a3] + (core + e) % 2
                picks.append(as_onehot(iota((slots, 128), 0) == slot))
            outs = []
            for h in range(2):
                for q in range(2):
                    val = dot(tabs[cls][h], picks[q])
                    code = jnp.where(val > 0.5, val - 1.0 + src_base, -1.0)
                    for b in range(8 * tokens // 128):
                        Pm[cls, h, q * rows:(q + 1) * rows, b * 128:(b + 1) * 128] = (
                            jnp.where(code == lane + float(b * 128), 1.0, 0.0))
                out = dot(Pm[cls, h].astype(BF16), G[cls, g, 2 * h:2 * h + 2].reshape(8 * tokens, sixth))
                outs.append(out.reshape(2, CAP, 8, sixth))
            both = jnp.concatenate(outs, axis=2).astype(BF16)
            for q in range(2):
                d = 2 + q - p * (1 + 2 * q)
                k = 2 * d + e
                Sb[cls, g, k] = both[q]
                dev = me + moved(a3, step_to(a3, d)) + (core + e) % 2 - core
                src, dst = Sb.at[cls, g, k], R.at[cls, g, pl.ds(core * CAP, CAP), pos[a3]]
                if q == 1:
                    mine = jnp.logical_and(n < 4, n % 2 == 1)

                    @pl.when(mine)
                    def _():
                        local(src, dst, d3r.at[e]).start()

                    @pl.when(jnp.logical_not(mine))
                    def _():
                        remote(src, dst, d3s, d3r.at[e], dev).start()
                else:
                    remote(src, dst, d3s, d3r.at[e], dev).start()
        return 0

    lax.fori_loop(0, 2 * RING, select, 0)

    for c in weight_copies[3:]:
        c.wait()
    blk = 3 * 64
    pi, pj = iota((blk, blk), 0), iota((blk, blk), 1)

    def bits(v):
        return v // 16 % 4, v // 4 % 4, v % 4

    ix, iz, iy = bits(pi)
    jx, jz, jy = bits(pj)
    to_first = {1: as_onehot(pj == pi // 64 * 64 + iy * 16 + ix * 4 + iz),
                2: as_onehot(pj == pi // 64 * 64 + iz * 16 + iy * 4 + ix)}
    from_first = {1: as_onehot(pi == pj // 64 * 64 + jy * 16 + jx * 4 + jz),
                  2: as_onehot(pi == pj // 64 * 64 + jz * 16 + jy * 4 + jx)}

    def permuted(mats, cls, value):
        if cls == 0:
            return value
        return jnp.concatenate([dot(mats[cls], value[i:i + blk]).astype(BF16)
                                for i in range(0, value.shape[0], blk)], axis=0)

    def expert(e, _):
        half = (core + e) % 2
        wait_bytes(R.at[:, :, 0:CAP], d3r.at[e])
        n = CAP * 64
        xs = jnp.concatenate([permuted(to_first, cls, R[cls, g, pl.ds(half * CAP, CAP)].reshape(n, sixth))
                              for cls in range(3) for g in range(2)], axis=1)
        mid = (jax.nn.silu(dot(xs, w1[...])) * dot(xs, w3[...])).astype(BF16)
        for cls, (a1, a2, a3) in enumerate(CLASSES):
            out = dot(mid, w2[:, cls * third:(cls + 1) * third]).astype(BF16)
            Ob[cls, pl.ds(half * CAP, CAP)] = permuted(from_first, cls, out).reshape(CAP, RING, 16, third)
            for d in (2, 1, 3, 0):
                v = step_to(a3, d)
                dev = me + moved(a3, v) + half - core
                src, dst = Ob.at[cls, pl.ds(half * CAP, CAP), v], Hb.at[cls, core, :, pos[a3]]
                if d == 0:
                    @pl.when(e == 0)
                    def _():
                        local(src, dst, d5r.at[e, cls]).start()

                    @pl.when(e != 0)
                    def _():
                        remote(src, dst, d5s, d5r.at[e, cls], dev).start()
                else:
                    remote(src, dst, d5s, d5r.at[e, cls], dev).start()
        return 0

    lax.fori_loop(0, 2, expert, 0)

    u2, v3 = pi // 16 % 4, pi // 4 % 4
    by_second = as_onehot(pj == pi // 64 * 64 + v3 * 16 + u2 * 4 + pi % 4)

    def regroup(e, _):
        half = (core + e) % 2
        for cls, (a1, a2, a3) in enumerate(CLASSES):
            wait_bytes(Hb.at[cls, half], d5r.at[e, cls])
            rows_in = Hb[cls, half].reshape(CAP * 64, third)
            Z[cls, half] = jnp.concatenate([dot(by_second, rows_in[i:i + blk]).astype(BF16) for i in
                                            range(0, CAP * 64, blk)], axis=0).reshape(CAP, RING, 16, third)
            for g, d in [(g, d) for g in range(2) for d in (2, 1, 3, 0)]:
                v = step_to(a2, d)
                part = pl.ds(g * sixth, sixth)
                src, dst = Z.at[cls, half, :, v, :, part], F.at[cls, half, :, pos[a2], :, part]
                if d == 0:
                    local(src, dst, d6r.at[e, g, cls]).start()
                else:
                    remote(src, dst, d6s, d6r.at[e, g, cls], me + moved(a2, v)).start()
        return 0

    lax.fori_loop(0, 2, regroup, 0)

    wait_bytes(Cr.at[:, 0:3], cr.at[0])

    def spreads(half):
        ei, ej = iota((128, 256), 0), iota((128, 256), 1)
        q = ej // 16 % 4 * 8 + half * 4 + ej // 4 % 4
        return [as_onehot(ei == q + 32 * part) for part in range(4)]

    def weigh(cls, half, spread_mats, targets, first, width):
        m = tokens * len(targets)
        lane_pos = iota((m, 256), 1)
        c = jnp.concatenate([Cr[cls, v] for v in targets], axis=0)
        w_exp = [dot(c, spread_mats[part]) for part in range(3)]
        source = jnp.concatenate([jnp.full((tokens, 256), v, jnp.int32) for v in targets], axis=0)
        rank_exp = jnp.where(lane_pos % 4 == source, dot(c, spread_mats[3]) - (lane_pos // 64).astype(F32), 99.0)
        acc = jnp.zeros((3 * m, width), F32)
        for r0 in range(0, CAP, 4):
            k = 64 * min(4, CAP - r0)
            hit = rank_exp == float(r0)
            w = jnp.concatenate([jnp.where(hit, w_exp[part], 0.0) for part in range(3)], axis=0).astype(BF16)
            acc = acc + dot(w[:, :k], F[cls, half, r0:r0 + k // 64, :, :, first:first + width].reshape(k, width))
        return (acc[2 * m:] + acc[m:2 * m] + acc[:m]).reshape(len(targets), tokens, width)

    mats = spreads(core)
    for cls in range(3):
        for g in range(2):
            wait_bytes(F.at[cls, core, :, :, :, 0:sixth], d6r.at[0, g, cls])
        U[cls] = weigh(cls, core, mats, list(range(RING)), 0, third)
    mats = spreads(1 - core)
    for g in range(2):
        here = slice(g * sixth, (g + 1) * sixth)
        part = pl.ds(g * sixth, sixth)
        for group in ((2,), (1, 3), (0,)):
            for cls, (a1, a2, a3) in enumerate(CLASSES):
                if group == (2,):
                    wait_bytes(F.at[cls, 1 - core, :, :, :, 0:sixth], d6r.at[1, g, cls])
                targets = [step_to(a1, d) for d in group]
                added = weigh(cls, 1 - core, mats, targets, g * sixth, sixth)
                for i, (d, v) in enumerate(zip(group, targets)):
                    if d == 0:
                        A[cls, pos[a1], :, here] = U[cls, v, :, here] + added[i]
                    else:
                        U[cls, v, :, here] = U[cls, v, :, here] + added[i]
                        remote(U.at[cls, v, :, part], A.at[cls, pos[a1], :, part], d7s, d7r.at[g, cls],
                               me + moved(a1, v)).start()
    for g in range(2):
        for cls in range(3):
            wait_bytes(A.at[cls, 0:3, :, 0:sixth], d7r.at[g, cls])
            here = slice(g * sixth, (g + 1) * sixth)
            there = slice((2 * cls + g) * sixth, (2 * cls + g + 1) * sixth)
            routed = (A[cls, 0, :, here] + A[cls, 1, :, here]) + (A[cls, 2, :, here] + A[cls, 3, :, here])
            y_ref[:, there] = (zs[:, there] + routed).astype(BF16)

    for ref, sem in ((T.at[:, 0, 0:3], t1s), (T.at[:, 0:3], t2s), (G.at[:, :, 0, 0:3], g1s), (G.at[:, :, 0:3], g2s),
                     (Cs.at[:, 0:3], cs), (Sb.at[:, :, 0:7], d3s), (Sb.at[:, :, 0:7], d5s), (Z.at[:, :, :, 0:3], d6s),
                     (U.at[:, 0:3], d7s)):
        wait_bytes(ref, sem)


def solution(mesh):
    def device_step(x_tokens, slot_expert, w1_slots, w3_slots, w2_slots, assign, w_router, w1_shared, w3_shared, w2_shared):
        tokens, dim = x_tokens.shape
        third = dim // 3
        slots = slot_expert.shape[0]
        vmem = pl.BlockSpec(memory_space=pltpu.VMEM)
        hbm = pl.BlockSpec(memory_space=pl.ANY)
        dma = pltpu.SemaphoreType.DMA
        V = pltpu.VMEM
        return pl.pallas_call(
            moe_kernel,
            out_shape=jax.ShapeDtypeStruct((tokens, dim), BF16),
            in_specs=[hbm] * 10,
            out_specs=vmem,
            scratch_shapes=[
                V((tokens, dim), BF16), V(assign.T.shape, jnp.int32), V((1, slots), jnp.int32), V(w_router.T.shape, BF16),
                V((3, 2, RING, RING, tokens, third // 2), BF16),
                V((3, RING, RING, 16, slots), BF16),
                V((16, slots), BF16),
                V((3, 2, 2 * CAP * 8, 8 * tokens), F32),
                V((3, 2, 8, CAP, 16, third // 2), BF16),
                V((3, 2, 2 * CAP, RING, 16, third // 2), BF16),
                V((3, 2 * CAP, RING, 16, third), BF16),
                V((3, 2, CAP, RING, 16, third), BF16),
                V((3, 2, CAP, RING, 16, third), BF16),
                V((3, 2, CAP, RING, 16, third), BF16),
                V((3, RING, tokens, 128), BF16), V((3, RING, tokens, 128), BF16),
                V((3, RING, tokens, third), F32), V((3, RING, tokens, third), F32),
                V((tokens, dim), F32),
                V(w1_slots.shape[1:], BF16), V(w3_slots.shape[1:], BF16), V(w2_slots.shape[1:], BF16),
                V(w1_shared.shape, BF16), V(w3_shared.shape, BF16), V(w2_shared.shape, BF16),
                dma((6,)), dma((4,)), dma((9,)), dma((1,)), dma((1,)), dma((1,)), dma((2, 3)), dma((2,)), dma((2, 4)), dma((1,)),
                dma((2,)), dma((2, 3)), dma((2, 2, 3)), dma((2, 3)),
            ],
            compiler_params=pltpu.CompilerParams(collective_id=0, has_side_effects=True,
                                                 vmem_limit_bytes=60 * 2 ** 20),
        )(x_tokens, assign.T, slot_expert.reshape(1, -1), w_router.T, w1_slots, w3_slots, w2_slots,
          w1_shared, w3_shared, w2_shared)

    token_spec = P(('dp', 'ep'), None)
    slot_spec = P('ep', None, None)
    return jax.shard_map(device_step, mesh=mesh,
                         in_specs=(token_spec, P(), slot_spec, slot_spec, slot_spec, token_spec, P(), P(), P(), P()),
                         out_specs=token_spec, check_vma=False)
```

```python
import jax
import jax.numpy as jnp
from jax import lax
from jax.experimental import pallas as pl
from jax.experimental.pallas import tpu as pltpu
from jax.sharding import PartitionSpec as P

ROUTE_SCALE = 2.5
RING = 4
CAP = 9
BF16 = jnp.bfloat16
F32 = jnp.float32
STRIDE = {'x': 2, 'y': 8, 'z': 32}
CLASSES = (('y', 'z', 'x'), ('z', 'x', 'y'), ('x', 'y', 'z'))


def iota(shape, dim):
    return lax.broadcasted_iota(jnp.int32, shape, dim)


def dot(a, b):
    return jnp.dot(a, b, preferred_element_type=F32)


def dot_t(a, b):
    return lax.dot_general(a, b, (((1,), (1,)), ((), ())), preferred_element_type=F32)


def as_onehot(cond):
    return jnp.where(cond, 1.0, 0.0).astype(BF16)


def three_parts(v):
    hi = v.astype(BF16)
    rest = v - hi.astype(F32)
    mid = rest.astype(BF16)
    lo = (rest - mid.astype(F32)).astype(BF16)
    return hi, mid, lo


def moe_kernel(x_hbm, assign_hbm, slot_expert_hbm, wr_hbm, w1_hbm, w3_hbm, w2_hbm, s1_hbm, s3_hbm, s2_hbm, y_ref,
               x_ref, assign_ref, slot_expert_ref, wr_ref,
               G, T, tab, Pm, Sb, R, Ob, Hb, Z, F, Cs, Cr, U, A, zs, w1, w3, w2, s1, s3, s2,
               wsem, isem, sent, t1r, t2r, g0r, g1r, g2r, cr, d3r, d5r, d6r, d7r):
    t1s, t2s, g1s, g2s, cs, d3s, d5s, d6s, d7s = (sent.at[i] for i in range(9))
    me = lax.axis_index('ep')
    core = me % 2
    pos = {'x': (me // 2) % RING, 'y': (me // 8) % RING, 'z': me // 32}
    third = x_ref.shape[1] // 3
    sixth = third // 2

    def moved(axis, value):
        return (value - pos[axis]) * STRIDE[axis]

    def step_to(axis, d):
        return (pos[axis] + d) % RING

    def remote(src, dst, ssem, rsem, dev):
        return pltpu.make_async_remote_copy(src_ref=src, dst_ref=dst, send_sem=ssem, recv_sem=rsem,
                                            device_id={'ep': dev}, device_id_type=pl.DeviceIdType.MESH)

    def local(src, dst, sem):
        return pltpu.make_async_copy(src, dst, sem)

    def wait_bytes(ref, sem):
        pltpu.make_async_copy(ref, ref, sem).wait()

    barrier = pltpu.get_barrier_semaphore()

    def greet(dev):
        pl.semaphore_signal(barrier, inc=1, device_id={'ep': dev}, device_id_type=pl.DeviceIdType.MESH)

    other = 1 - 2 * core
    greet(me + other)
    for axis in 'xyz':
        for d in range(1, RING):
            dev = me + moved(axis, step_to(axis, d))
            greet(dev)
            greet(dev + other)

    input_copies = [local(s, d, isem.at[i]) for i, (s, d) in enumerate(
        ((assign_hbm, assign_ref), (x_hbm, x_ref), (slot_expert_hbm, slot_expert_ref), (wr_hbm, wr_ref)))]
    for c in input_copies:
        c.start()
    expert_weights = [(w2_hbm.at[0], w2, 3)]
    for g in range(2):
        for cls in range(3):
            src, dst = pl.ds((2 * cls + g) * sixth, sixth), pl.ds((3 * g + cls) * sixth, sixth)
            expert_weights += [(w1_hbm.at[0, src], w1.at[dst], 4), (w3_hbm.at[0, src], w3.at[dst], 5)]
    weight_copies = [local(s, d, wsem.at[i]) for s, d, i in
                     [(s1_hbm, s1, 0), (s3_hbm, s3, 1), (s2_hbm, s2, 2)] + expert_weights]
    for c in weight_copies:
        c.start()

    input_copies[0].wait()
    tokens = x_ref.shape[0]
    slots = slot_expert_ref.shape[1]
    slot_row = iota((slots, tokens), 0)
    chosen_t = jnp.zeros((slots, tokens), F32)
    for k in range(assign_ref.shape[0]):
        chosen_t = chosen_t + jnp.where(assign_ref[k:k + 1, :] == slot_row, 1.0, 0.0)
    ti, tj = iota((tokens, tokens), 0), iota((tokens, tokens), 1)
    chosen = dot_t(as_onehot(ti == tj), chosen_t.astype(BF16))
    rank = jnp.where(chosen > 0.5, dot(as_onehot(tj < ti), chosen.astype(BF16)), 99.0)
    token_id = (iota((tokens, slots), 0) + 1).astype(F32)
    tab_rows = [jnp.sum(jnp.where(rank == float(r), token_id, 0.0), axis=0, keepdims=True) for r in range(CAP)]
    tab[...] = jnp.concatenate(tab_rows + [jnp.zeros((16 - CAP, slots), F32)], axis=0).astype(BF16)

    for c in input_copies[1:]:
        c.wait()
    pl.semaphore_wait(barrier, 19)

    def cols(cls, g):
        return x_ref.at[:, pl.ds((2 * cls + g) * sixth, sixth)]

    def spread(cls, g, k, src, to):
        a2 = CLASSES[cls][1]
        for d in (1, 3, 2):
            remote(src, G.at[cls, g, pos[a2], to], g2s, g2r.at[g],
                   me + moved(a2, step_to(a2, d))).start()

    for g in range(2):
        for cls, (a1, a2, a3) in enumerate(CLASSES):
            for d in (1, 3, 2):
                dev = me + moved(a1, step_to(a1, d))
                if g == 0:
                    remote(tab, T.at[cls, pos[a2], pos[a1]], t1s, t1r.at[0], dev).start()
                remote(cols(cls, g), G.at[cls, g, pos[a2], pos[a1]], g1s, g1r.at[g, d - 1], dev).start()
        for cls, (a1, a2, a3) in enumerate(CLASSES):
            spread(cls, g, 0, cols(cls, g), pos[a1])
            local(cols(cls, g), G.at[cls, g, pos[a2], pos[a1]], g0r.at[0]).start()
            if g == 0:
                T[cls, pos[a2], pos[a1]] = tab[...]

    gate = jax.nn.sigmoid(dot_t(x_ref[...], wr_ref[...]))
    num_experts = wr_ref.shape[0]
    slot_of = as_onehot(iota((num_experts, slots), 0) == slot_expert_ref[...])
    gate_slot = sum(dot(p, slot_of) for p in three_parts(gate))
    picked = jnp.where(chosen > 0.5, gate_slot, 0.0)
    route = ROUTE_SCALE * picked / jnp.maximum(jnp.sum(picked, axis=1, keepdims=True), 1e-30)
    route_rank = jnp.concatenate(three_parts(route) + (rank.astype(BF16),), axis=1)

    for g in range(2):
        for d in (3, 1, 2):
            wait_bytes(G.at[:, g, 0, 0], g1r.at[g, d - 1])
            for cls, (a1, a2, a3) in enumerate(CLASSES):
                owner = (pos[a1] + RING - d) % RING
                spread(cls, g, d, G.at[cls, g, pos[a2], owner], owner)
        if g == 0:
            wait_bytes(T.at[:, 0, 0:3], t1r.at[0])
            for cls, (a1, a2, a3) in enumerate(CLASSES):
                row = T.at[cls, pos[a2]]
                for d in (1, 3, 2):
                    remote(row, row, t2s, t2r.at[0], me + moved(a2, step_to(a2, d))).start()

    si, sj = iota((4 * slots, 128), 0), iota((4 * slots, 128), 1)
    for cls, (a1, a2, a3) in enumerate(CLASSES):
        q_slot = (sj // 32 * slots + sj // 8 % 4 * STRIDE[a2] + sj // 4 % 2 + sj % 4 * STRIDE[a3])
        for v in range(RING):
            Cs[cls, v] = dot(route_rank, as_onehot(si == q_slot + v * STRIDE[a1])).astype(BF16)

    for c in weight_copies[:3]:
        c.wait()
    ff_shared = s1.shape[1]
    step = 512
    acc = jnp.zeros((tokens, x_ref.shape[1]), F32)
    for f in range(0, ff_shared, step):
        xs = x_ref[...]
        mid = (jax.nn.silu(dot(xs, s1[:, f:f + step])) * dot(xs, s3[:, f:f + step])).astype(BF16)
        acc = acc + dot(mid, s2[f:f + step, :])
    zs[...] = acc

    rows = CAP * 8
    qi, qj = iota((rows, 256), 0), iota((rows, 256), 1)
    by_rank = [as_onehot(qj == (qi % 8 + 8 * h) * 16 + qi // 8) for h in range(2)]
    src_base = ((iota((rows, 128), 0) % 8) * tokens).astype(F32)
    lane = iota((rows, 128), 1).astype(F32)
    tabs, lines = [], []

    wait_bytes(G.at[:, :, 0, 0], g0r.at[0])
    wait_bytes(G.at[:, 0, 0:3], g2r.at[0])
    wait_bytes(T.at[:, 0:3], t2r.at[0])
    for cls, (a1, a2, a3) in enumerate(CLASSES):
        tabs.append([dot(m, T[cls].reshape(256, slots)).astype(BF16) for m in by_rank])
        lines.append(me - core - pos[a3] * STRIDE[a3])

    def select(n, _):
        g, e, p = n // 2 % 2, n // 4, n % 2

        @pl.when(n == 2)
        def _():
            wait_bytes(G.at[:, 1, 0:3], g2r.at[1])

        @pl.when(g == 0)
        def _():
            for cls, (a1, a2, a3) in enumerate(CLASSES):
                for q in range(2):
                    d = 2 + q - p * (1 + 2 * q)
                    slot = lines[cls] + step_to(a3, d) * STRIDE[a3] + (core + e) % 2
                    pick = as_onehot(iota((slots, 128), 0) == slot)
                    for h in range(2):
                        val = dot(tabs[cls][h], pick)
                        code = jnp.where(val > 0.5, val - 1.0 + src_base, -1.0)
                        for b in range(8 * tokens // 128):
                            Pm[p, cls, h, q * rows:(q + 1) * rows, b * 128:(b + 1) * 128] = (
                                jnp.where(code == lane + float(b * 128), 1.0, 0.0))

        for cls, (a1, a2, a3) in enumerate(CLASSES):
            outs = []
            for h in range(2):
                out = dot(Pm[p, cls, h].astype(BF16), G[cls, g, 2 * h:2 * h + 2].reshape(8 * tokens, sixth))
                outs.append(out.reshape(2, CAP, 8, sixth))
            both = jnp.concatenate(outs, axis=2).astype(BF16)
            for q in range(2):
                d = 2 + q - p * (1 + 2 * q)
                k = 2 * d + e
                Sb[cls, g, k] = both[q]
                dev = me + moved(a3, step_to(a3, d)) + (core + e) % 2 - core
                src, dst = Sb.at[cls, g, k], R.at[cls, g, pl.ds(core * CAP, CAP), pos[a3]]
                if q == 1:
                    mine = jnp.logical_and(n < 4, n % 2 == 1)

                    @pl.when(mine)
                    def _():
                        local(src, dst, d3r.at[e, g]).start()

                    @pl.when(jnp.logical_not(mine))
                    def _():
                        remote(src, dst, d3s, d3r.at[e, g], dev).start()
                else:
                    remote(src, dst, d3s, d3r.at[e, g], dev).start()
        return 0

    lax.fori_loop(0, 2 * RING, select, 0)

    for cls, (a1, a2, a3) in enumerate(CLASSES):
        for d in (1, 3, 2, 0):
            v = step_to(a1, d)
            if d == 0:
                Cr[cls, pos[a1]] = Cs[cls, v]
            else:
                remote(Cs.at[cls, v], Cr.at[cls, pos[a1]], cs, cr.at[0], me + moved(a1, v)).start()

    for w, i in ((w2, 3), (w1, 4), (w3, 5)):
        wait_bytes(w, wsem.at[i])
    blk = 3 * 64
    pi, pj = iota((blk, blk), 0), iota((blk, blk), 1)

    def bits(v):
        return v // 16 % 4, v // 4 % 4, v % 4

    ix, iz, iy = bits(pi)
    jx, jz, jy = bits(pj)
    to_first = {1: as_onehot(pj == pi // 64 * 64 + iy * 16 + ix * 4 + iz),
                2: as_onehot(pj == pi // 64 * 64 + iz * 16 + iy * 4 + ix)}
    from_first = {1: as_onehot(pi == pj // 64 * 64 + jy * 16 + jx * 4 + jz),
                  2: as_onehot(pi == pj // 64 * 64 + jz * 16 + jy * 4 + jx)}

    def permuted(mats, cls, value):
        if cls == 0:
            return value
        return jnp.concatenate([dot(mats[cls], value[i:i + blk]).astype(BF16)
                                for i in range(0, value.shape[0], blk)], axis=0)

    def expert(e, _):
        half = (core + e) % 2
        n = CAP * 64
        h_gate = h_up = 0.0
        for g in range(2):
            wait_bytes(R.at[:, g, 0:CAP], d3r.at[e, g])
            xs = jnp.concatenate([permuted(to_first, cls, R[cls, g, pl.ds(half * CAP, CAP)].reshape(n, sixth))
                                  for cls in range(3)], axis=1)
            part = slice(3 * g * sixth, 3 * (g + 1) * sixth)
            h_gate = h_gate + dot(xs, w1[part])
            h_up = h_up + dot(xs, w3[part])
        mid = (jax.nn.silu(h_gate) * h_up).astype(BF16)
        for cls, (a1, a2, a3) in enumerate(CLASSES):
            out = dot(mid, w2[:, cls * third:(cls + 1) * third]).astype(BF16)
            Ob[cls, pl.ds(half * CAP, CAP)] = permuted(from_first, cls, out).reshape(CAP, RING, 16, third)
            for d in (2, 1, 3, 0):
                v = step_to(a3, d)
                dev = me + moved(a3, v) + half - core
                src, dst = Ob.at[cls, pl.ds(half * CAP, CAP), v], Hb.at[cls, core, :, pos[a3]]
                if d == 0:
                    @pl.when(e == 0)
                    def _():
                        local(src, dst, d5r.at[e, cls]).start()

                    @pl.when(e != 0)
                    def _():
                        remote(src, dst, d5s, d5r.at[e, cls], dev).start()
                else:
                    remote(src, dst, d5s, d5r.at[e, cls], dev).start()
        return 0

    lax.fori_loop(0, 2, expert, 0)

    u2, v3 = pi // 16 % 4, pi // 4 % 4
    by_second = as_onehot(pj == pi // 64 * 64 + v3 * 16 + u2 * 4 + pi % 4)

    def regroup(e, _):
        half = (core + e) % 2
        for cls, (a1, a2, a3) in enumerate(CLASSES):
            wait_bytes(Hb.at[cls, half], d5r.at[e, cls])
            rows_in = Hb[cls, half].reshape(CAP * 64, third)
            Z[cls, half] = jnp.concatenate([dot(by_second, rows_in[i:i + blk]).astype(BF16) for i in
                                            range(0, CAP * 64, blk)], axis=0).reshape(CAP, RING, 16, third)
            for d in (2, 1, 3, 0):
                v = step_to(a2, d)
                src, dst = Z.at[cls, half, :, v], F.at[cls, half, :, pos[a2]]
                if d == 0:
                    local(src, dst, d6r.at[e, cls]).start()
                else:
                    remote(src, dst, d6s, d6r.at[e, cls], me + moved(a2, v)).start()
        return 0

    lax.fori_loop(0, 2, regroup, 0)

    wait_bytes(Cr.at[:, 0:3], cr.at[0])

    def spreads(half):
        ei, ej = iota((128, 256), 0), iota((128, 256), 1)
        q = ej // 16 % 4 * 8 + half * 4 + ej // 4 % 4
        return [as_onehot(ei == q + 32 * part) for part in range(4)]

    def weigh(cls, half, spread_mats, targets):
        m = tokens * len(targets)
        lane_pos = iota((m, 256), 1)
        c = jnp.concatenate([Cr[cls, v] for v in targets], axis=0)
        w_exp = [dot(c, spread_mats[part]) for part in range(3)]
        source = jnp.concatenate([jnp.full((tokens, 256), v, jnp.int32) for v in targets], axis=0)
        rank_exp = jnp.where(lane_pos % 4 == source, dot(c, spread_mats[3]) - (lane_pos // 64).astype(F32), 99.0)
        acc = jnp.zeros((3 * m, third), F32)
        for r0 in range(0, CAP, 4):
            k = 64 * min(4, CAP - r0)
            hit = rank_exp == float(r0)
            w = jnp.concatenate([jnp.where(hit, w_exp[part], 0.0) for part in range(3)], axis=0).astype(BF16)
            acc = acc + dot(w[:, :k], F[cls, half, r0:r0 + k // 64].reshape(k, third))
        return (acc[2 * m:] + acc[m:2 * m] + acc[:m]).reshape(len(targets), tokens, third)

    mats = spreads(core)
    for cls in range(3):
        wait_bytes(F.at[cls, core], d6r.at[0, cls])
        U[cls] = weigh(cls, core, mats, list(range(RING)))
    mats = spreads(1 - core)
    for group in ((2,), (1, 3), (0,)):
        for cls, (a1, a2, a3) in enumerate(CLASSES):
            if group == (2,):
                wait_bytes(F.at[cls, 1 - core], d6r.at[1, cls])
            targets = [step_to(a1, d) for d in group]
            part = weigh(cls, 1 - core, mats, targets)
            for i, (d, v) in enumerate(zip(group, targets)):
                if d == 0:
                    A[cls, pos[a1]] = U[cls, v] + part[i]
                else:
                    U[cls, v] = U[cls, v] + part[i]
                    remote(U.at[cls, v], A.at[cls, pos[a1]], d7s, d7r.at[cls], me + moved(a1, v)).start()
    for cls in range(3):
        wait_bytes(A.at[cls, 0:3], d7r.at[cls])
        routed = (A[cls, 0] + A[cls, 1]) + (A[cls, 2] + A[cls, 3])
        y_ref[:, cls * third:(cls + 1) * third] = (zs[:, cls * third:(cls + 1) * third] + routed).astype(BF16)

    for ref, sem in ((T.at[:, 0, 0:3], t1s), (T.at[:, 0:3], t2s), (G.at[:, :, 0, 0:3], g1s), (G.at[:, :, 0:3], g2s),
                     (Cs.at[:, 0:3], cs), (Sb.at[:, :, 0:7], d3s), (Sb.at[:, :, 0:7], d5s), (Z.at[:, :, :, 0:3], d6s),
                     (U.at[:, 0:3], d7s)):
        wait_bytes(ref, sem)


def solution(mesh):
    def device_step(x_tokens, slot_expert, w1_slots, w3_slots, w2_slots, assign, w_router, w1_shared, w3_shared, w2_shared):
        tokens, dim = x_tokens.shape
        third = dim // 3
        slots = slot_expert.shape[0]
        vmem = pl.BlockSpec(memory_space=pltpu.VMEM)
        hbm = pl.BlockSpec(memory_space=pltpu.HBM)
        dma = pltpu.SemaphoreType.DMA
        V = pltpu.VMEM
        return pl.pallas_call(
            moe_kernel,
            out_shape=jax.ShapeDtypeStruct((tokens, dim), BF16),
            in_specs=[hbm] * 10,
            out_specs=vmem,
            scratch_shapes=[
                V((tokens, dim), BF16), V(assign.T.shape, jnp.int32), V((1, slots), jnp.int32), V(w_router.T.shape, BF16),
                V((3, 2, RING, RING, tokens, third // 2), BF16),
                V((3, RING, RING, 16, slots), BF16),
                V((16, slots), BF16),
                V((2, 3, 2, 2 * CAP * 8, 8 * tokens), F32),
                V((3, 2, 8, CAP, 16, third // 2), BF16),
                V((3, 2, 2 * CAP, RING, 16, third // 2), BF16),
                V((3, 2 * CAP, RING, 16, third), BF16),
                V((3, 2, CAP, RING, 16, third), BF16),
                V((3, 2, CAP, RING, 16, third), BF16),
                V((3, 2, CAP, RING, 16, third), BF16),
                V((3, RING, tokens, 128), BF16), V((3, RING, tokens, 128), BF16),
                V((3, RING, tokens, third), F32), V((3, RING, tokens, third), F32),
                V((tokens, dim), F32),
                V(w1_slots.shape[1:], BF16), V(w3_slots.shape[1:], BF16), V(w2_slots.shape[1:], BF16),
                V(w1_shared.shape, BF16), V(w3_shared.shape, BF16), V(w2_shared.shape, BF16),
                dma((6,)), dma((4,)), dma((9,)), dma((1,)), dma((1,)), dma((1,)), dma((2, 3)), dma((2,)), dma((1,)),
                dma((2, 2)), dma((2, 3)), dma((2, 3)), dma((3,)),
            ],
            compiler_params=pltpu.CompilerParams(collective_id=0, has_side_effects=True,
                                                 vmem_limit_bytes=52 * 2 ** 20),
        )(x_tokens, assign.T, slot_expert.reshape(1, -1), w_router.T, w1_slots, w3_slots, w2_slots,
          w1_shared, w3_shared, w2_shared)

    token_spec = P(('dp', 'ep'), None)
    slot_spec = P('ep', None, None)
    return jax.shard_map(device_step, mesh=mesh,
                         in_specs=(token_spec, P(), slot_spec, slot_spec, slot_spec, token_spec, P(), P(), P(), P()),
                         out_specs=token_spec, check_vma=False)
```

```python
import jax
import jax.numpy as jnp
from jax import lax
from jax.experimental import pallas as pl
from jax.experimental.pallas import tpu as pltpu
from jax.sharding import PartitionSpec as P

ROUTE_SCALE = 2.5
RING = 4
CAP = 9
BF16 = jnp.bfloat16
F32 = jnp.float32
STRIDE = {'x': 2, 'y': 8, 'z': 32}
CLASSES = (('y', 'z', 'x'), ('z', 'x', 'y'), ('x', 'y', 'z'))


def iota(shape, dim):
    return lax.broadcasted_iota(jnp.int32, shape, dim)


def dot(a, b):
    return jnp.dot(a, b, preferred_element_type=F32)


def dot_t(a, b):
    return lax.dot_general(a, b, (((1,), (1,)), ((), ())), preferred_element_type=F32)


def as_onehot(cond):
    return jnp.where(cond, 1.0, 0.0).astype(BF16)


def three_parts(v):
    hi = v.astype(BF16)
    rest = v - hi.astype(F32)
    mid = rest.astype(BF16)
    lo = (rest - mid.astype(F32)).astype(BF16)
    return hi, mid, lo


def moe_kernel(x_hbm, assign_hbm, slot_expert_hbm, wr_hbm, w1_hbm, w3_hbm, w2_hbm, s1_hbm, s3_hbm, s2_hbm, y_ref,
               x_ref, assign_ref, slot_expert_ref, wr_ref,
               G, T, tab, Pm, Sb, R, Ob, Hb, Z, F, Cs, Cr, U, A, zs, w1, w3, w2, s1, s3, s2,
               wsem, isem, sent, t1r, t2r, g0r, g1r, g2r, cr, d3r, d5r, d6r, d7r):
    t1s, t2s, g1s, g2s, cs, d3s, d5s, d6s, d7s = (sent.at[i] for i in range(9))
    me = lax.axis_index('ep')
    core = me % 2
    pos = {'x': (me // 2) % RING, 'y': (me // 8) % RING, 'z': me // 32}
    third = x_ref.shape[1] // 3
    sixth = third // 2

    def moved(axis, value):
        return (value - pos[axis]) * STRIDE[axis]

    def step_to(axis, d):
        return (pos[axis] + d) % RING

    def remote(src, dst, ssem, rsem, dev):
        return pltpu.make_async_remote_copy(src_ref=src, dst_ref=dst, send_sem=ssem, recv_sem=rsem,
                                            device_id={'ep': dev}, device_id_type=pl.DeviceIdType.MESH)

    def local(src, dst, sem):
        return pltpu.make_async_copy(src, dst, sem)

    def wait_bytes(ref, sem):
        pltpu.make_async_copy(ref, ref, sem).wait()

    barrier = pltpu.get_barrier_semaphore()

    def greet(dev):
        pl.semaphore_signal(barrier, inc=1, device_id={'ep': dev}, device_id_type=pl.DeviceIdType.MESH)

    other = 1 - 2 * core
    greet(me + other)
    for axis in 'xyz':
        for d in range(1, RING):
            dev = me + moved(axis, step_to(axis, d))
            greet(dev)
            greet(dev + other)

    input_copies = [local(s, d, isem.at[i]) for i, (s, d) in enumerate(
        ((assign_hbm, assign_ref), (x_hbm, x_ref), (slot_expert_hbm, slot_expert_ref), (wr_hbm, wr_ref)))]
    for c in input_copies:
        c.start()
    expert_weights = [(w2_hbm.at[0], w2, 3)]
    for g in range(2):
        for cls in range(3):
            src, dst = pl.ds((2 * cls + g) * sixth, sixth), pl.ds((3 * g + cls) * sixth, sixth)
            expert_weights += [(w1_hbm.at[0, src], w1.at[dst], 4), (w3_hbm.at[0, src], w3.at[dst], 5)]
    weight_copies = [local(s, d, wsem.at[i]) for s, d, i in
                     [(s1_hbm, s1, 0), (s3_hbm, s3, 1), (s2_hbm, s2, 2)] + expert_weights]
    for c in weight_copies:
        c.start()

    input_copies[0].wait()
    tokens = x_ref.shape[0]
    slots = slot_expert_ref.shape[1]
    slot_row = iota((slots, tokens), 0)
    chosen_t = jnp.zeros((slots, tokens), F32)
    for k in range(assign_ref.shape[0]):
        chosen_t = chosen_t + jnp.where(assign_ref[k:k + 1, :] == slot_row, 1.0, 0.0)
    ti, tj = iota((tokens, tokens), 0), iota((tokens, tokens), 1)
    chosen = dot_t(as_onehot(ti == tj), chosen_t.astype(BF16))
    rank = jnp.where(chosen > 0.5, dot(as_onehot(tj < ti), chosen.astype(BF16)), 99.0)
    token_id = (iota((tokens, slots), 0) + 1).astype(F32)
    tab_rows = [jnp.sum(jnp.where(rank == float(r), token_id, 0.0), axis=0, keepdims=True) for r in range(CAP)]
    tab[...] = jnp.concatenate(tab_rows + [jnp.zeros((16 - CAP, slots), F32)], axis=0).astype(BF16)

    for c in input_copies[1:]:
        c.wait()
    pl.semaphore_wait(barrier, 19)

    def cols(cls, g):
        return x_ref.at[:, pl.ds((2 * cls + g) * sixth, sixth)]

    def spread(cls, g, k, src, to):
        a2 = CLASSES[cls][1]
        for d in (1, 3, 2):
            remote(src, G.at[cls, g, pos[a2], to], g2s, g2r.at[g],
                   me + moved(a2, step_to(a2, d))).start()

    for g in range(2):
        for cls, (a1, a2, a3) in enumerate(CLASSES):
            for d in (1, 3, 2):
                dev = me + moved(a1, step_to(a1, d))
                if g == 0:
                    remote(tab, T.at[cls, pos[a2], pos[a1]], t1s, t1r.at[0], dev).start()
                remote(cols(cls, g), G.at[cls, g, pos[a2], pos[a1]], g1s, g1r.at[g, d - 1], dev).start()
        for cls, (a1, a2, a3) in enumerate(CLASSES):
            spread(cls, g, 0, cols(cls, g), pos[a1])
            local(cols(cls, g), G.at[cls, g, pos[a2], pos[a1]], g0r.at[0]).start()
            if g == 0:
                T[cls, pos[a2], pos[a1]] = tab[...]

    gate = jax.nn.sigmoid(dot_t(x_ref[...], wr_ref[...]))
    num_experts = wr_ref.shape[0]
    slot_of = as_onehot(iota((num_experts, slots), 0) == slot_expert_ref[...])
    gate_slot = sum(dot(p, slot_of) for p in three_parts(gate))
    picked = jnp.where(chosen > 0.5, gate_slot, 0.0)
    route = ROUTE_SCALE * picked / jnp.maximum(jnp.sum(picked, axis=1, keepdims=True), 1e-30)
    route_rank = jnp.concatenate(three_parts(route) + (rank.astype(BF16),), axis=1)

    for g in range(2):
        for d in (3, 1, 2):
            wait_bytes(G.at[:, g, 0, 0], g1r.at[g, d - 1])
            for cls, (a1, a2, a3) in enumerate(CLASSES):
                owner = (pos[a1] + RING - d) % RING
                spread(cls, g, d, G.at[cls, g, pos[a2], owner], owner)
        if g == 0:
            wait_bytes(T.at[:, 0, 0:3], t1r.at[0])
            for cls, (a1, a2, a3) in enumerate(CLASSES):
                row = T.at[cls, pos[a2]]
                for d in (1, 3, 2):
                    remote(row, row, t2s, t2r.at[0], me + moved(a2, step_to(a2, d))).start()

    si, sj = iota((4 * slots, 128), 0), iota((4 * slots, 128), 1)
    for cls, (a1, a2, a3) in enumerate(CLASSES):
        q_slot = (sj // 32 * slots + sj // 8 % 4 * STRIDE[a2] + sj // 4 % 2 + sj % 4 * STRIDE[a3])
        for v in range(RING):
            Cs[cls, v] = dot(route_rank, as_onehot(si == q_slot + v * STRIDE[a1])).astype(BF16)

    for c in weight_copies[:3]:
        c.wait()
    ff_shared = s1.shape[1]
    step = 512
    acc = jnp.zeros((tokens, x_ref.shape[1]), F32)
    for f in range(0, ff_shared, step):
        xs = x_ref[...]
        mid = (jax.nn.silu(dot(xs, s1[:, f:f + step])) * dot(xs, s3[:, f:f + step])).astype(BF16)
        acc = acc + dot(mid, s2[f:f + step, :])
    zs[...] = acc

    rows = CAP * 8
    qi, qj = iota((rows, 256), 0), iota((rows, 256), 1)
    by_rank = [as_onehot(qj == (qi % 8 + 8 * h) * 16 + qi // 8) for h in range(2)]
    src_base = ((iota((rows, 128), 0) % 8) * tokens).astype(F32)
    lane = iota((rows, 128), 1).astype(F32)
    tabs, lines = [], []

    wait_bytes(G.at[:, :, 0, 0], g0r.at[0])
    wait_bytes(G.at[:, 0, 0:3], g2r.at[0])
    wait_bytes(T.at[:, 0:3], t2r.at[0])
    for cls, (a1, a2, a3) in enumerate(CLASSES):
        tabs.append([dot(m, T[cls].reshape(256, slots)).astype(BF16) for m in by_rank])
        lines.append(me - core - pos[a3] * STRIDE[a3])

    def select(n, _):
        g, e, p = n // 2 % 2, n // 4, n % 2

        @pl.when(n == 2)
        def _():
            wait_bytes(G.at[:, 1, 0:3], g2r.at[1])

        @pl.when(g == 0)
        def _():
            for cls, (a1, a2, a3) in enumerate(CLASSES):
                for q in range(2):
                    d = 2 + q - p * (1 + 2 * q)
                    slot = lines[cls] + step_to(a3, d) * STRIDE[a3] + (core + e) % 2
                    pick = as_onehot(iota((slots, 128), 0) == slot)
                    for h in range(2):
                        val = dot(tabs[cls][h], pick)
                        code = jnp.where(val > 0.5, val - 1.0 + src_base, -1.0)
                        for b in range(8 * tokens // 128):
                            Pm[p, cls, h, q * rows:(q + 1) * rows, b * 128:(b + 1) * 128] = (
                                jnp.where(code == lane + float(b * 128), 1.0, 0.0))

        for cls, (a1, a2, a3) in enumerate(CLASSES):
            outs = []
            for h in range(2):
                out = dot(Pm[p, cls, h].astype(BF16), G[cls, g, 2 * h:2 * h + 2].reshape(8 * tokens, sixth))
                outs.append(out.reshape(2, CAP, 8, sixth))
            both = jnp.concatenate(outs, axis=2).astype(BF16)
            for q in range(2):
                d = 2 + q - p * (1 + 2 * q)
                k = 2 * d + e
                Sb[cls, g, k] = both[q]
                dev = me + moved(a3, step_to(a3, d)) + (core + e) % 2 - core
                src, dst = Sb.at[cls, g, k], R.at[cls, g, pl.ds(core * CAP, CAP), pos[a3]]
                if q == 1:
                    mine = jnp.logical_and(n < 4, n % 2 == 1)

                    @pl.when(mine)
                    def _():
                        local(src, dst, d3r.at[e, g]).start()

                    @pl.when(jnp.logical_not(mine))
                    def _():
                        remote(src, dst, d3s, d3r.at[e, g], dev).start()
                else:
                    remote(src, dst, d3s, d3r.at[e, g], dev).start()
        return 0

    lax.fori_loop(0, 2 * RING, select, 0)

    for cls, (a1, a2, a3) in enumerate(CLASSES):
        for d in (1, 3, 2, 0):
            v = step_to(a1, d)
            if d == 0:
                Cr[cls, pos[a1]] = Cs[cls, v]
            else:
                remote(Cs.at[cls, v], Cr.at[cls, pos[a1]], cs, cr.at[0], me + moved(a1, v)).start()

    for w, i in ((w2, 3), (w1, 4), (w3, 5)):
        wait_bytes(w, wsem.at[i])
    blk = 3 * 64
    pi, pj = iota((blk, blk), 0), iota((blk, blk), 1)

    def bits(v):
        return v // 16 % 4, v // 4 % 4, v % 4

    ix, iz, iy = bits(pi)
    jx, jz, jy = bits(pj)
    to_first = {1: as_onehot(pj == pi // 64 * 64 + iy * 16 + ix * 4 + iz),
                2: as_onehot(pj == pi // 64 * 64 + iz * 16 + iy * 4 + ix)}
    from_first = {1: as_onehot(pi == pj // 64 * 64 + jy * 16 + jx * 4 + jz),
                  2: as_onehot(pi == pj // 64 * 64 + jz * 16 + jy * 4 + jx)}

    def permuted(mats, cls, value):
        if cls == 0:
            return value
        return jnp.concatenate([dot(mats[cls], value[i:i + blk]).astype(BF16)
                                for i in range(0, value.shape[0], blk)], axis=0)

    def expert(e, _):
        half = (core + e) % 2
        n = CAP * 64
        h_gate = h_up = 0.0
        for g in range(2):
            wait_bytes(R.at[:, g, 0:CAP], d3r.at[e, g])
            xs = jnp.concatenate([permuted(to_first, cls, R[cls, g, pl.ds(half * CAP, CAP)].reshape(n, sixth))
                                  for cls in range(3)], axis=1)
            part = slice(3 * g * sixth, 3 * (g + 1) * sixth)
            h_gate = h_gate + dot(xs, w1[part])
            h_up = h_up + dot(xs, w3[part])
        mid = (jax.nn.silu(h_gate) * h_up).astype(BF16)
        for cls, (a1, a2, a3) in enumerate(CLASSES):
            out = dot(mid, w2[:, cls * third:(cls + 1) * third]).astype(BF16)
            Ob[cls, pl.ds(half * CAP, CAP)] = permuted(from_first, cls, out).reshape(CAP, RING, 16, third)
            for d in (2, 1, 3, 0):
                v = step_to(a3, d)
                dev = me + moved(a3, v) + half - core
                src, dst = Ob.at[cls, pl.ds(half * CAP, CAP), v], Hb.at[cls, core, :, pos[a3]]
                if d == 0:
                    @pl.when(e == 0)
                    def _():
                        local(src, dst, d5r.at[e, cls]).start()

                    @pl.when(e != 0)
                    def _():
                        remote(src, dst, d5s, d5r.at[e, cls], dev).start()
                else:
                    remote(src, dst, d5s, d5r.at[e, cls], dev).start()
        return 0

    lax.fori_loop(0, 2, expert, 0)

    u2, v3 = pi // 16 % 4, pi // 4 % 4
    by_second = as_onehot(pj == pi // 64 * 64 + v3 * 16 + u2 * 4 + pi % 4)

    def regroup(e, _):
        half = (core + e) % 2
        for cls, (a1, a2, a3) in enumerate(CLASSES):
            wait_bytes(Hb.at[cls, half], d5r.at[e, cls])
            rows_in = Hb[cls, half].reshape(CAP * 64, third)
            Z[cls, half] = jnp.concatenate([dot(by_second, rows_in[i:i + blk]).astype(BF16) for i in
                                            range(0, CAP * 64, blk)], axis=0).reshape(CAP, RING, 16, third)
            for d in (2, 1, 3, 0):
                v = step_to(a2, d)
                src, dst = Z.at[cls, half, :, v], F.at[cls, half, :, pos[a2]]
                if d == 0:
                    local(src, dst, d6r.at[e, cls]).start()
                else:
                    remote(src, dst, d6s, d6r.at[e, cls], me + moved(a2, v)).start()
        return 0

    lax.fori_loop(0, 2, regroup, 0)

    wait_bytes(Cr.at[:, 0:3], cr.at[0])

    def spreads(half):
        ei, ej = iota((128, 256), 0), iota((128, 256), 1)
        q = ej // 16 % 4 * 8 + half * 4 + ej // 4 % 4
        return [as_onehot(ei == q + 32 * part) for part in range(4)]

    def weigh(cls, half, spread_mats, targets):
        m = tokens * len(targets)
        lane_pos = iota((m, 256), 1)
        c = jnp.concatenate([Cr[cls, v] for v in targets], axis=0)
        w_exp = [dot(c, spread_mats[part]) for part in range(3)]
        source = jnp.concatenate([jnp.full((tokens, 256), v, jnp.int32) for v in targets], axis=0)
        rank_exp = jnp.where(lane_pos % 4 == source, dot(c, spread_mats[3]) - (lane_pos // 64).astype(F32), 99.0)
        acc = jnp.zeros((3 * m, third), F32)
        for r0 in range(0, CAP, 4):
            k = 64 * min(4, CAP - r0)
            hit = rank_exp == float(r0)
            w = jnp.concatenate([jnp.where(hit, w_exp[part], 0.0) for part in range(3)], axis=0).astype(BF16)
            acc = acc + dot(w[:, :k], F[cls, half, r0:r0 + k // 64].reshape(k, third))
        return (acc[2 * m:] + acc[m:2 * m] + acc[:m]).reshape(len(targets), tokens, third)

    mats = spreads(core)
    for cls in range(3):
        wait_bytes(F.at[cls, core], d6r.at[0, cls])
        U[cls] = weigh(cls, core, mats, list(range(RING)))
    mats = spreads(1 - core)
    for group in ((2,), (1, 3), (0,)):
        for cls, (a1, a2, a3) in enumerate(CLASSES):
            if group == (2,):
                wait_bytes(F.at[cls, 1 - core], d6r.at[1, cls])
            targets = [step_to(a1, d) for d in group]
            part = weigh(cls, 1 - core, mats, targets)
            for i, (d, v) in enumerate(zip(group, targets)):
                if d == 0:
                    A[cls, pos[a1]] = U[cls, v] + part[i]
                else:
                    U[cls, v] = U[cls, v] + part[i]
                    remote(U.at[cls, v], A.at[cls, pos[a1]], d7s, d7r.at[cls], me + moved(a1, v)).start()
    for cls in range(3):
        wait_bytes(A.at[cls, 0:3], d7r.at[cls])
        routed = (A[cls, 0] + A[cls, 1]) + (A[cls, 2] + A[cls, 3])
        y_ref[:, cls * third:(cls + 1) * third] = (zs[:, cls * third:(cls + 1) * third] + routed).astype(BF16)

    for ref, sem in ((T.at[:, 0, 0:3], t1s), (T.at[:, 0:3], t2s), (G.at[:, :, 0, 0:3], g1s), (G.at[:, :, 0:3], g2s),
                     (Cs.at[:, 0:3], cs), (Sb.at[:, :, 0:7], d3s), (Sb.at[:, :, 0:7], d5s), (Z.at[:, :, :, 0:3], d6s),
                     (U.at[:, 0:3], d7s)):
        wait_bytes(ref, sem)


def solution(mesh):
    def device_step(x_tokens, slot_expert, w1_slots, w3_slots, w2_slots, assign, w_router, w1_shared, w3_shared, w2_shared):
        tokens, dim = x_tokens.shape
        third = dim // 3
        slots = slot_expert.shape[0]
        vmem = pl.BlockSpec(memory_space=pltpu.VMEM)
        hbm = pl.BlockSpec(memory_space=pltpu.HBM)
        dma = pltpu.SemaphoreType.DMA
        V = pltpu.VMEM
        return pl.pallas_call(
            moe_kernel,
            out_shape=jax.ShapeDtypeStruct((tokens, dim), BF16),
            in_specs=[hbm] * 10,
            out_specs=vmem,
            scratch_shapes=[
                V((tokens, dim), BF16), V(assign.T.shape, jnp.int32), V((1, slots), jnp.int32), V(w_router.T.shape, BF16),
                V((3, 2, RING, RING, tokens, third // 2), BF16),
                V((3, RING, RING, 16, slots), BF16),
                V((16, slots), BF16),
                V((2, 3, 2, 2 * CAP * 8, 8 * tokens), F32),
                V((3, 2, 8, CAP, 16, third // 2), BF16),
                V((3, 2, 2 * CAP, RING, 16, third // 2), BF16),
                V((3, 2 * CAP, RING, 16, third), BF16),
                V((3, 2, CAP, RING, 16, third), BF16),
                V((3, 2, CAP, RING, 16, third), BF16),
                V((3, 2, CAP, RING, 16, third), BF16),
                V((3, RING, tokens, 128), BF16), V((3, RING, tokens, 128), BF16),
                V((3, RING, tokens, third), F32), V((3, RING, tokens, third), F32),
                V((tokens, dim), F32),
                V(w1_slots.shape[1:], BF16), V(w3_slots.shape[1:], BF16), V(w2_slots.shape[1:], BF16),
                V(w1_shared.shape, BF16), V(w3_shared.shape, BF16), V(w2_shared.shape, BF16),
                dma((6,)), dma((4,)), dma((9,)), dma((1,)), dma((1,)), dma((1,)), dma((2, 3)), dma((2,)), dma((1,)),
                dma((2, 2)), dma((2, 3)), dma((2, 3)), dma((3,)),
            ],
            compiler_params=pltpu.CompilerParams(collective_id=0, has_side_effects=True,
                                                 vmem_limit_bytes=54950 * 1024),
        )(x_tokens, assign.T, slot_expert.reshape(1, -1), w_router.T, w1_slots, w3_slots, w2_slots,
          w1_shared, w3_shared, w2_shared)

    token_spec = P(('dp', 'ep'), None)
    slot_spec = P('ep', None, None)
    return jax.shard_map(device_step, mesh=mesh,
                         in_specs=(token_spec, P(), slot_spec, slot_spec, slot_spec, token_spec, P(), P(), P(), P()),
                         out_specs=token_spec, check_vma=False)
```

```python
import jax
import jax.numpy as jnp
from jax import lax
from jax.experimental import pallas as pl
from jax.experimental.pallas import tpu as pltpu
from jax.sharding import PartitionSpec as P

ROUTE_SCALE = 2.5
RING = 4
CAP = 9
BF16 = jnp.bfloat16
F32 = jnp.float32
STRIDE = {'x': 2, 'y': 8, 'z': 32}
CLASSES = (('y', 'z', 'x'), ('z', 'x', 'y'), ('x', 'y', 'z'))


def iota(shape, dim):
    return lax.broadcasted_iota(jnp.int32, shape, dim)


def dot(a, b):
    return jnp.dot(a, b, preferred_element_type=F32)


def dot_t(a, b):
    return lax.dot_general(a, b, (((1,), (1,)), ((), ())), preferred_element_type=F32)


def as_onehot(cond):
    return jnp.where(cond, 1.0, 0.0).astype(BF16)


def three_parts(v):
    hi = v.astype(BF16)
    rest = v - hi.astype(F32)
    mid = rest.astype(BF16)
    lo = (rest - mid.astype(F32)).astype(BF16)
    return hi, mid, lo


def moe_kernel(x_hbm, assign_hbm, slot_expert_hbm, wr_hbm, w1_hbm, w3_hbm, w2_hbm, s1_hbm, s3_hbm, s2_hbm, y_ref,
               x_ref, assign_ref, slot_expert_ref, wr_ref,
               G, T, tab, Pm, Sb, R, Ob, Hb, Z, F, Cs, Cr, U, A, zs, w1, w3, w2, s1, s3, s2,
               wsem, isem, sent, t1r, t2r, g0r, g1r, g2r, cr, d3r, d5r, d6r, d7r):
    t1s, t2s, g1s, g2s, cs, d3s, d5s, d6s, d7s = (sent.at[i] for i in range(9))
    me = lax.axis_index('ep')
    core = me % 2
    pos = {'x': (me // 2) % RING, 'y': (me // 8) % RING, 'z': me // 32}
    third = x_ref.shape[1] // 3
    sixth = third // 2

    def moved(axis, value):
        return (value - pos[axis]) * STRIDE[axis]

    def step_to(axis, d):
        return (pos[axis] + d) % RING

    def remote(src, dst, ssem, rsem, dev):
        return pltpu.make_async_remote_copy(src_ref=src, dst_ref=dst, send_sem=ssem, recv_sem=rsem,
                                            device_id={'ep': dev}, device_id_type=pl.DeviceIdType.MESH)

    def local(src, dst, sem):
        return pltpu.make_async_copy(src, dst, sem)

    def wait_bytes(ref, sem):
        pltpu.make_async_copy(ref, ref, sem).wait()

    barrier = pltpu.get_barrier_semaphore()

    def greet(dev):
        pl.semaphore_signal(barrier, inc=1, device_id={'ep': dev}, device_id_type=pl.DeviceIdType.MESH)

    other = 1 - 2 * core
    greet(me + other)
    for axis in 'xyz':
        for d in range(1, RING):
            dev = me + moved(axis, step_to(axis, d))
            greet(dev)
            greet(dev + other)

    input_copies = [local(s, d, isem.at[i]) for i, (s, d) in enumerate(
        ((assign_hbm, assign_ref), (x_hbm, x_ref), (slot_expert_hbm, slot_expert_ref), (wr_hbm, wr_ref)))]
    for c in input_copies:
        c.start()
    expert_weights = [(w2_hbm.at[0], w2, 3)]
    for g in range(2):
        for cls in range(3):
            src, dst = pl.ds((2 * cls + g) * sixth, sixth), pl.ds((3 * g + cls) * sixth, sixth)
            expert_weights += [(w1_hbm.at[0, src], w1.at[dst], 4), (w3_hbm.at[0, src], w3.at[dst], 5)]
    weight_copies = [local(s, d, wsem.at[i]) for s, d, i in
                     [(s1_hbm, s1, 0), (s3_hbm, s3, 1), (s2_hbm, s2, 2)] + expert_weights]

    input_copies[0].wait()
    tokens = x_ref.shape[0]
    slots = slot_expert_ref.shape[1]
    slot_row = iota((slots, tokens), 0)
    chosen_t = jnp.zeros((slots, tokens), F32)
    for k in range(assign_ref.shape[0]):
        chosen_t = chosen_t + jnp.where(assign_ref[k:k + 1, :] == slot_row, 1.0, 0.0)
    ti, tj = iota((tokens, tokens), 0), iota((tokens, tokens), 1)
    chosen = dot_t(as_onehot(ti == tj), chosen_t.astype(BF16))
    rank = jnp.where(chosen > 0.5, dot(as_onehot(tj < ti), chosen.astype(BF16)), 99.0)
    token_id = (iota((tokens, slots), 0) + 1).astype(F32)
    tab_rows = [jnp.sum(jnp.where(rank == float(r), token_id, 0.0), axis=0, keepdims=True) for r in range(CAP)]
    tab[...] = jnp.concatenate(tab_rows + [jnp.zeros((16 - CAP, slots), F32)], axis=0).astype(BF16)

    for c in input_copies[1:]:
        c.wait()
    pl.semaphore_wait(barrier, 19)

    def cols(cls, g):
        return x_ref.at[:, pl.ds((2 * cls + g) * sixth, sixth)]

    def spread(cls, g, k, src, to):
        a2 = CLASSES[cls][1]
        for d in (1, 3, 2):
            remote(src, G.at[cls, g, pos[a2], to], g2s, g2r.at[g],
                   me + moved(a2, step_to(a2, d))).start()

    for g in range(2):
        for cls, (a1, a2, a3) in enumerate(CLASSES):
            for d in (1, 3, 2):
                dev = me + moved(a1, step_to(a1, d))
                if g == 0:
                    remote(tab, T.at[cls, pos[a2], pos[a1]], t1s, t1r.at[0], dev).start()
                remote(cols(cls, g), G.at[cls, g, pos[a2], pos[a1]], g1s, g1r.at[g, d - 1], dev).start()
        for cls, (a1, a2, a3) in enumerate(CLASSES):
            spread(cls, g, 0, cols(cls, g), pos[a1])
            local(cols(cls, g), G.at[cls, g, pos[a2], pos[a1]], g0r.at[0]).start()
            if g == 0:
                T[cls, pos[a2], pos[a1]] = tab[...]

    for c in weight_copies:
        c.start()

    gate = jax.nn.sigmoid(dot_t(x_ref[...], wr_ref[...]))
    num_experts = wr_ref.shape[0]
    slot_of = as_onehot(iota((num_experts, slots), 0) == slot_expert_ref[...])
    gate_slot = sum(dot(p, slot_of) for p in three_parts(gate))
    picked = jnp.where(chosen > 0.5, gate_slot, 0.0)
    route = ROUTE_SCALE * picked / jnp.maximum(jnp.sum(picked, axis=1, keepdims=True), 1e-30)
    route_rank = jnp.concatenate(three_parts(route) + (rank.astype(BF16),), axis=1)

    for g in range(2):
        for d in (3, 1, 2):
            wait_bytes(G.at[:, g, 0, 0], g1r.at[g, d - 1])
            for cls, (a1, a2, a3) in enumerate(CLASSES):
                owner = (pos[a1] + RING - d) % RING
                spread(cls, g, d, G.at[cls, g, pos[a2], owner], owner)
        if g == 0:
            wait_bytes(T.at[:, 0, 0:3], t1r.at[0])
            for cls, (a1, a2, a3) in enumerate(CLASSES):
                row = T.at[cls, pos[a2]]
                for d in (1, 3, 2):
                    remote(row, row, t2s, t2r.at[0], me + moved(a2, step_to(a2, d))).start()

    si, sj = iota((4 * slots, 128), 0), iota((4 * slots, 128), 1)
    for cls, (a1, a2, a3) in enumerate(CLASSES):
        q_slot = (sj // 32 * slots + sj // 8 % 4 * STRIDE[a2] + sj // 4 % 2 + sj % 4 * STRIDE[a3])
        for v in range(RING):
            Cs[cls, v] = dot(route_rank, as_onehot(si == q_slot + v * STRIDE[a1])).astype(BF16)

    for c in weight_copies[:3]:
        c.wait()
    ff_shared = s1.shape[1]
    step = 512
    acc = jnp.zeros((tokens, x_ref.shape[1]), F32)
    for f in range(0, ff_shared, step):
        xs = x_ref[...]
        mid = (jax.nn.silu(dot(xs, s1[:, f:f + step])) * dot(xs, s3[:, f:f + step])).astype(BF16)
        acc = acc + dot(mid, s2[f:f + step, :])
    zs[...] = acc

    rows = CAP * 8
    qi, qj = iota((rows, 256), 0), iota((rows, 256), 1)
    by_rank = [as_onehot(qj == (qi % 8 + 8 * h) * 16 + qi // 8) for h in range(2)]
    src_base = ((iota((rows, 128), 0) % 8) * tokens).astype(F32)
    lane = iota((rows, 128), 1).astype(F32)
    tabs, lines = [], []

    wait_bytes(G.at[:, :, 0, 0], g0r.at[0])
    wait_bytes(G.at[:, 0, 0:3], g2r.at[0])
    wait_bytes(T.at[:, 0:3], t2r.at[0])
    for cls, (a1, a2, a3) in enumerate(CLASSES):
        tabs.append([dot(m, T[cls].reshape(256, slots)).astype(BF16) for m in by_rank])
        lines.append(me - core - pos[a3] * STRIDE[a3])

    def select(n, _):
        g, e, p = n // 2 % 2, n // 4, n % 2

        @pl.when(n == 2)
        def _():
            wait_bytes(G.at[:, 1, 0:3], g2r.at[1])

        @pl.when(g == 0)
        def _():
            for cls, (a1, a2, a3) in enumerate(CLASSES):
                for q in range(2):
                    d = 2 + q - p * (1 + 2 * q)
                    slot = lines[cls] + step_to(a3, d) * STRIDE[a3] + (core + e) % 2
                    pick = as_onehot(iota((slots, 128), 0) == slot)
                    for h in range(2):
                        val = dot(tabs[cls][h], pick)
                        code = jnp.where(val > 0.5, val - 1.0 + src_base, -1.0)
                        for b in range(8 * tokens // 128):
                            Pm[p, cls, h, q * rows:(q + 1) * rows, b * 128:(b + 1) * 128] = (
                                jnp.where(code == lane + float(b * 128), 1.0, 0.0))

        for cls, (a1, a2, a3) in enumerate(CLASSES):
            outs = []
            for h in range(2):
                out = dot(Pm[p, cls, h].astype(BF16), G[cls, g, 2 * h:2 * h + 2].reshape(8 * tokens, sixth))
                outs.append(out.reshape(2, CAP, 8, sixth))
            both = jnp.concatenate(outs, axis=2).astype(BF16)
            for q in range(2):
                d = 2 + q - p * (1 + 2 * q)
                k = 2 * d + e
                Sb[cls, g, k] = both[q]
                dev = me + moved(a3, step_to(a3, d)) + (core + e) % 2 - core
                src, dst = Sb.at[cls, g, k], R.at[cls, g, pl.ds(core * CAP, CAP), pos[a3]]
                if q == 1:
                    mine = jnp.logical_and(n < 4, n % 2 == 1)

                    @pl.when(mine)
                    def _():
                        local(src, dst, d3r.at[e, g]).start()

                    @pl.when(jnp.logical_not(mine))
                    def _():
                        remote(src, dst, d3s, d3r.at[e, g], dev).start()
                else:
                    remote(src, dst, d3s, d3r.at[e, g], dev).start()
        return 0

    lax.fori_loop(0, 2 * RING, select, 0)

    for cls, (a1, a2, a3) in enumerate(CLASSES):
        for d in (1, 3, 2, 0):
            v = step_to(a1, d)
            if d == 0:
                Cr[cls, pos[a1]] = Cs[cls, v]
            else:
                remote(Cs.at[cls, v], Cr.at[cls, pos[a1]], cs, cr.at[0], me + moved(a1, v)).start()

    for w, i in ((w2, 3), (w1, 4), (w3, 5)):
        wait_bytes(w, wsem.at[i])
    blk = 3 * 64
    pi, pj = iota((blk, blk), 0), iota((blk, blk), 1)

    def bits(v):
        return v // 16 % 4, v // 4 % 4, v % 4

    ix, iz, iy = bits(pi)
    jx, jz, jy = bits(pj)
    to_first = {1: as_onehot(pj == pi // 64 * 64 + iy * 16 + ix * 4 + iz),
                2: as_onehot(pj == pi // 64 * 64 + iz * 16 + iy * 4 + ix)}
    from_first = {1: as_onehot(pi == pj // 64 * 64 + jy * 16 + jx * 4 + jz),
                  2: as_onehot(pi == pj // 64 * 64 + jz * 16 + jy * 4 + jx)}

    def permuted(mats, cls, value):
        if cls == 0:
            return value
        return jnp.concatenate([dot(mats[cls], value[i:i + blk]).astype(BF16)
                                for i in range(0, value.shape[0], blk)], axis=0)

    def expert(e, _):
        half = (core + e) % 2
        n = CAP * 64
        h_gate = h_up = 0.0
        for g in range(2):
            wait_bytes(R.at[:, g, 0:CAP], d3r.at[e, g])
            xs = jnp.concatenate([permuted(to_first, cls, R[cls, g, pl.ds(half * CAP, CAP)].reshape(n, sixth))
                                  for cls in range(3)], axis=1)
            part = slice(3 * g * sixth, 3 * (g + 1) * sixth)
            h_gate = h_gate + dot(xs, w1[part])
            h_up = h_up + dot(xs, w3[part])
        mid = (jax.nn.silu(h_gate) * h_up).astype(BF16)
        for cls, (a1, a2, a3) in enumerate(CLASSES):
            out = dot(mid, w2[:, cls * third:(cls + 1) * third]).astype(BF16)
            Ob[cls, pl.ds(half * CAP, CAP)] = permuted(from_first, cls, out).reshape(CAP, RING, 16, third)
            for d in (2, 1, 3, 0):
                v = step_to(a3, d)
                dev = me + moved(a3, v) + half - core
                src, dst = Ob.at[cls, pl.ds(half * CAP, CAP), v], Hb.at[cls, core, :, pos[a3]]
                if d == 0:
                    @pl.when(e == 0)
                    def _():
                        local(src, dst, d5r.at[e, cls]).start()

                    @pl.when(e != 0)
                    def _():
                        remote(src, dst, d5s, d5r.at[e, cls], dev).start()
                else:
                    remote(src, dst, d5s, d5r.at[e, cls], dev).start()
        return 0

    lax.fori_loop(0, 2, expert, 0)

    u2, v3 = pi // 16 % 4, pi // 4 % 4
    by_second = as_onehot(pj == pi // 64 * 64 + v3 * 16 + u2 * 4 + pi % 4)

    def regroup(e, _):
        half = (core + e) % 2
        for cls, (a1, a2, a3) in enumerate(CLASSES):
            wait_bytes(Hb.at[cls, half], d5r.at[e, cls])
            rows_in = Hb[cls, half].reshape(CAP * 64, third)
            Z[cls, half] = jnp.concatenate([dot(by_second, rows_in[i:i + blk]).astype(BF16) for i in
                                            range(0, CAP * 64, blk)], axis=0).reshape(CAP, RING, 16, third)
            for d in (2, 1, 3, 0):
                v = step_to(a2, d)
                src, dst = Z.at[cls, half, :, v], F.at[cls, half, :, pos[a2]]
                if d == 0:
                    local(src, dst, d6r.at[e, cls]).start()
                else:
                    remote(src, dst, d6s, d6r.at[e, cls], me + moved(a2, v)).start()
        return 0

    lax.fori_loop(0, 2, regroup, 0)

    wait_bytes(Cr.at[:, 0:3], cr.at[0])

    def spreads(half):
        ei, ej = iota((128, 256), 0), iota((128, 256), 1)
        q = ej // 16 % 4 * 8 + half * 4 + ej // 4 % 4
        return [as_onehot(ei == q + 32 * part) for part in range(4)]

    def weigh(cls, half, spread_mats, targets):
        m = tokens * len(targets)
        lane_pos = iota((m, 256), 1)
        c = jnp.concatenate([Cr[cls, v] for v in targets], axis=0)
        w_exp = [dot(c, spread_mats[part]) for part in range(3)]
        source = jnp.concatenate([jnp.full((tokens, 256), v, jnp.int32) for v in targets], axis=0)
        rank_exp = jnp.where(lane_pos % 4 == source, dot(c, spread_mats[3]) - (lane_pos // 64).astype(F32), 99.0)
        acc = jnp.zeros((3 * m, third), F32)
        for r0 in range(0, CAP, 4):
            k = 64 * min(4, CAP - r0)
            hit = rank_exp == float(r0)
            w = jnp.concatenate([jnp.where(hit, w_exp[part], 0.0) for part in range(3)], axis=0).astype(BF16)
            acc = acc + dot(w[:, :k], F[cls, half, r0:r0 + k // 64].reshape(k, third))
        return (acc[2 * m:] + acc[m:2 * m] + acc[:m]).reshape(len(targets), tokens, third)

    mats = spreads(core)
    for cls in range(3):
        wait_bytes(F.at[cls, core], d6r.at[0, cls])
        U[cls] = weigh(cls, core, mats, list(range(RING)))
    mats = spreads(1 - core)
    for group in ((2,), (1, 3), (0,)):
        for cls, (a1, a2, a3) in enumerate(CLASSES):
            if group == (2,):
                wait_bytes(F.at[cls, 1 - core], d6r.at[1, cls])
            targets = [step_to(a1, d) for d in group]
            part = weigh(cls, 1 - core, mats, targets)
            for i, (d, v) in enumerate(zip(group, targets)):
                if d == 0:
                    A[cls, pos[a1]] = U[cls, v] + part[i]
                else:
                    U[cls, v] = U[cls, v] + part[i]
                    remote(U.at[cls, v], A.at[cls, pos[a1]], d7s, d7r.at[cls], me + moved(a1, v)).start()
    for cls in range(3):
        wait_bytes(A.at[cls, 0:3], d7r.at[cls])
        routed = (A[cls, 0] + A[cls, 1]) + (A[cls, 2] + A[cls, 3])
        y_ref[:, cls * third:(cls + 1) * third] = (zs[:, cls * third:(cls + 1) * third] + routed).astype(BF16)

    for ref, sem in ((T.at[:, 0, 0:3], t1s), (T.at[:, 0:3], t2s), (G.at[:, :, 0, 0:3], g1s), (G.at[:, :, 0:3], g2s),
                     (Cs.at[:, 0:3], cs), (Sb.at[:, :, 0:7], d3s), (Sb.at[:, :, 0:7], d5s), (Z.at[:, :, :, 0:3], d6s),
                     (U.at[:, 0:3], d7s)):
        wait_bytes(ref, sem)


def solution(mesh):
    def device_step(x_tokens, slot_expert, w1_slots, w3_slots, w2_slots, assign, w_router, w1_shared, w3_shared, w2_shared):
        tokens, dim = x_tokens.shape
        third = dim // 3
        slots = slot_expert.shape[0]
        vmem = pl.BlockSpec(memory_space=pltpu.VMEM)
        hbm = pl.BlockSpec(memory_space=pltpu.HBM)
        dma = pltpu.SemaphoreType.DMA
        V = pltpu.VMEM
        return pl.pallas_call(
            moe_kernel,
            out_shape=jax.ShapeDtypeStruct((tokens, dim), BF16),
            in_specs=[hbm] * 10,
            out_specs=vmem,
            scratch_shapes=[
                V((tokens, dim), BF16), V(assign.T.shape, jnp.int32), V((1, slots), jnp.int32), V(w_router.T.shape, BF16),
                V((3, 2, RING, RING, tokens, third // 2), BF16),
                V((3, RING, RING, 16, slots), BF16),
                V((16, slots), BF16),
                V((2, 3, 2, 2 * CAP * 8, 8 * tokens), F32),
                V((3, 2, 8, CAP, 16, third // 2), BF16),
                V((3, 2, 2 * CAP, RING, 16, third // 2), BF16),
                V((3, 2 * CAP, RING, 16, third), BF16),
                V((3, 2, CAP, RING, 16, third), BF16),
                V((3, 2, CAP, RING, 16, third), BF16),
                V((3, 2, CAP, RING, 16, third), BF16),
                V((3, RING, tokens, 128), BF16), V((3, RING, tokens, 128), BF16),
                V((3, RING, tokens, third), F32), V((3, RING, tokens, third), F32),
                V((tokens, dim), F32),
                V(w1_slots.shape[1:], BF16), V(w3_slots.shape[1:], BF16), V(w2_slots.shape[1:], BF16),
                V(w1_shared.shape, BF16), V(w3_shared.shape, BF16), V(w2_shared.shape, BF16),
                dma((6,)), dma((4,)), dma((9,)), dma((1,)), dma((1,)), dma((1,)), dma((2, 3)), dma((2,)), dma((1,)),
                dma((2, 2)), dma((2, 3)), dma((2, 3)), dma((3,)),
            ],
            compiler_params=pltpu.CompilerParams(collective_id=0, has_side_effects=True,
                                                 vmem_limit_bytes=54950 * 1024),
        )(x_tokens, assign.T, slot_expert.reshape(1, -1), w_router.T, w1_slots, w3_slots, w2_slots,
          w1_shared, w3_shared, w2_shared)

    token_spec = P(('dp', 'ep'), None)
    slot_spec = P('ep', None, None)
    return jax.shard_map(device_step, mesh=mesh,
                         in_specs=(token_spec, P(), slot_spec, slot_spec, slot_spec, token_spec, P(), P(), P(), P()),
                         out_specs=token_spec, check_vma=False)
```

```python
import jax
import jax.numpy as jnp
from jax import lax
from jax.experimental import pallas as pl
from jax.experimental.pallas import tpu as pltpu
from jax.sharding import PartitionSpec as P

ROUTE_SCALE = 2.5
RING = 4
CAP = 9
BF16 = jnp.bfloat16
F32 = jnp.float32
STRIDE = {'x': 2, 'y': 8, 'z': 32}
CLASSES = (('y', 'z', 'x'), ('z', 'x', 'y'), ('x', 'y', 'z'))


def iota(shape, dim):
    return lax.broadcasted_iota(jnp.int32, shape, dim)


def dot(a, b):
    return jnp.dot(a, b, preferred_element_type=F32)


def dot_t(a, b):
    return lax.dot_general(a, b, (((1,), (1,)), ((), ())), preferred_element_type=F32)


def as_onehot(cond):
    return jnp.where(cond, 1.0, 0.0).astype(BF16)


def three_parts(v):
    hi = v.astype(BF16)
    rest = v - hi.astype(F32)
    mid = rest.astype(BF16)
    lo = (rest - mid.astype(F32)).astype(BF16)
    return hi, mid, lo


def moe_kernel(x_hbm, assign_hbm, slot_expert_hbm, wr_hbm, w1_hbm, w3_hbm, w2_hbm, s1_hbm, s3_hbm, s2_hbm, y_ref,
               x_ref, assign_ref, slot_expert_ref, wr_ref,
               G, T, tab, Pm, Sb, R, Ob, Hb, Z, F, Cs, Cr, U, A, zs, w1, w3, w2, s1, s3, s2,
               wsem, isem, sent, t1r, t2r, g0r, g1r, g2r, cr, d3r, d5r, d6r, d7r):
    t1s, t2s, g1s, g2s, cs, d3s, d5s, d6s, d7s = (sent.at[i] for i in range(9))
    me = lax.axis_index('ep')
    core = me % 2
    pos = {'x': (me // 2) % RING, 'y': (me // 8) % RING, 'z': me // 32}
    third = x_ref.shape[1] // 3
    sixth = third // 2

    def moved(axis, value):
        return (value - pos[axis]) * STRIDE[axis]

    def step_to(axis, d):
        return (pos[axis] + d) % RING

    def remote(src, dst, ssem, rsem, dev):
        return pltpu.make_async_remote_copy(src_ref=src, dst_ref=dst, send_sem=ssem, recv_sem=rsem,
                                            device_id={'ep': dev}, device_id_type=pl.DeviceIdType.MESH)

    def local(src, dst, sem):
        return pltpu.make_async_copy(src, dst, sem)

    def wait_bytes(ref, sem):
        pltpu.make_async_copy(ref, ref, sem).wait()

    barrier = pltpu.get_barrier_semaphore()

    def greet(dev):
        pl.semaphore_signal(barrier, inc=1, device_id={'ep': dev}, device_id_type=pl.DeviceIdType.MESH)

    other = 1 - 2 * core
    greet(me + other)
    for axis in 'xyz':
        for d in range(1, RING):
            dev = me + moved(axis, step_to(axis, d))
            greet(dev)
            greet(dev + other)

    input_copies = [local(s, d, isem.at[i]) for i, (s, d) in enumerate(
        ((assign_hbm, assign_ref), (x_hbm, x_ref), (slot_expert_hbm, slot_expert_ref), (wr_hbm, wr_ref)))]
    for c in input_copies:
        c.start()
    expert_weights = [(w2_hbm.at[0], w2, 3)]
    for g in range(2):
        for cls in range(3):
            src, dst = pl.ds((2 * cls + g) * sixth, sixth), pl.ds((3 * g + cls) * sixth, sixth)
            expert_weights += [(w1_hbm.at[0, src], w1.at[dst], 4), (w3_hbm.at[0, src], w3.at[dst], 5)]
    weight_copies = [local(s, d, wsem.at[i]) for s, d, i in
                     [(s1_hbm, s1, 0), (s3_hbm, s3, 1), (s2_hbm, s2, 2)] + expert_weights]

    input_copies[0].wait()
    tokens = x_ref.shape[0]
    slots = slot_expert_ref.shape[1]
    slot_row = iota((slots, tokens), 0)
    chosen_t = jnp.zeros((slots, tokens), F32)
    for k in range(assign_ref.shape[0]):
        chosen_t = chosen_t + jnp.where(assign_ref[k:k + 1, :] == slot_row, 1.0, 0.0)
    ti, tj = iota((tokens, tokens), 0), iota((tokens, tokens), 1)
    chosen = dot_t(as_onehot(ti == tj), chosen_t.astype(BF16))
    rank = jnp.where(chosen > 0.5, dot(as_onehot(tj < ti), chosen.astype(BF16)), 99.0)
    token_id = (iota((tokens, slots), 0) + 1).astype(F32)
    tab_rows = [jnp.sum(jnp.where(rank == float(r), token_id, 0.0), axis=0, keepdims=True) for r in range(CAP)]
    tab[...] = jnp.concatenate(tab_rows + [jnp.zeros((16 - CAP, slots), F32)], axis=0).astype(BF16)

    for c in input_copies[1:]:
        c.wait()
    pl.semaphore_wait(barrier, 19)

    def cols(cls, g):
        return x_ref.at[:, pl.ds((2 * cls + g) * sixth, sixth)]

    def spread(cls, g, k, src, to):
        a2 = CLASSES[cls][1]
        for d in (1, 3, 2):
            remote(src, G.at[cls, g, pos[a2], to], g2s, g2r.at[g],
                   me + moved(a2, step_to(a2, d))).start()

    for g in range(2):
        for cls, (a1, a2, a3) in enumerate(CLASSES):
            for d in (1, 3, 2):
                dev = me + moved(a1, step_to(a1, d))
                if g == 0:
                    remote(tab, T.at[cls, pos[a2], pos[a1]], t1s, t1r.at[0], dev).start()
                remote(cols(cls, g), G.at[cls, g, pos[a2], pos[a1]], g1s, g1r.at[g, d - 1], dev).start()
        for cls, (a1, a2, a3) in enumerate(CLASSES):
            spread(cls, g, 0, cols(cls, g), pos[a1])
            local(cols(cls, g), G.at[cls, g, pos[a2], pos[a1]], g0r.at[0]).start()
            if g == 0:
                T[cls, pos[a2], pos[a1]] = tab[...]

    for c in weight_copies:
        c.start()

    gate = jax.nn.sigmoid(dot_t(x_ref[...], wr_ref[...]))
    num_experts = wr_ref.shape[0]
    slot_of = as_onehot(iota((num_experts, slots), 0) == slot_expert_ref[...])
    gate_slot = sum(dot(p, slot_of) for p in three_parts(gate))
    picked = jnp.where(chosen > 0.5, gate_slot, 0.0)
    route = ROUTE_SCALE * picked / jnp.maximum(jnp.sum(picked, axis=1, keepdims=True), 1e-30)
    route_rank = jnp.concatenate(three_parts(route) + (rank.astype(BF16),), axis=1)

    for g in range(2):
        for d in (3, 1, 2):
            wait_bytes(G.at[:, g, 0, 0], g1r.at[g, d - 1])
            for cls, (a1, a2, a3) in enumerate(CLASSES):
                owner = (pos[a1] + RING - d) % RING
                spread(cls, g, d, G.at[cls, g, pos[a2], owner], owner)
        if g == 0:
            wait_bytes(T.at[:, 0, 0:3], t1r.at[0])
            for cls, (a1, a2, a3) in enumerate(CLASSES):
                row = T.at[cls, pos[a2]]
                for d in (1, 3, 2):
                    remote(row, row, t2s, t2r.at[0], me + moved(a2, step_to(a2, d))).start()

    si, sj = iota((4 * slots, 128), 0), iota((4 * slots, 128), 1)
    for cls, (a1, a2, a3) in enumerate(CLASSES):
        q_slot = (sj // 32 * slots + sj // 8 % 4 * STRIDE[a2] + sj // 4 % 2 + sj % 4 * STRIDE[a3])
        for v in range(RING):
            Cs[cls, v] = dot(route_rank, as_onehot(si == q_slot + v * STRIDE[a1])).astype(BF16)

    for c in weight_copies[:3]:
        c.wait()
    ff_shared = s1.shape[1]
    step = 512
    acc = jnp.zeros((tokens, x_ref.shape[1]), F32)
    for f in range(0, ff_shared, step):
        xs = x_ref[...]
        mid = (jax.nn.silu(dot(xs, s1[:, f:f + step])) * dot(xs, s3[:, f:f + step])).astype(BF16)
        acc = acc + dot(mid, s2[f:f + step, :])
    zs[...] = acc

    rows = CAP * 8
    qi, qj = iota((rows, 256), 0), iota((rows, 256), 1)
    by_rank = [as_onehot(qj == (qi % 8 + 8 * h) * 16 + qi // 8) for h in range(2)]
    src_base = ((iota((rows, 128), 0) % 8) * tokens).astype(F32)
    lane = iota((rows, 128), 1).astype(F32)
    tabs, lines = [], []

    wait_bytes(G.at[:, :, 0, 0], g0r.at[0])
    wait_bytes(G.at[:, 0, 0:3], g2r.at[0])
    wait_bytes(T.at[:, 0:3], t2r.at[0])
    for cls, (a1, a2, a3) in enumerate(CLASSES):
        tabs.append([dot(m, T[cls].reshape(256, slots)).astype(BF16) for m in by_rank])
        lines.append(me - core - pos[a3] * STRIDE[a3])

    def select(n, _):
        g, e, p = n // 2 % 2, n // 4, n % 2

        @pl.when(n == 2)
        def _():
            wait_bytes(G.at[:, 1, 0:3], g2r.at[1])

        @pl.when(g == 0)
        def _():
            for cls, (a1, a2, a3) in enumerate(CLASSES):
                for q in range(2):
                    d = 2 + q - p * (1 + 2 * q)
                    slot = lines[cls] + step_to(a3, d) * STRIDE[a3] + (core + e) % 2
                    pick = as_onehot(iota((slots, 128), 0) == slot)
                    for h in range(2):
                        val = dot(tabs[cls][h], pick)
                        code = jnp.where(val > 0.5, val - 1.0 + src_base, -1.0)
                        for b in range(8 * tokens // 128):
                            Pm[p, cls, h, q * rows:(q + 1) * rows, b * 128:(b + 1) * 128] = (
                                jnp.where(code == lane + float(b * 128), 1.0, 0.0))

        for cls, (a1, a2, a3) in enumerate(CLASSES):
            outs = []
            for h in range(2):
                out = dot(Pm[p, cls, h].astype(BF16), G[cls, g, 2 * h:2 * h + 2].reshape(8 * tokens, sixth))
                outs.append(out.reshape(2, CAP, 8, sixth))
            both = jnp.concatenate(outs, axis=2).astype(BF16)
            for q in range(2):
                d = 2 + q - p * (1 + 2 * q)
                k = 2 * d + e
                Sb[cls, g, k] = both[q]
                dev = me + moved(a3, step_to(a3, d)) + (core + e) % 2 - core
                src, dst = Sb.at[cls, g, k], R.at[cls, g, pl.ds(core * CAP, CAP), pos[a3]]
                if q == 1:
                    mine = jnp.logical_and(n < 4, n % 2 == 1)

                    @pl.when(mine)
                    def _():
                        local(src, dst, d3r.at[e, g]).start()

                    @pl.when(jnp.logical_not(mine))
                    def _():
                        remote(src, dst, d3s, d3r.at[e, g], dev).start()
                else:
                    remote(src, dst, d3s, d3r.at[e, g], dev).start()
        return 0

    lax.fori_loop(0, 2 * RING, select, 0)

    for cls, (a1, a2, a3) in enumerate(CLASSES):
        for d in (1, 3, 2, 0):
            v = step_to(a1, d)
            if d == 0:
                Cr[cls, pos[a1]] = Cs[cls, v]
            else:
                remote(Cs.at[cls, v], Cr.at[cls, pos[a1]], cs, cr.at[0], me + moved(a1, v)).start()

    for w, i in ((w2, 3), (w1, 4), (w3, 5)):
        wait_bytes(w, wsem.at[i])
    blk = 3 * 64
    pi, pj = iota((blk, blk), 0), iota((blk, blk), 1)

    def bits(v):
        return v // 16 % 4, v // 4 % 4, v % 4

    ix, iz, iy = bits(pi)
    jx, jz, jy = bits(pj)
    to_first = {1: as_onehot(pj == pi // 64 * 64 + iy * 16 + ix * 4 + iz),
                2: as_onehot(pj == pi // 64 * 64 + iz * 16 + iy * 4 + ix)}
    from_first = {1: as_onehot(pi == pj // 64 * 64 + jy * 16 + jx * 4 + jz),
                  2: as_onehot(pi == pj // 64 * 64 + jz * 16 + jy * 4 + jx)}

    def permuted(mats, cls, value):
        if cls == 0:
            return value
        return jnp.concatenate([dot(mats[cls], value[i:i + blk]).astype(BF16)
                                for i in range(0, value.shape[0], blk)], axis=0)

    def expert(e, _):
        half = (core + e) % 2
        n = CAP * 64
        h_gate = h_up = 0.0
        for g in range(2):
            wait_bytes(R.at[:, g, 0:CAP], d3r.at[e, g])
            xs = jnp.concatenate([permuted(to_first, cls, R[cls, g, pl.ds(half * CAP, CAP)].reshape(n, sixth))
                                  for cls in range(3)], axis=1)
            part = slice(3 * g * sixth, 3 * (g + 1) * sixth)
            h_gate = h_gate + dot(xs, w1[part])
            h_up = h_up + dot(xs, w3[part])
        mid = (jax.nn.silu(h_gate) * h_up).astype(BF16)
        for cls, (a1, a2, a3) in enumerate(CLASSES):
            out = dot(mid, w2[:, cls * third:(cls + 1) * third]).astype(BF16)
            Ob[cls, pl.ds(half * CAP, CAP)] = permuted(from_first, cls, out).reshape(CAP, RING, 16, third)
            for d in (2, 1, 3, 0):
                v = step_to(a3, d)
                dev = me + moved(a3, v) + half - core
                src, dst = Ob.at[cls, pl.ds(half * CAP, CAP), v], Hb.at[cls, core, :, pos[a3]]
                if d == 0:
                    @pl.when(e == 0)
                    def _():
                        local(src, dst, d5r.at[e, cls]).start()

                    @pl.when(e != 0)
                    def _():
                        remote(src, dst, d5s, d5r.at[e, cls], dev).start()
                else:
                    remote(src, dst, d5s, d5r.at[e, cls], dev).start()
        return 0

    lax.fori_loop(0, 2, expert, 0)

    u2, v3 = pi // 16 % 4, pi // 4 % 4
    by_second = as_onehot(pj == pi // 64 * 64 + v3 * 16 + u2 * 4 + pi % 4)

    def regroup(e):
        half = (core + e) % 2
        for cls, (a1, a2, a3) in enumerate(CLASSES):
            wait_bytes(Hb.at[cls, half], d5r.at[e, cls])
            rows_in = Hb[cls, half].reshape(CAP * 64, third)
            Z[cls, half] = jnp.concatenate([dot(by_second, rows_in[i:i + blk]).astype(BF16) for i in
                                            range(0, CAP * 64, blk)], axis=0).reshape(CAP, RING, 16, third)
            parts = [pl.ds(0, third)] if e == 0 else [pl.ds(0, sixth), pl.ds(sixth, sixth)]
            for i, part in enumerate(parts):
                for d in (2, 1, 3, 0):
                    v = step_to(a2, d)
                    src, dst = Z.at[cls, half, :, v, :, part], F.at[cls, half, :, pos[a2], :, part]
                    if d == 0:
                        local(src, dst, d6r.at[e + i, cls]).start()
                    else:
                        remote(src, dst, d6s, d6r.at[e + i, cls], me + moved(a2, v)).start()
    for e in range(2):
        regroup(e)

    wait_bytes(Cr.at[:, 0:3], cr.at[0])

    def spreads(half):
        ei, ej = iota((128, 256), 0), iota((128, 256), 1)
        q = ej // 16 % 4 * 8 + half * 4 + ej // 4 % 4
        return [as_onehot(ei == q + 32 * part) for part in range(4)]

    chunks = [(r0, min(4, CAP - r0)) for r0 in range(0, CAP, 4)]

    def weights(cls, spread_mats, targets):
        lane_pos = iota((tokens * len(targets), 256), 1)
        c = jnp.concatenate([Cr[cls, v] for v in targets], axis=0)
        w_exp = [dot(c, spread_mats[part]) for part in range(3)]
        source = jnp.concatenate([jnp.full((tokens, 256), v, jnp.int32) for v in targets], axis=0)
        rank_exp = jnp.where(lane_pos % 4 == source, dot(c, spread_mats[3]) - (lane_pos // 64).astype(F32), 99.0)
        return [[jnp.where(rank_exp == float(r0), w, 0.0).astype(BF16) for w in w_exp] for r0, _ in chunks]

    def weigh(mats, rows_of, count, width):
        m = tokens * count
        acc = jnp.zeros((3 * m, width), F32)
        for (r0, k), w in zip(chunks, mats):
            acc = acc + dot(jnp.concatenate(w, axis=0)[:, :64 * k], rows_of(r0, k).reshape(64 * k, width))
        return (acc[2 * m:] + acc[m:2 * m] + acc[:m]).reshape(count, tokens, width)

    every = list(range(RING))
    first, second = spreads(core), spreads(1 - core)
    for cls in range(3):
        wait_bytes(F.at[cls, core], d6r.at[0, cls])
        U[cls] = weigh(weights(cls, first, every), lambda r0, k: F[cls, core, r0:r0 + k], RING, third)

    def place(i, part, v):
        t = (i * 3 + part) * RING + v
        return t // (2 * CAP), t % (2 * CAP)

    for cls in range(3):
        for i, mats in enumerate(weights(cls, second, every)):
            for part in range(3):
                for v in every:
                    R[(cls,) + place(i, part, v)] = mats[part][v * tokens:(v + 1) * tokens].reshape(RING, 16, sixth)
    for g in range(2):
        here = slice(g * sixth, (g + 1) * sixth)
        span = pl.ds(g * sixth, sixth)
        for group in ((2,), (1, 3, 0)):
            for cls, (a1, a2, a3) in enumerate(CLASSES):
                if group == (2,):
                    wait_bytes(F.at[cls, 1 - core, :, :, :, 0:sixth], d6r.at[1 + g, cls])
                targets = [step_to(a1, d) for d in group]
                mats = [[jnp.concatenate([R[(cls,) + place(i, part, v)].reshape(tokens, sixth) for v in targets], axis=0)
                         for part in range(3)] for i in range(len(chunks))]
                added = weigh(mats, lambda r0, k: F[cls, 1 - core, r0:r0 + k, :, :, here], len(group), sixth)
                for i, (d, v) in enumerate(zip(group, targets)):
                    if d == 0:
                        A[cls, pos[a1], :, here] = U[cls, v, :, here] + added[i]
                    else:
                        U[cls, v, :, here] = U[cls, v, :, here] + added[i]
                        remote(U.at[cls, v, :, span], A.at[cls, pos[a1], :, span], d7s, d7r.at[g, cls],
                               me + moved(a1, v)).start()
    for g in range(2):
        for cls in range(3):
            wait_bytes(A.at[cls, 0:3, :, 0:sixth], d7r.at[g, cls])
            here = slice(g * sixth, (g + 1) * sixth)
            there = slice((2 * cls + g) * sixth, (2 * cls + g + 1) * sixth)
            routed = (A[cls, 0, :, here] + A[cls, 1, :, here]) + (A[cls, 2, :, here] + A[cls, 3, :, here])
            y_ref[:, there] = (zs[:, there] + routed).astype(BF16)

    for ref, sem in ((T.at[:, 0, 0:3], t1s), (T.at[:, 0:3], t2s), (G.at[:, :, 0, 0:3], g1s), (G.at[:, :, 0:3], g2s),
                     (Cs.at[:, 0:3], cs), (Sb.at[:, :, 0:7], d3s), (Sb.at[:, :, 0:7], d5s), (Z.at[:, :, :, 0:3], d6s),
                     (U.at[:, 0:3], d7s)):
        wait_bytes(ref, sem)


def solution(mesh):
    def device_step(x_tokens, slot_expert, w1_slots, w3_slots, w2_slots, assign, w_router, w1_shared, w3_shared, w2_shared):
        tokens, dim = x_tokens.shape
        third = dim // 3
        slots = slot_expert.shape[0]
        vmem = pl.BlockSpec(memory_space=pltpu.VMEM)
        hbm = pl.BlockSpec(memory_space=pltpu.HBM)
        dma = pltpu.SemaphoreType.DMA
        V = pltpu.VMEM
        return pl.pallas_call(
            moe_kernel,
            out_shape=jax.ShapeDtypeStruct((tokens, dim), BF16),
            in_specs=[hbm] * 10,
            out_specs=vmem,
            scratch_shapes=[
                V((tokens, dim), BF16), V(assign.T.shape, jnp.int32), V((1, slots), jnp.int32), V(w_router.T.shape, BF16),
                V((3, 2, RING, RING, tokens, third // 2), BF16),
                V((3, RING, RING, 16, slots), BF16),
                V((16, slots), BF16),
                V((2, 3, 2, 2 * CAP * 8, 8 * tokens), F32),
                V((3, 2, 8, CAP, 16, third // 2), BF16),
                V((3, 2, 2 * CAP, RING, 16, third // 2), BF16),
                V((3, 2 * CAP, RING, 16, third), BF16),
                V((3, 2, CAP, RING, 16, third), BF16),
                V((3, 2, CAP, RING, 16, third), BF16),
                V((3, 2, CAP, RING, 16, third), BF16),
                V((3, RING, tokens, 128), BF16), V((3, RING, tokens, 128), BF16),
                V((3, RING, tokens, third), F32), V((3, RING, tokens, third), F32),
                V((tokens, dim), F32),
                V(w1_slots.shape[1:], BF16), V(w3_slots.shape[1:], BF16), V(w2_slots.shape[1:], BF16),
                V(w1_shared.shape, BF16), V(w3_shared.shape, BF16), V(w2_shared.shape, BF16),
                dma((6,)), dma((4,)), dma((9,)), dma((1,)), dma((1,)), dma((1,)), dma((2, 3)), dma((2,)), dma((1,)),
                dma((2, 2)), dma((2, 3)), dma((3, 3)), dma((2, 3)),
            ],
            compiler_params=pltpu.CompilerParams(collective_id=0, has_side_effects=True,
                                                 vmem_limit_bytes=54950 * 1024),
        )(x_tokens, assign.T, slot_expert.reshape(1, -1), w_router.T, w1_slots, w3_slots, w2_slots,
          w1_shared, w3_shared, w2_shared)

    token_spec = P(('dp', 'ep'), None)
    slot_spec = P('ep', None, None)
    return jax.shard_map(device_step, mesh=mesh,
                         in_specs=(token_spec, P(), slot_spec, slot_spec, slot_spec, token_spec, P(), P(), P(), P()),
                         out_specs=token_spec, check_vma=False)
```

```python
import jax
import jax.numpy as jnp
from jax import lax
from jax.experimental import pallas as pl
from jax.experimental.pallas import tpu as pltpu
from jax.sharding import PartitionSpec as P

ROUTE_SCALE = 2.5
RING = 4
CAP = 9
BF16 = jnp.bfloat16
F32 = jnp.float32
STRIDE = {'x': 2, 'y': 8, 'z': 32}
CLASSES = (('y', 'z', 'x'), ('z', 'x', 'y'), ('x', 'y', 'z'))


def iota(shape, dim):
    return lax.broadcasted_iota(jnp.int32, shape, dim)


def dot(a, b):
    return jnp.dot(a, b, preferred_element_type=F32)


def dot_t(a, b):
    return lax.dot_general(a, b, (((1,), (1,)), ((), ())), preferred_element_type=F32)


def as_onehot(cond):
    return jnp.where(cond, 1.0, 0.0).astype(BF16)


def three_parts(v):
    hi = v.astype(BF16)
    rest = v - hi.astype(F32)
    mid = rest.astype(BF16)
    lo = (rest - mid.astype(F32)).astype(BF16)
    return hi, mid, lo


def moe_kernel(x_hbm, assign_hbm, slot_expert_hbm, wr_hbm, w1_hbm, w3_hbm, w2_hbm, s1_hbm, s3_hbm, s2_hbm, y_ref,
               x_ref, assign_ref, slot_expert_ref, wr_ref,
               G, T, tab, Pm, Sb, R, Ob, Hb, Z, F, Cs, Cr, U, A, zs, w1, w3, w2, s1, s3, s2,
               wsem, isem, sent, t1r, t2r, g0r, g1r, g2r, cr, d3r, d5r, d6r, d7r):
    t1s, t2s, g1s, g2s, cs, d3s, d5s, d6s, d7s = (sent.at[i] for i in range(9))
    me = lax.axis_index('ep')
    core = me % 2
    pos = {'x': (me // 2) % RING, 'y': (me // 8) % RING, 'z': me // 32}
    third = x_ref.shape[1] // 3
    sixth = third // 2

    def moved(axis, value):
        return (value - pos[axis]) * STRIDE[axis]

    def step_to(axis, d):
        return (pos[axis] + d) % RING

    def remote(src, dst, ssem, rsem, dev):
        return pltpu.make_async_remote_copy(src_ref=src, dst_ref=dst, send_sem=ssem, recv_sem=rsem,
                                            device_id={'ep': dev}, device_id_type=pl.DeviceIdType.MESH)

    def local(src, dst, sem):
        return pltpu.make_async_copy(src, dst, sem)

    def wait_bytes(ref, sem):
        pltpu.make_async_copy(ref, ref, sem).wait()

    barrier = pltpu.get_barrier_semaphore()

    def greet(dev):
        pl.semaphore_signal(barrier, inc=1, device_id={'ep': dev}, device_id_type=pl.DeviceIdType.MESH)

    other = 1 - 2 * core
    greet(me + other)
    for axis in 'xyz':
        for d in range(1, RING):
            dev = me + moved(axis, step_to(axis, d))
            greet(dev)
            greet(dev + other)

    input_copies = [local(s, d, isem.at[i]) for i, (s, d) in enumerate(
        ((assign_hbm, assign_ref), (x_hbm, x_ref), (slot_expert_hbm, slot_expert_ref), (wr_hbm, wr_ref)))]
    for c in input_copies:
        c.start()
    expert_weights = [(w2_hbm.at[0], w2, 3)]
    for g in range(2):
        for cls in range(3):
            src, dst = pl.ds((2 * cls + g) * sixth, sixth), pl.ds((3 * g + cls) * sixth, sixth)
            expert_weights += [(w1_hbm.at[0, src], w1.at[dst], 4), (w3_hbm.at[0, src], w3.at[dst], 5)]
    weight_copies = [local(s, d, wsem.at[i]) for s, d, i in
                     [(s1_hbm, s1, 0), (s3_hbm, s3, 1), (s2_hbm, s2, 2)] + expert_weights]

    input_copies[0].wait()
    tokens = x_ref.shape[0]
    slots = slot_expert_ref.shape[1]
    slot_row = iota((slots, tokens), 0)
    chosen_t = jnp.zeros((slots, tokens), F32)
    for k in range(assign_ref.shape[0]):
        chosen_t = chosen_t + jnp.where(assign_ref[k:k + 1, :] == slot_row, 1.0, 0.0)
    ti, tj = iota((tokens, tokens), 0), iota((tokens, tokens), 1)
    chosen = dot_t(as_onehot(ti == tj), chosen_t.astype(BF16))
    rank = jnp.where(chosen > 0.5, dot(as_onehot(tj < ti), chosen.astype(BF16)), 99.0)
    token_id = (iota((tokens, slots), 0) + 1).astype(F32)
    tab_rows = [jnp.sum(jnp.where(rank == float(r), token_id, 0.0), axis=0, keepdims=True) for r in range(CAP)]
    tab[...] = jnp.concatenate(tab_rows + [jnp.zeros((16 - CAP, slots), F32)], axis=0).astype(BF16)

    for c in input_copies[1:]:
        c.wait()
    pl.semaphore_wait(barrier, 19)

    def cols(cls, g):
        return x_ref.at[:, pl.ds((2 * cls + g) * sixth, sixth)]

    def spread(cls, g, k, src, to):
        a2 = CLASSES[cls][1]
        for d in (1, 3, 2):
            remote(src, G.at[cls, g, pos[a2], to], g2s, g2r.at[g],
                   me + moved(a2, step_to(a2, d))).start()

    for g in range(2):
        for cls, (a1, a2, a3) in enumerate(CLASSES):
            for d in (1, 3, 2):
                dev = me + moved(a1, step_to(a1, d))
                if g == 0:
                    remote(tab, T.at[cls, pos[a2], pos[a1]], t1s, t1r.at[0], dev).start()
                remote(cols(cls, g), G.at[cls, g, pos[a2], pos[a1]], g1s, g1r.at[g, d - 1], dev).start()
        for cls, (a1, a2, a3) in enumerate(CLASSES):
            spread(cls, g, 0, cols(cls, g), pos[a1])
            local(cols(cls, g), G.at[cls, g, pos[a2], pos[a1]], g0r.at[0]).start()
            if g == 0:
                T[cls, pos[a2], pos[a1]] = tab[...]

    for c in weight_copies:
        c.start()

    gate = jax.nn.sigmoid(dot_t(x_ref[...], wr_ref[...]))
    num_experts = wr_ref.shape[0]
    slot_of = as_onehot(iota((num_experts, slots), 0) == slot_expert_ref[...])
    gate_slot = sum(dot(p, slot_of) for p in three_parts(gate))
    picked = jnp.where(chosen > 0.5, gate_slot, 0.0)
    route = ROUTE_SCALE * picked / jnp.maximum(jnp.sum(picked, axis=1, keepdims=True), 1e-30)
    route_rank = jnp.concatenate(three_parts(route) + (rank.astype(BF16),), axis=1)

    for g in range(2):
        for d in (3, 1, 2):
            wait_bytes(G.at[:, g, 0, 0], g1r.at[g, d - 1])
            for cls, (a1, a2, a3) in enumerate(CLASSES):
                owner = (pos[a1] + RING - d) % RING
                spread(cls, g, d, G.at[cls, g, pos[a2], owner], owner)
        if g == 0:
            wait_bytes(T.at[:, 0, 0:3], t1r.at[0])
            for cls, (a1, a2, a3) in enumerate(CLASSES):
                row = T.at[cls, pos[a2]]
                for d in (1, 3, 2):
                    remote(row, row, t2s, t2r.at[0], me + moved(a2, step_to(a2, d))).start()

    si, sj = iota((4 * slots, 128), 0), iota((4 * slots, 128), 1)
    for cls, (a1, a2, a3) in enumerate(CLASSES):
        q_slot = (sj // 32 * slots + sj // 8 % 4 * STRIDE[a2] + sj // 4 % 2 + sj % 4 * STRIDE[a3])
        for v in range(RING):
            Cs[cls, v] = dot(route_rank, as_onehot(si == q_slot + v * STRIDE[a1])).astype(BF16)

    for c in weight_copies[:3]:
        c.wait()
    ff_shared = s1.shape[1]
    step = 512
    acc = jnp.zeros((tokens, x_ref.shape[1]), F32)
    for f in range(0, ff_shared, step):
        xs = x_ref[...]
        mid = (jax.nn.silu(dot(xs, s1[:, f:f + step])) * dot(xs, s3[:, f:f + step])).astype(BF16)
        acc = acc + dot(mid, s2[f:f + step, :])
    zs[...] = acc

    rows = CAP * 8
    qi, qj = iota((rows, 256), 0), iota((rows, 256), 1)
    by_rank = [as_onehot(qj == (qi % 8 + 8 * h) * 16 + qi // 8) for h in range(2)]
    src_base = ((iota((rows, 128), 0) % 8) * tokens).astype(F32)
    lane = iota((rows, 128), 1).astype(F32)
    tabs, lines = [], []

    wait_bytes(G.at[:, :, 0, 0], g0r.at[0])
    wait_bytes(G.at[:, 0, 0:3], g2r.at[0])
    wait_bytes(T.at[:, 0:3], t2r.at[0])
    for cls, (a1, a2, a3) in enumerate(CLASSES):
        tabs.append([dot(m, T[cls].reshape(256, slots)).astype(BF16) for m in by_rank])
        lines.append(me - core - pos[a3] * STRIDE[a3])

    def select(n, _):
        g, e, p = n // 2 % 2, n // 4, n % 2

        @pl.when(n == 2)
        def _():
            wait_bytes(G.at[:, 1, 0:3], g2r.at[1])

        @pl.when(g == 0)
        def _():
            for cls, (a1, a2, a3) in enumerate(CLASSES):
                for q in range(2):
                    d = 2 + q - p * (1 + 2 * q)
                    slot = lines[cls] + step_to(a3, d) * STRIDE[a3] + (core + e) % 2
                    pick = as_onehot(iota((slots, 128), 0) == slot)
                    for h in range(2):
                        val = dot(tabs[cls][h], pick)
                        code = jnp.where(val > 0.5, val - 1.0 + src_base, -1.0)
                        for b in range(8 * tokens // 128):
                            Pm[p, cls, h, q * rows:(q + 1) * rows, b * 128:(b + 1) * 128] = (
                                jnp.where(code == lane + float(b * 128), 1.0, 0.0))

        for cls, (a1, a2, a3) in enumerate(CLASSES):
            outs = []
            for h in range(2):
                out = dot(Pm[p, cls, h].astype(BF16), G[cls, g, 2 * h:2 * h + 2].reshape(8 * tokens, sixth))
                outs.append(out.reshape(2, CAP, 8, sixth))
            both = jnp.concatenate(outs, axis=2).astype(BF16)
            for q in range(2):
                d = 2 + q - p * (1 + 2 * q)
                k = 2 * d + e
                Sb[cls, g, k] = both[q]
                dev = me + moved(a3, step_to(a3, d)) + (core + e) % 2 - core
                src, dst = Sb.at[cls, g, k], R.at[cls, g, pl.ds(core * CAP, CAP), pos[a3]]
                if q == 1:
                    mine = jnp.logical_and(n < 4, n % 2 == 1)

                    @pl.when(mine)
                    def _():
                        local(src, dst, d3r.at[e, g]).start()

                    @pl.when(jnp.logical_not(mine))
                    def _():
                        remote(src, dst, d3s, d3r.at[e, g], dev).start()
                else:
                    remote(src, dst, d3s, d3r.at[e, g], dev).start()
        return 0

    lax.fori_loop(0, 2 * RING, select, 0)

    for cls, (a1, a2, a3) in enumerate(CLASSES):
        for d in (1, 3, 2, 0):
            v = step_to(a1, d)
            if d == 0:
                Cr[cls, pos[a1]] = Cs[cls, v]
            else:
                remote(Cs.at[cls, v], Cr.at[cls, pos[a1]], cs, cr.at[0], me + moved(a1, v)).start()

    for w, i in ((w2, 3), (w1, 4), (w3, 5)):
        wait_bytes(w, wsem.at[i])
    blk = 3 * 64
    pi, pj = iota((blk, blk), 0), iota((blk, blk), 1)

    def bits(v):
        return v // 16 % 4, v // 4 % 4, v % 4

    ix, iz, iy = bits(pi)
    jx, jz, jy = bits(pj)
    to_first = {1: as_onehot(pj == pi // 64 * 64 + iy * 16 + ix * 4 + iz),
                2: as_onehot(pj == pi // 64 * 64 + iz * 16 + iy * 4 + ix)}
    from_first = {1: as_onehot(pi == pj // 64 * 64 + jy * 16 + jx * 4 + jz),
                  2: as_onehot(pi == pj // 64 * 64 + jz * 16 + jy * 4 + jx)}

    def permuted(mats, cls, value):
        if cls == 0:
            return value
        return jnp.concatenate([dot(mats[cls], value[i:i + blk]).astype(BF16)
                                for i in range(0, value.shape[0], blk)], axis=0)

    def expert(e, _):
        half = (core + e) % 2
        n = CAP * 64
        h_gate = h_up = 0.0
        for g in range(2):
            wait_bytes(R.at[:, g, 0:CAP], d3r.at[e, g])
            xs = jnp.concatenate([permuted(to_first, cls, R[cls, g, pl.ds(half * CAP, CAP)].reshape(n, sixth))
                                  for cls in range(3)], axis=1)
            part = slice(3 * g * sixth, 3 * (g + 1) * sixth)
            h_gate = h_gate + dot(xs, w1[part])
            h_up = h_up + dot(xs, w3[part])
        mid = (jax.nn.silu(h_gate) * h_up).astype(BF16)
        for cls, (a1, a2, a3) in enumerate(CLASSES):
            out = dot(mid, w2[:, cls * third:(cls + 1) * third]).astype(BF16)
            Ob[cls, pl.ds(half * CAP, CAP)] = permuted(from_first, cls, out).reshape(CAP, RING, 16, third)
            for d in (2, 1, 3, 0):
                v = step_to(a3, d)
                dev = me + moved(a3, v) + half - core
                src, dst = Ob.at[cls, pl.ds(half * CAP, CAP), v], Hb.at[cls, core, :, pos[a3]]
                if d == 0:
                    @pl.when(e == 0)
                    def _():
                        local(src, dst, d5r.at[e, cls]).start()

                    @pl.when(e != 0)
                    def _():
                        remote(src, dst, d5s, d5r.at[e, cls], dev).start()
                else:
                    remote(src, dst, d5s, d5r.at[e, cls], dev).start()
        return 0

    lax.fori_loop(0, 2, expert, 0)

    u2, v3 = pi // 16 % 4, pi // 4 % 4
    by_second = as_onehot(pj == pi // 64 * 64 + v3 * 16 + u2 * 4 + pi % 4)

    def regroup(e):
        half = (core + e) % 2
        for cls, (a1, a2, a3) in enumerate(CLASSES):
            wait_bytes(Hb.at[cls, half], d5r.at[e, cls])
            rows_in = Hb[cls, half].reshape(CAP * 64, third)
            Z[cls, half] = jnp.concatenate([dot(by_second, rows_in[i:i + blk]).astype(BF16) for i in
                                            range(0, CAP * 64, blk)], axis=0).reshape(CAP, RING, 16, third)
            parts = [pl.ds(0, third)] if e == 0 else [pl.ds(0, sixth), pl.ds(sixth, sixth)]
            for i, part in enumerate(parts):
                for d in (2, 1, 3, 0):
                    v = step_to(a2, d)
                    src, dst = Z.at[cls, half, :, v, :, part], F.at[cls, half, :, pos[a2], :, part]
                    if d == 0:
                        local(src, dst, d6r.at[e + i, cls]).start()
                    else:
                        remote(src, dst, d6s, d6r.at[e + i, cls], me + moved(a2, v)).start()
    for e in range(2):
        regroup(e)

    wait_bytes(Cr.at[:, 0:3], cr.at[0])

    def spreads(half):
        ei, ej = iota((128, 256), 0), iota((128, 256), 1)
        q = ej // 16 % 4 * 8 + half * 4 + ej // 4 % 4
        return [as_onehot(ei == q + 32 * part) for part in range(4)]

    chunks = [(r0, min(4, CAP - r0)) for r0 in range(0, CAP, 4)]

    def weights(cls, spread_mats, targets):
        lane_pos = iota((tokens * len(targets), 256), 1)
        c = jnp.concatenate([Cr[cls, v] for v in targets], axis=0)
        w_exp = [dot(c, spread_mats[part]) for part in range(3)]
        source = jnp.concatenate([jnp.full((tokens, 256), v, jnp.int32) for v in targets], axis=0)
        rank_exp = jnp.where(lane_pos % 4 == source, dot(c, spread_mats[3]) - (lane_pos // 64).astype(F32), 99.0)
        return [[jnp.where(rank_exp == float(r0), w, 0.0).astype(BF16) for w in w_exp] for r0, _ in chunks]

    def weigh(mats, rows_of, count, width):
        m = tokens * count
        acc = jnp.zeros((3 * m, width), F32)
        for (r0, k), w in zip(chunks, mats):
            acc = acc + dot(jnp.concatenate(w, axis=0)[:, :64 * k], rows_of(r0, k).reshape(64 * k, width))
        return (acc[2 * m:] + acc[m:2 * m] + acc[:m]).reshape(count, tokens, width)

    every = list(range(RING))
    first, second = spreads(core), spreads(1 - core)
    for cls in range(3):
        wait_bytes(F.at[cls, core], d6r.at[0, cls])
        U[cls] = weigh(weights(cls, first, every), lambda r0, k: F[cls, core, r0:r0 + k], RING, third)

    def place(i, part, v):
        t = (i * 3 + part) * RING + v
        return t // (2 * CAP), t % (2 * CAP)

    for cls in range(3):
        for i, mats in enumerate(weights(cls, second, every)):
            for part in range(3):
                for v in every:
                    R[(cls,) + place(i, part, v)] = mats[part][v * tokens:(v + 1) * tokens].reshape(RING, 16, sixth)
    for g, groups in ((0, ((2,), (1, 3))), (1, ((2,), (1, 3), (0,))), (0, ((0,),))):
        here = slice(g * sixth, (g + 1) * sixth)
        span = pl.ds(g * sixth, sixth)
        for group in groups:
            for cls, (a1, a2, a3) in enumerate(CLASSES):
                if group == (2,):
                    wait_bytes(F.at[cls, 1 - core, :, :, :, 0:sixth], d6r.at[1 + g, cls])
                targets = [step_to(a1, d) for d in group]
                mats = [[jnp.concatenate([R[(cls,) + place(i, part, v)].reshape(tokens, sixth) for v in targets], axis=0)
                         for part in range(3)] for i in range(len(chunks))]
                added = weigh(mats, lambda r0, k: F[cls, 1 - core, r0:r0 + k, :, :, here], len(group), sixth)
                for i, (d, v) in enumerate(zip(group, targets)):
                    if d == 0:
                        A[cls, pos[a1], :, here] = U[cls, v, :, here] + added[i]
                    else:
                        U[cls, v, :, here] = U[cls, v, :, here] + added[i]
                        remote(U.at[cls, v, :, span], A.at[cls, pos[a1], :, span], d7s, d7r.at[g, cls],
                               me + moved(a1, v)).start()
    for g in range(2):
        for cls in range(3):
            wait_bytes(A.at[cls, 0:3, :, 0:sixth], d7r.at[g, cls])
            here = slice(g * sixth, (g + 1) * sixth)
            there = slice((2 * cls + g) * sixth, (2 * cls + g + 1) * sixth)
            routed = (A[cls, 0, :, here] + A[cls, 1, :, here]) + (A[cls, 2, :, here] + A[cls, 3, :, here])
            y_ref[:, there] = (zs[:, there] + routed).astype(BF16)

    for ref, sem in ((T.at[:, 0, 0:3], t1s), (T.at[:, 0:3], t2s), (G.at[:, :, 0, 0:3], g1s), (G.at[:, :, 0:3], g2s),
                     (Cs.at[:, 0:3], cs), (Sb.at[:, :, 0:7], d3s), (Sb.at[:, :, 0:7], d5s), (Z.at[:, :, :, 0:3], d6s),
                     (U.at[:, 0:3], d7s)):
        wait_bytes(ref, sem)


def solution(mesh):
    def device_step(x_tokens, slot_expert, w1_slots, w3_slots, w2_slots, assign, w_router, w1_shared, w3_shared, w2_shared):
        tokens, dim = x_tokens.shape
        third = dim // 3
        slots = slot_expert.shape[0]
        vmem = pl.BlockSpec(memory_space=pltpu.VMEM)
        hbm = pl.BlockSpec(memory_space=pltpu.HBM)
        dma = pltpu.SemaphoreType.DMA
        V = pltpu.VMEM
        return pl.pallas_call(
            moe_kernel,
            out_shape=jax.ShapeDtypeStruct((tokens, dim), BF16),
            in_specs=[hbm] * 10,
            out_specs=vmem,
            scratch_shapes=[
                V((tokens, dim), BF16), V(assign.T.shape, jnp.int32), V((1, slots), jnp.int32), V(w_router.T.shape, BF16),
                V((3, 2, RING, RING, tokens, third // 2), BF16),
                V((3, RING, RING, 16, slots), BF16),
                V((16, slots), BF16),
                V((2, 3, 2, 2 * CAP * 8, 8 * tokens), F32),
                V((3, 2, 8, CAP, 16, third // 2), BF16),
                V((3, 2, 2 * CAP, RING, 16, third // 2), BF16),
                V((3, 2 * CAP, RING, 16, third), BF16),
                V((3, 2, CAP, RING, 16, third), BF16),
                V((3, 2, CAP, RING, 16, third), BF16),
                V((3, 2, CAP, RING, 16, third), BF16),
                V((3, RING, tokens, 128), BF16), V((3, RING, tokens, 128), BF16),
                V((3, RING, tokens, third), F32), V((3, RING, tokens, third), F32),
                V((tokens, dim), F32),
                V(w1_slots.shape[1:], BF16), V(w3_slots.shape[1:], BF16), V(w2_slots.shape[1:], BF16),
                V(w1_shared.shape, BF16), V(w3_shared.shape, BF16), V(w2_shared.shape, BF16),
                dma((6,)), dma((4,)), dma((9,)), dma((1,)), dma((1,)), dma((1,)), dma((2, 3)), dma((2,)), dma((1,)),
                dma((2, 2)), dma((2, 3)), dma((3, 3)), dma((2, 3)),
            ],
            compiler_params=pltpu.CompilerParams(collective_id=0, has_side_effects=True,
                                                 vmem_limit_bytes=54950 * 1024),
        )(x_tokens, assign.T, slot_expert.reshape(1, -1), w_router.T, w1_slots, w3_slots, w2_slots,
          w1_shared, w3_shared, w2_shared)

    token_spec = P(('dp', 'ep'), None)
    slot_spec = P('ep', None, None)
    return jax.shard_map(device_step, mesh=mesh,
                         in_specs=(token_spec, P(), slot_spec, slot_spec, slot_spec, token_spec, P(), P(), P(), P()),
                         out_specs=token_spec, check_vma=False)
```
